32 devices in a mesh: gx: 4 (over x, core), gy: 8 (over z, y).
Axes of the slice: x: 2, y: 2, z: 4, core: 2. Of those that a mesh axis runs over, the one named last changes fastest.
Arguments:
- right_side: float32 [2, 64, 256, 128], P(None, 'gx', 'gy'), may hold values from -6 to 6
- wavenumber: float32 [64, 256, 128], P('gx', 'gy'), may hold values from 0.2 to 1
- pml_layer: int32 [64, 256, 128], P('gx', 'gy'), may hold values from 0 to 3
- aggregate: int32 [64, 256, 128], P('gx', 'gy'), may hold values from 0 to 15, as said below
- coarse_inverse: float32 [2, 512, 512], P(None, ('gx', 'gy')), may hold values from -0.0029296875 to 0.0029296875
Outputs:
- solution: float32 [2, 64, 256, 128], P(None, 'gx', 'gy')
- hessenberg: float32 [2, 5, 4], replicated
The draws below stay inside these ranges and needn't reach their ends.
Inputs may be any that keep to these rules, and one draw needn't show every extreme that they name: `aggregate`: along the third dimension the value never falls, and every value of 0 to 15 occurs in every column of cells.
All inputs are finite; a program needn't handle non-finite values.
Results may differ from the reference program's by a relative error of at most 0.00015.
Values sent between devices are 32-bit elements; how exact they have to be, the bound alone decides.
No kernel may reach another device: no remote copies, remote signals or barrier semaphores. Data moves between devices by JAX's collectives and lax.ppermute only.
A program may use at most 64 MiB of HBM per device.

```python
import math
import jax
import jax.numpy as jnp
from jax import lax

CX = 16
CY = 32
CZ = 128
AGG_DEV = 16
ITERS = 4
NX = 64
NY = 256
NZ = 128
COARSE = 512
N_GX = 4
N_GY = 8


def draw_aggregate(key, part):
    band = CZ // AGG_DEV
    offset = jax.random.randint(key, (NX, NY, 1), -(band // 2), band // 2 + 1, dtype=jnp.int32)
    depth = jnp.arange(NZ, dtype=jnp.int32)[None, None, :]
    return jnp.clip((depth + offset) // band, 0, AGG_DEV - 1).astype(jnp.int32)


def with_ends(entries, stream_key, low, high):
    shape = entries.shape
    spot = [jax.random.randint(jax.random.fold_in(stream_key, axis), (), 0, shape[axis]) for axis in range(len(shape))]
    entries = entries.at[tuple(spot)].set(low)
    longest = shape.index(max(shape))
    spot[longest] = (spot[longest] + 1) % shape[longest]
    return entries.at[tuple(spot)].set(high)


def shard_levels(stream_key, dims, cuts, low, high):
    level = 1.0
    for dim, parts in cuts:
        draws = jax.random.uniform(jax.random.fold_in(jax.random.fold_in(stream_key, 6), dim), (parts,), jnp.float32, low / len(cuts), high / len(cuts))
        level = level * jnp.repeat(jnp.exp(draws), dims[dim] // parts).reshape((-1,) + (1,) * (len(dims) - 1 - dim))
    return level


def scatter_about(rng, extent, width, bound, split=(), kind=jnp.bfloat16):
    result = jax.random.normal(rng, extent, jnp.float32) * width
    if len(split) > 0:
        result = shard_levels(rng, extent, split, -0.22, 0.18) * result
    return jnp.clip(result, min=-bound, max=bound).astype(kind)


def setup_inputs(seed: int = 0) -> dict:
    splits = jax.random.split(jax.random.key(seed), 6)
    right_side = scatter_about(splits[0], (2, NX, NY, NZ), 1.0, 6.0, ((1, 4), (2, 8)), jnp.float32)
    wavenumber = jnp.clip(jnp.exp(math.log(1.0) - 1.609438 * jax.random.uniform(splits[1], (NX, NY, NZ), jnp.float32) ** shard_levels(splits[1], (NX, NY, NZ), ((0, 4), (1, 8)), -0.2, 0.2)), 0.2, 1.0)
    pml_layer = with_ends(jax.random.randint(splits[2], (NX, NY, NZ), 0, 4), jax.random.fold_in(splits[2], 1), 0, 3).astype(jnp.int32)
    aggregate = draw_aggregate(jax.random.fold_in(splits[5], 71), 0)
    coarse_inverse = scatter_about(splits[4], (2, COARSE, COARSE), (2 * COARSE * CX * CY * (CZ // AGG_DEV)) ** -0.5, 0.0029296875, ((1, 32),), jnp.float32)
    return {"right_side": right_side, "wavenumber": wavenumber, "pml_layer": pml_layer, "aggregate": aggregate, "coarse_inverse": coarse_inverse}


damping = 0.8
pml_strength = 3.0
epsilon = 1e-06

def coefficients(wavenumber, layer_float):
    wave_sq = wavenumber * wavenumber
    depth = layer_float / 3.0
    absorb = wave_sq * (pml_strength * depth * depth)
    diag_re = 6.0 - wave_sq
    magnitude = diag_re * diag_re + absorb * absorb
    return (wave_sq, absorb, damping * diag_re / magnitude, damping * absorb / magnitude)

def operate(field, wave_sq, absorb):
    padded = jnp.pad(field, ((0, 0), (1, 1), (1, 1), (1, 1)))
    beside = padded[:, 2:, 1:-1, 1:-1] + padded[:, :-2, 1:-1, 1:-1] + padded[:, 1:-1, 2:, 1:-1] + padded[:, 1:-1, :-2, 1:-1] + padded[:, 1:-1, 1:-1, 2:] + padded[:, 1:-1, 1:-1, :-2]
    real_part = (6.0 - wave_sq) * field[0] - beside[0] + absorb * field[1]
    imag_part = (6.0 - wave_sq) * field[1] - beside[1] - absorb * field[0]
    return jnp.stack([real_part, imag_part])

def smooth(field, scale_re, scale_im):
    return jnp.stack([scale_re * field[0] - scale_im * field[1], scale_re * field[1] + scale_im * field[0]])

def complex_scale(scale_re, scale_im, field):
    return jnp.stack([scale_re * field[0] - scale_im * field[1], scale_re * field[1] + scale_im * field[0]])

def inner(left, right):
    return jnp.stack([jnp.sum(left[0] * right[0] + left[1] * right[1]), jnp.sum(left[0] * right[1] - left[1] * right[0])])

def least_squares(hessenberg, beta):
    real_h = hessenberg[0]
    imag_h = hessenberg[1]
    stacked = jnp.concatenate([jnp.concatenate([real_h, -imag_h], 1), jnp.concatenate([imag_h, real_h], 1)], 0)
    count = stacked.shape[1]
    target = jnp.zeros((stacked.shape[0],), jnp.float32).at[0].set(beta)
    ortho = []
    upper = {}
    for column in range(count):
        vector = stacked[:, column]
        for position in range(column):
            upper[position, column] = jnp.zeros((), jnp.float32)
        for repeat in range(2):
            for position in range(len(ortho)):
                weight = jnp.sum(ortho[position] * vector)
                vector = vector - weight * ortho[position]
                upper[position, column] = upper[position, column] + weight
        norm_value = jnp.sqrt(jnp.sum(vector * vector))
        upper[column, column] = norm_value
        ortho.append(vector / norm_value)
    project = [jnp.sum(basis_vec * target) for basis_vec in ortho]
    solved = [None] * count
    for column in reversed(range(count)):
        total = project[column]
        for later in range(column + 1, count):
            total = total - upper[column, later] * solved[later]
        solved[column] = total / upper[column, column]
    return solved

def precondition(vector, wave_sq, absorb, scale_re, scale_im, global_ids, coarse_inverse):
    highest = lax.Precision.HIGHEST
    first = smooth(vector, scale_re, scale_im)
    second = first + smooth(vector - operate(first, wave_sq, absorb), scale_re, scale_im)
    remainder = vector - operate(second, wave_sq, absorb)
    coarse_rhs = jax.ops.segment_sum(remainder.reshape(2, -1).T, global_ids, num_segments=COARSE).T
    coarse_re = jnp.dot(coarse_inverse[0], coarse_rhs[0], precision=highest) - jnp.dot(coarse_inverse[1], coarse_rhs[1], precision=highest)
    coarse_im = jnp.dot(coarse_inverse[0], coarse_rhs[1], precision=highest) + jnp.dot(coarse_inverse[1], coarse_rhs[0], precision=highest)
    spread = jnp.stack([coarse_re[global_ids], coarse_im[global_ids]]).reshape(remainder.shape)
    return second + spread

def reference(right_side, wavenumber, pml_layer, aggregate, coarse_inverse):
    wave_sq, absorb, scale_re, scale_im = coefficients(wavenumber, pml_layer.astype(jnp.float32))
    owner_x = jnp.arange(NX, dtype=jnp.int32) // (NX // N_GX)
    owner_y = jnp.arange(NY, dtype=jnp.int32) // (NY // N_GY)
    owner = (owner_x[:, None] * N_GY + owner_y[None, :]) * AGG_DEV
    global_ids = (owner[:, :, None] + aggregate).reshape(-1).astype(jnp.int32)
    beta = jnp.sqrt(jnp.sum(right_side * right_side) + epsilon)
    basis = [right_side / beta]
    directions = []
    columns_re = []
    columns_im = []
    for column in range(ITERS):
        direction = precondition(basis[column], wave_sq, absorb, scale_re, scale_im, global_ids, coarse_inverse)
        image = operate(direction, wave_sq, absorb)
        dots = jnp.stack([inner(vector, image) for vector in basis], 1)
        for position in range(len(basis)):
            image = image - complex_scale(dots[0, position], dots[1, position], basis[position])
        length = jnp.sqrt(jnp.sum(image * image) + epsilon)
        tail = jnp.zeros((ITERS - 1 - column,), jnp.float32)
        columns_re.append(jnp.concatenate([dots[0], length[None], tail]))
        columns_im.append(jnp.concatenate([dots[1], jnp.zeros((1,), jnp.float32), tail]))
        directions.append(direction)
        if column + 1 < ITERS:
            basis.append(image / length)
    hessenberg = jnp.stack([jnp.stack(columns_re, 1), jnp.stack(columns_im, 1)])
    solved = least_squares(hessenberg, beta)
    solution = jnp.zeros_like(right_side)
    for column in range(ITERS):
        solution = solution + complex_scale(solved[column], solved[ITERS + column], directions[column])
    return (solution, hessenberg)
```

```python
import functools

import jax
import jax.numpy as jnp
from jax import lax
from jax.experimental import pallas as pl
from jax.experimental.pallas import tpu as pltpu
from jax.sharding import PartitionSpec as P

ITERS = 4
HALO = 2 * ITERS
AXES = ("gx", "gy")
AGG = 16
damping = 0.8
pml_strength = 3.0
epsilon = 1e-06
F32 = jnp.float32
VLIMIT = 24 * 1024 * 1024


def lanes(shape):
    return lax.broadcasted_iota(jnp.int32, shape, len(shape) - 1)


def turn(x):
    odd = (lanes(x.shape) // AGG) % 2 == 1
    return jnp.where(odd, pltpu.roll(x, AGG, 1), -pltpu.roll(x, x.shape[1] - AGG, 1))


def turn_rows(x):
    parts = [turn(x[:, i : i + 128]) for i in range(0, x.shape[1], 128)]
    return jnp.concatenate(parts, axis=1)


def pick(row, lane):
    return jnp.broadcast_to(row[:, lane : lane + 1], (8, 128))


def take(table, index):
    rows = index.shape[0]
    src = jnp.broadcast_to(table, (rows, 128))
    return jnp.take_along_axis(src, index, axis=1, mode="promise_in_bounds")


def planes(lo, hi, fn, carry=None, unroll=1):
    if carry is None:
        def go(x, c):
            fn(x)
            return c
        return lax.fori_loop(lo, hi, go, 0, unroll=unroll)
    return lax.fori_loop(lo, hi, fn, carry, unroll=unroll)


def stencil(ref, c, x, y0, y1):
    mid = ref[c, x, 8 + y0 : 8 + y1, :]
    total = (
        ref[c, x - 1, 8 + y0 : 8 + y1, :]
        + ref[c, x + 1, 8 + y0 : 8 + y1, :]
        + ref[c, x, 7 + y0 : 7 + y1, :]
        + ref[c, x, 9 + y0 : 9 + y1, :]
    )
    lane = lanes(mid.shape)
    last = mid.shape[-1] - 1
    total = total + jnp.where(lane == 0, 0.0, pltpu.roll(mid, 1, 1))
    total = total + jnp.where(lane == last, 0.0, pltpu.roll(mid, last, 1))
    return mid, total


def operate_plane(ref, diag, absorb, x, y0, y1):
    d = diag[x, y0:y1, :]
    a = absorb[x, y0:y1, :]
    m0, t0 = stencil(ref, 0, x, y0, y1)
    m1, t1 = stencil(ref, 1, x, y0, y1)
    return d * m0 - t0 + a * m1, d * m1 - t1 - a * m0


def zero_pads(ref, ey):
    shape = ref.shape
    z = jnp.zeros((8, shape[3]), F32)
    for c in range(2):
        def go(x, carry, c=c):
            ref[c, x, 0:8, :] = z
            ref[c, x, 8 + ey : 16 + ey, :] = z
            return carry
        lax.fori_loop(0, shape[1], go, 0)


def fold8(x):
    out = x[0:8]
    for i in range(8, x.shape[0], 8):
        out = out + x[i : i + 8]
    return out


def prefix(x):
    lane = lanes(x.shape)
    step = 1
    while step < x.shape[1]:
        x = x + jnp.where(lane >= step, pltpu.roll(x, step, 1), 0.0)
        step *= 2
    return x


def spread_rhs(g0, g1, cols_ref, pad_ref, out_ref, scalars, grid):
    gx, gy = grid
    n = gx * gy
    lane = lanes((1, 128))
    rows = []
    for g in (g0, g1):
        total = jnp.sum(g, axis=0, keepdims=True)
        rows.append(jnp.where(lane == 0, total, total - pltpu.roll(total, 1, 1)))
    z = []
    for row in rows:
        acc = None
        for q in range(4):
            weight = take(row, lanes((8, 128)) // 32 + 4 * q)[0:1]
            term = cols_ref[:, 128 * q : 128 * (q + 1)] * weight
            acc = term if acc is None else acc + term
        acc = acc + pltpu.roll(acc, 64, 1)
        z.append(acc + pltpu.roll(acc, 32, 1))
    whole = z[0] + turn(z[1])
    margin = (pad_ref.shape[0] - n) // 2
    pad_ref[0:margin, :] = jnp.zeros((margin, 128), F32)
    pad_ref[margin + n : 2 * margin + n, :] = jnp.zeros((margin, 128), F32)
    pad_ref[margin : margin + n, :] = whole
    place = lax.broadcasted_iota(jnp.int32, (n, 128), 0) % gy
    group = lanes((n, 128)) // 32
    outs = [jnp.zeros((n, 128), F32) for _ in range(3)]
    for dx in (-1, 0, 1):
        for dy in (-1, 0, 1):
            k = (dx + 1) * 3 + dy + 1
            start = margin + dx * gy + dy
            piece = pad_ref[start : start + n, :]
            ok = (group == k % 4) & (place + dy >= 0) & (place + dy < gy)
            outs[k // 4] = jnp.where(ok, piece, outs[k // 4])
    outs[2] = outs[2] + jnp.broadcast_to(scalars, (n, 128))
    for r in range(3):
        out_ref[:, 128 * r : 128 * (r + 1)] = outs[r]


def scalar_row(items):
    lane = lanes((1, 128))
    row = jnp.zeros((1, 128), F32)
    for where, acc in items:
        s = jnp.sum(jnp.sum(acc, axis=0, keepdims=True), axis=1, keepdims=True)
        row = jnp.where(lane == where, jnp.broadcast_to(s, (1, 128)), row)
    return row


def second_passes(f, g, u_at, coefs, halo, own, ends, t_ref, s_ref, ey):
    diag, absorb, sre, sim = coefs
    cx, cy = own

    def smooth_pass(x):
        a0, a1 = operate_plane(f, diag, absorb, x, 0, ey)
        u0, u1 = u_at(x, 0, ey)
        e0, e1 = u0 - a0, u1 - a1
        p, q = sre[x], sim[x]
        g[0, x, 8 : 8 + ey, :] = f[0, x, 8 : 8 + ey, :] + (p * e0 - q * e1)
        g[1, x, 8 : 8 + ey, :] = f[1, x, 8 : 8 + ey, :] + (p * e1 + q * e0)

    planes(HALO - halo - 1, HALO + cx + halo + 1, smooth_pass)

    def edge(x):
        a0, a1 = operate_plane(g, diag, absorb, x, 0, ey)
        t_ref[0, x], t_ref[1, x] = a0, a1

    if halo > 0:
        planes(HALO - halo, HALO, edge)
        planes(HALO + cx, HALO + cx + halo, edge)
    y0, y1 = HALO, HALO + cy

    def middle(x, carry):
        g0, g1 = carry
        if halo > 0:
            a0, a1 = operate_plane(g, diag, absorb, x, 0, ey)
            t_ref[0, x], t_ref[1, x] = a0, a1
            a0, a1 = a0[y0:y1], a1[y0:y1]
        else:
            a0, a1 = operate_plane(g, diag, absorb, x, y0, y1)
            t_ref[0, x, y0:y1, :], t_ref[1, x, y0:y1, :] = a0, a1
        u0, u1 = u_at(x, y0, y1)
        s_ref[0, x - HALO] = g[0, x, 8 + y0 : 8 + y1, :]
        s_ref[1, x - HALO] = g[1, x, 8 + y0 : 8 + y1, :]
        index = ends[x - HALO]
        w0 = jnp.take_along_axis(prefix(u0 - a0), index, axis=1, mode="promise_in_bounds")
        w1 = jnp.take_along_axis(prefix(u1 - a1), index, axis=1, mode="promise_in_bounds")
        return g0 + fold8(w0), g1 + fold8(w1)

    zero = jnp.zeros((8, 128), F32)
    return planes(HALO, HALO + cx, middle, (zero, zero))


def start_kernel(grid, own,
                 rhs, wave, layer, agg, ylo, yhi, xlo, xhi, cols,
                 diag, absorb, sre, sim, ids, ends, t_ref, s_ref, out_ref,
                 u, f, g, pad):
    cx, cy = own
    ex, ey = cx + 2 * HALO, cy + 2 * HALO
    zero_pads(f, ey)
    zero_pads(g, ey)

    def fill(x, y0, y1, r0, r1, k, l, a):
        sq = k * k
        depth = l / 3.0
        ab = sq * (pml_strength * depth * depth)
        d = 6.0 - sq
        w = jnp.where(k > 0.0, damping / (d * d + ab * ab), 0.0)
        p, q = d * w, ab * w
        diag[x, y0:y1, :] = d
        absorb[x, y0:y1, :] = ab
        sre[x, y0:y1, :] = p
        sim[x, y0:y1, :] = q
        ids[x, y0:y1, :] = a
        u[0, x, y0:y1, :] = r0
        u[1, x, y0:y1, :] = r1
        f[0, x, 8 + y0 : 8 + y1, :] = p * r0 - q * r1
        f[1, x, 8 + y0 : 8 + y1, :] = p * r1 + q * r0

    def from_buffer(buf, base, y0, y1):
        def go(x):
            i = x - base
            fill(x, y0, y1, buf[0, i], buf[1, i], buf[2, i], buf[3, i], buf[4, i].astype(jnp.int32))
        return go

    planes(0, HALO, from_buffer(xlo, 0, 0, ey))
    planes(HALO + cx, ex, from_buffer(xhi, HALO + cx, 0, ey))
    y0, y1 = HALO, HALO + cy

    def inner(x, acc):
        i = x - HALO
        r0, r1 = rhs[0, i], rhs[1, i]
        from_buffer(ylo, HALO, 0, HALO)(x)
        from_buffer(yhi, HALO, HALO + cy, ey)(x)
        a = agg[i]
        fill(x, y0, y1, r0, r1, wave[i], layer[i].astype(F32), a)
        lane = lanes(a.shape)
        low = jnp.zeros(a.shape, jnp.int32)
        step = a.shape[1] // 2
        while step >= 1:
            probe = low + step
            val = jnp.take_along_axis(a, probe - 1, axis=1, mode="promise_in_bounds")
            low = jnp.where(val <= lane, probe, low)
            step //= 2
        val = jnp.take_along_axis(a, low, axis=1, mode="promise_in_bounds")
        low = jnp.where(val <= lane, low + 1, low)
        ends[i] = jnp.maximum(low - 1, 0)
        return acc + fold8(r0 * r0 + r1 * r1)

    sq = planes(HALO, HALO + cx, inner, jnp.zeros((8, 128), F32))

    def u_at(x, y0, y1):
        return u[0, x, y0:y1, :], u[1, x, y0:y1, :]

    g0, g1 = second_passes(f, g, u_at, (diag, absorb, sre, sim), HALO - 2, own, ends, t_ref, s_ref, ey)
    spread_rhs(g0, g1, cols, pad, out_ref, scalar_row([(40, sq)]), grid)


def step_kernel(j, grid, own, *refs):
    refs = list(refs)
    take_refs = lambda k: [refs.pop(0) for _ in range(k)]
    rcv, diag, absorb, sre, sim, ids, ends, cols, t_in, u_in, s_in = take_refs(11)
    m_old, v_old, z_old, c_old = take_refs(j), take_refs(j), take_refs(j), take_refs(j)
    last = j == ITERS - 1
    m_out = None if last else refs.pop(0)
    v_out, z_out, c_out, h_out = take_refs(4)
    if not last:
        u_out, s_out, t_out = take_refs(3)
    out_ref = refs.pop(0)
    pc = refs.pop(0)
    if not last:
        f, u, pad = take_refs(3)
    cx, cy = own
    ey = cy + 2 * HALO
    halo = HALO - 2 - 2 * j
    y0, y1 = HALO, HALO + cy

    zero_pads(pc, ey)
    if not last:
        zero_pads(f, ey)
    row = jnp.sum(rcv[...], axis=0, keepdims=True)
    scal = row[:, 256:384]
    h_out[...] = scal
    sq = pick(scal, 40)
    hr = [pick(scal, 32 + 2 * i) for i in range(j)]
    hi = [pick(scal, 33 + 2 * i) for i in range(j)]
    for i in range(j):
        sq = sq - (hr[i] * hr[i] + hi[i] * hi[i])
    inv = 1.0 / jnp.sqrt(jnp.maximum(sq, 0.0) + epsilon)
    table = row
    for i in range(j):
        old = c_old[i][...]
        wide = lambda v: jnp.concatenate([v[0:1]] * 3, axis=1)
        table = table - (wide(hr[i]) * old + wide(hi[i]) * turn_rows(old))
    table = table * jnp.concatenate([inv[0:1]] * 3, axis=1)
    c_out[...] = table

    def like(v, rows):
        return jnp.concatenate([v] * (rows // 8), axis=0)

    def combine(new, old, x, rows):
        a0, a1 = new
        for i in range(j):
            b0, b1 = old(i)
            r, q = like(hr[i], rows), like(hi[i], rows)
            a0 = a0 - (r * b0 - q * b1)
            a1 = a1 - (r * b1 + q * b0)
        s = like(inv, rows)
        return a0 * s, a1 * s

    def prolong(dx):
        def go(x):
            for dy, lo, hi_ in ((0, 0, HALO), (1, HALO, HALO + cy), (2, HALO + cy, ey)):
                n = dx * 3 + dy
                src = table[:, 128 * (n // 4) : 128 * (n // 4) + 128]
                index = ids[x, lo:hi_, :] + 32 * (n % 4)
                pc[0, x, 8 + lo : 8 + hi_, :] = take(src, index)
                pc[1, x, 8 + lo : 8 + hi_, :] = take(src, index + AGG)
        return go

    planes(HALO - halo - 1, HALO, prolong(0))
    planes(HALO, HALO + cx, prolong(1))
    planes(HALO + cx, HALO + cx + halo + 1, prolong(2))

    def image_plane(x, lo, hi_):
        a0, a1 = operate_plane(pc, diag, absorb, x, lo, hi_)
        m0, m1 = combine(
            (t_in[0, x, lo:hi_, :], t_in[1, x, lo:hi_, :]),
            lambda i: (m_old[i][0, x, lo:hi_, :], m_old[i][1, x, lo:hi_, :]),
            x, hi_ - lo,
        )
        if not last:
            m_out[0, x, lo:hi_, :], m_out[1, x, lo:hi_, :] = m0, m1
        u0, u1 = m0 + a0, m1 + a1
        if not last:
            p, q = sre[x, lo:hi_, :], sim[x, lo:hi_, :]
            u[0, x, lo:hi_, :], u[1, x, lo:hi_, :] = u0, u1
            f[0, x, 8 + lo : 8 + hi_, :] = p * u0 - q * u1
            f[1, x, 8 + lo : 8 + hi_, :] = p * u1 + q * u0
        return u0, u1

    if halo > 0:
        edge = lambda x: (image_plane(x, 0, ey), None)[1]
        planes(HALO - halo, HALO, edge)
        planes(HALO + cx, HALO + cx + halo, edge)

    def middle(x, acc):
        i = x - HALO
        if halo > 0:
            u0, u1 = image_plane(x, 0, ey)
            u0, u1 = u0[y0:y1], u1[y0:y1]
        else:
            u0, u1 = image_plane(x, y0, y1)
        if not last:
            u_out[0, i], u_out[1, i] = u0, u1
        v0, v1 = combine((u_in[0, i], u_in[1, i]), lambda k: (v_old[k][0, i], v_old[k][1, i]), x, cy)
        v_out[0, i], v_out[1, i] = v0, v1
        z0, z1 = combine((s_in[0, i], s_in[1, i]), lambda k: (z_old[k][0, i], z_old[k][1, i]), x, cy)
        z_out[0, i], z_out[1, i] = z0, z1
        new = []
        for k in range(j + 1):
            b0, b1 = (v0, v1) if k == j else (v_old[k][0, i], v_old[k][1, i])
            new.append(fold8(b0 * u0 + b1 * u1))
            new.append(fold8(b0 * u1 - b1 * u0))
        new.append(fold8(u0 * u0 + u1 * u1))
        return tuple(a + b for a, b in zip(acc, new))

    zero = jnp.zeros((8, 128), F32)
    acc = planes(HALO, HALO + cx, middle, (zero,) * (2 * j + 3))
    items = [(32 + k, acc[k]) for k in range(2 * j + 2)] + [(40, acc[-1])]
    scalars = scalar_row(items)
    if last:
        n = out_ref.shape[0]
        for r in range(2):
            out_ref[:, 128 * r : 128 * r + 128] = jnp.zeros((n, 128), F32)
        out_ref[:, 256:384] = jnp.broadcast_to(scalars, (n, 128))
        return

    def u_at(x, lo, hi_):
        return u[0, x, lo:hi_, :], u[1, x, lo:hi_, :]

    g0, g1 = second_passes(f, pc, u_at, (diag, absorb, sre, sim), halo - 2, own, ends, t_out, s_out, ey)
    spread_rhs(g0, g1, cols, pad, out_ref, scalars, grid)


def cmul(a, b):
    return a[0] * b[0] - a[1] * b[1], a[0] * b[1] + a[1] * b[0]


def finish_kernel(own, *refs):
    rcv, ids = refs[0], refs[1]
    z = refs[2 : 2 + ITERS]
    c = refs[2 + ITERS : 2 + 2 * ITERS]
    rows = refs[2 + 2 * ITERS : 2 + 3 * ITERS]
    sol, hess = refs[2 + 3 * ITERS :]
    cx, cy = own
    final = jnp.sum(rcv[:, 256:384], axis=0, keepdims=True)
    scal = [r[...] for r in rows] + [final]
    beta = jnp.sqrt(pick(scal[0], 40) + epsilon)
    upper = []
    sub = []
    for j in range(ITERS):
        row = scal[j + 1]
        col = [(pick(row, 32 + 2 * i), pick(row, 33 + 2 * i)) for i in range(j + 1)]
        sq = pick(row, 40)
        for a, b in col:
            sq = sq - (a * a + b * b)
        upper.append(col)
        sub.append(jnp.sqrt(jnp.maximum(sq, 0.0) + epsilon))
    r_i = lax.broadcasted_iota(jnp.int32, (8, 128), 0)
    c_i = lanes((8, 128))
    for comp in range(2):
        block = jnp.zeros((8, 128), F32)
        for j in range(ITERS):
            for i in range(j + 1):
                block = jnp.where((r_i == i) & (c_i == j), upper[j][i][comp], block)
            if comp == 0:
                block = jnp.where((r_i == j + 1) & (c_i == j), sub[j], block)
        hess[comp] = block[0 : ITERS + 1, 0:ITERS]
    zero = jnp.zeros((8, 128), F32)
    target = [(beta, zero)]
    rot = []
    tri = []
    for j in range(ITERS):
        col = list(upper[j])
        for i in range(j):
            cr, ci, s = rot[i]
            a, b = col[i], col[i + 1]
            up = cmul((cr, -ci), a)
            dn = cmul((cr, ci), b)
            col[i] = (up[0] + s * b[0], up[1] + s * b[1])
            col[i + 1] = (dn[0] - s * a[0], dn[1] - s * a[1])
        a = col[j]
        big = jnp.sqrt(a[0] * a[0] + a[1] * a[1] + sub[j] * sub[j])
        w = 1.0 / big
        cr, ci, s = a[0] * w, a[1] * w, sub[j] * w
        rot.append((cr, ci, s))
        g = target[j]
        target[j] = cmul((cr, -ci), g)
        target.append((-s * g[0], -s * g[1]))
        col[j] = big
        tri.append(col)
    y = [None] * ITERS
    for j in reversed(range(ITERS)):
        a0, a1 = target[j]
        for k in range(j + 1, ITERS):
            b = cmul(tri[k][j], y[k])
            a0, a1 = a0 - b[0], a1 - b[1]
        w = 1.0 / tri[j][j]
        y[j] = (a0 * w, a1 * w)
    table = jnp.zeros((1, 128), F32)
    for j in range(ITERS):
        old = c[j][:, 128:256]
        table = table + (y[j][0][0:1] * old + y[j][1][0:1] * turn(old))

    def like(v):
        return jnp.concatenate([v] * (cy // 8), axis=0)

    def go(i):
        index = ids[HALO + i, HALO : HALO + cy, :]
        a0, a1 = take(table, index), take(table, index + AGG)
        for j in range(ITERS):
            b = cmul((like(y[j][0]), like(y[j][1])), (z[j][0, i], z[j][1, i]))
            a0, a1 = a0 + b[0], a1 + b[1]
        sol[0, i], sol[1, i] = a0, a1

    planes(0, cx, go)


def shape(*dims, dtype=F32):
    return jax.ShapeDtypeStruct(dims, dtype)


def call(kernel, outs, scratch, args, name, flops=200_000_000):
    vm = pl.BlockSpec(memory_space=pltpu.VMEM)
    return pl.pallas_call(
        kernel,
        out_shape=outs,
        in_specs=[vm] * len(args),
        out_specs=[vm] * len(outs),
        scratch_shapes=scratch,
        compiler_params=pltpu.CompilerParams(vmem_limit_bytes=VLIMIT),
        cost_estimate=pl.CostEstimate(flops=flops, bytes_accessed=1_000_000, transcendentals=0),
        name=name,
    )(*args)


def exchange(x):
    return lax.all_to_all(x, AXES, 0, 0, tiled=True)


def body(right_side, wavenumber, pml_layer, aggregate, coarse_inverse):
    gx, gy = lax.axis_size("gx"), lax.axis_size("gy")
    n = gx * gy
    cx, cy, cz = wavenumber.shape
    own = (cx, cy)
    ex, ey = cx + 2 * HALO, cy + 2 * HALO
    grid = (gx, gy)
    margin = -(-(gy + 1) // 8) * 8

    fields = jnp.concatenate(
        [right_side, wavenumber[None], pml_layer.astype(F32)[None], aggregate.astype(F32)[None]], 0
    )

    def swap(block, axis, dim):
        count = lax.axis_size(axis)
        up = [(i, i + 1) for i in range(count - 1)]
        down = [(b, a) for a, b in up]
        size = block.shape[dim]
        low = lax.ppermute(lax.slice_in_dim(block, size - HALO, size, axis=dim), axis, up)
        high = lax.ppermute(lax.slice_in_dim(block, 0, HALO, axis=dim), axis, down)
        return low, high

    ylo, yhi = swap(fields, "gy", 2)
    inverse = coarse_inverse.reshape(2, AGG, n, AGG).transpose(2, 3, 0, 1).reshape(n, 2 * AGG * AGG)
    cols = exchange(inverse)
    edges = jnp.concatenate([ylo, fields, yhi], axis=2)
    xlo, xhi = swap(edges, "gx", 1)

    ext = shape(ex, ey, cz)
    ext2 = shape(2, ex, ey, cz)
    mine = shape(2, cx, cy, cz)
    chunk = shape(n, 384)
    tab = shape(1, 384)
    padded = pltpu.VMEM((2, ex, ey + 16, cz), F32)
    wide = pltpu.VMEM((2, ex, ey, cz), F32)
    pad = pltpu.VMEM((n + 2 * margin, 128), F32)

    diag, absorb, sre, sim, ids, ends, t, s, send = call(
        functools.partial(start_kernel, grid, own),
        [ext, ext, ext, ext, shape(ex, ey, cz, dtype=jnp.int32), shape(cx, cy, cz, dtype=jnp.int32), ext2, mine, chunk],
        [wide, padded, padded, pad],
        [right_side, wavenumber, pml_layer, aggregate, ylo, yhi, xlo, xhi, cols],
        "start",
    )
    u = right_side
    ms, vs, zs, cs, hs = [], [], [], [], []
    for j in range(ITERS):
        got = exchange(send)
        last = j == ITERS - 1
        args = [got, diag, absorb, sre, sim, ids, ends, cols, t, u, s] + ms + vs + zs + cs
        outs = ([] if last else [ext2]) + [mine, mine, tab, shape(1, 128)]
        scratch = [padded]
        if not last:
            outs += [mine, mine, ext2]
            scratch += [padded, wide, pad]
        outs += [chunk]
        res = list(call(functools.partial(step_kernel, j, grid, own), outs, scratch, args, f"step{j}"))
        if not last:
            ms.append(res.pop(0))
        vs.append(res.pop(0))
        zs.append(res.pop(0))
        cs.append(res.pop(0))
        hs.append(res.pop(0))
        if not last:
            u, s, t = res.pop(0), res.pop(0), res.pop(0)
        send = res.pop(0)
    got = exchange(send)
    sol, hess = call(
        functools.partial(finish_kernel, own),
        [mine, shape(2, ITERS + 1, ITERS)],
        [],
        [got, ids] + zs + cs + hs,
        "finish",
    )
    return sol, hess


def solution(mesh):
    return jax.shard_map(
        body,
        mesh=mesh,
        in_specs=(
            P(None, "gx", "gy", None),
            P("gx", "gy", None),
            P("gx", "gy", None),
            P("gx", "gy", None),
            P(None, ("gx", "gy"), None),
        ),
        out_specs=(P(None, "gx", "gy", None), P()),
        check_vma=False,
    )
```

```python
import functools

import jax
import jax.numpy as jnp
from jax import lax
from jax.experimental import pallas as pl
from jax.experimental.pallas import tpu as pltpu
from jax.sharding import PartitionSpec as P


ITERS = 4
HALO = 2 * ITERS
NEAR = 2
AXES = ("gx", "gy")
AGG = 16
damping = 0.8
pml_strength = 3.0
epsilon = 1e-06
F32 = jnp.float32
VLIMIT = 16 * 1024 * 1024


def lanes(shape):
    return lax.broadcasted_iota(jnp.int32, shape, len(shape) - 1)


def turn(x):
    odd = (lanes(x.shape) // AGG) % 2 == 1
    return jnp.where(odd, pltpu.roll(x, AGG, 1), -pltpu.roll(x, x.shape[1] - AGG, 1))


def turn_rows(x):
    parts = [turn(x[:, i : i + 128]) for i in range(0, x.shape[1], 128)]
    return jnp.concatenate(parts, axis=1)


def pick(row, lane):
    return jnp.broadcast_to(row[:, lane : lane + 1], (8, 128))


def take(table, index):
    rows = index.shape[0]
    src = jnp.broadcast_to(table, (rows, 128))
    return jnp.take_along_axis(src, index, axis=1, mode="promise_in_bounds")


def planes(lo, hi, fn, carry=None, width=8):
    count = hi - lo
    step = max(d for d in range(1, count + 1) if count % d == 0 and d <= width + width // 2)
    if step * 2 < width and count > width:
        step = width
    whole = count // step * step

    def go(i, c):
        for k in range(step):
            x = lo + i * step + k
            if carry is None:
                fn(x)
            else:
                c = fn(x, c)
        return c

    c = 0 if carry is None else carry
    if whole // step == 1:
        c = go(0, c)
    else:
        c = lax.fori_loop(0, whole // step, go, c)
    for x in range(lo + whole, hi):
        if carry is None:
            fn(x)
        else:
            c = fn(x, c)
    return c


def stencil(ref, c, x, y0, y1):
    mid = ref[c, x, 8 + y0 : 8 + y1, :]
    total = (
        ref[c, x - 1, 8 + y0 : 8 + y1, :]
        + ref[c, x + 1, 8 + y0 : 8 + y1, :]
        + ref[c, x, 7 + y0 : 7 + y1, :]
        + ref[c, x, 9 + y0 : 9 + y1, :]
    )
    lane = lanes(mid.shape)
    last = mid.shape[-1] - 1
    total = total + jnp.where(lane == 0, 0.0, pltpu.roll(mid, 1, 1))
    total = total + jnp.where(lane == last, 0.0, pltpu.roll(mid, last, 1))
    return mid, total


def operate_plane(ref, k, coefs, y0, y1):
    refs, i = coefs
    d = refs[0][i, y0:y1, :]
    a = refs[1][i, y0:y1, :]
    m0, t0 = stencil(ref, 0, k, y0, y1)
    m1, t1 = stencil(ref, 1, k, y0, y1)
    return d * m0 - t0 + a * m1, d * m1 - t1 - a * m0


def fold8(x):
    out = x[0:8]
    for i in range(8, x.shape[0], 8):
        out = out + x[i : i + 8]
    return out


def keep_split(ref, c, i, x):
    top = x.astype(jnp.bfloat16)
    ref[c, i, :, 0:128] = top
    ref[c, i, :, 128:256] = (x - top.astype(F32)).astype(jnp.bfloat16)


def restrict(split, ends, own):
    cx, cy = own
    r = lax.broadcasted_iota(jnp.int32, (256, 128), 0) % 128
    ones = jnp.where(r <= lanes((256, 128)), 1.0, 0.0).astype(jnp.bfloat16)
    per = 4
    out = []
    for c in range(2):
        acc = jnp.zeros((8, 128), F32)
        for i in range(0, cx, per):
            block = split[c, i : i + per].reshape(cy * per, 256)
            sums = jnp.dot(block, ones, preferred_element_type=F32)
            for k in range(per):
                part = sums[cy * k : cy * (k + 1)]
                acc = acc + fold8(jnp.take_along_axis(part, ends[i + k], axis=1, mode="promise_in_bounds"))
        out.append(acc)
    return out


def spread_rhs(g0, g1, cols_ref, pad_ref, out_ref, scalars, grid):
    gx, gy = grid
    n = gx * gy
    lane = lanes((1, 128))
    rows = []
    for g in (g0, g1):
        total = jnp.sum(g, axis=0, keepdims=True)
        rows.append(jnp.where(lane == 0, total, total - pltpu.roll(total, 1, 1)))
    z = []
    for row in rows:
        acc = None
        for q in range(4):
            weight = take(row, lanes((8, 128)) // 32 + 4 * q)[0:1]
            term = cols_ref[pl.ds(q, n, stride=4), :] * weight
            acc = term if acc is None else acc + term
        acc = acc + pltpu.roll(acc, 64, 1)
        z.append(acc + pltpu.roll(acc, 32, 1))
    whole = z[0] + turn(z[1])
    margin = (pad_ref.shape[0] - n) // 2
    pad_ref[0:margin, :] = jnp.zeros((margin, 128), F32)
    pad_ref[margin + n : 2 * margin + n, :] = jnp.zeros((margin, 128), F32)
    pad_ref[margin : margin + n, :] = whole
    place = lax.broadcasted_iota(jnp.int32, (n, 128), 0) % gy
    group = lanes((n, 128)) // 32
    outs = [jnp.zeros((n, 128), F32) for _ in range(3)]
    for dx in (-1, 0, 1):
        for dy in (-1, 0, 1):
            k = (dx + 1) * 3 + dy + 1
            start = margin + dx * gy + dy
            piece = pad_ref[start : start + n, :]
            ok = (group == k % 4) & (place + dy >= 0) & (place + dy < gy)
            outs[k // 4] = jnp.where(ok, piece, outs[k // 4])
    outs[2] = outs[2] + jnp.broadcast_to(scalars, (n, 128))
    for r in range(3):
        out_ref[:, 128 * r : 128 * (r + 1)] = outs[r]


def scalar_row(items):
    lane = lanes((1, 128))
    row = jnp.zeros((1, 128), F32)
    for where, acc in items:
        s = jnp.sum(jnp.sum(acc, axis=0, keepdims=True), axis=1, keepdims=True)
        row = jnp.where(lane == where, jnp.broadcast_to(s, (1, 128)), row)
    return row


def smooth_plane(f, g, u, k, coefs, y0, y1):
    a0, a1 = operate_plane(f, k, coefs, y0, y1)
    e0, e1 = u[0, k, y0:y1, :] - a0, u[1, k, y0:y1, :] - a1
    refs, i = coefs
    p, q = refs[2][i, y0:y1, :], refs[3][i, y0:y1, :]
    g[0, k, 8 + y0 : 8 + y1, :] = f[0, k, 8 + y0 : 8 + y1, :] + (p * e0 - q * e1)
    g[1, k, 8 + y0 : 8 + y1, :] = f[1, k, 8 + y0 : 8 + y1, :] + (p * e1 + q * e0)


def pairs(lo, hi, size, fn, low, high):
    if hi > lo:
        def go(x):
            fn(x, low(x))
            y = size - 1 - x
            fn(y, high(y))

        planes(lo, hi, go, width=4)


def centre(f, g, u, t, t_rim, places, halo, s, edge, split, ends, own, rows, t_rows):
    mine, low, high = places
    cx, cy = own
    size = cx + 2 * HALO
    y0, y1 = HALO, HALO + cy
    r0, r1 = t_rows
    pairs(HALO - halo + 1, HALO, size, lambda k, c: smooth_plane(f, g, u, k, c, *rows), low, high)
    planes(HALO, HALO + cx, lambda x: smooth_plane(f, g, u, x, mine(x), *rows))

    def outer(k, c):
        a0, a1 = operate_plane(g, k, c, r0, r1)
        t_rim[0, c[1], r0:r1, :], t_rim[1, c[1], r0:r1, :] = a0, a1

    pairs(HALO - halo + 2, HALO, size, outer, low, high)

    def middle(x):
        i = x - HALO
        a0, a1 = operate_plane(g, x, mine(x), r0, r1)
        t[0, i, r0:r1, :], t[1, i, r0:r1, :] = a0, a1
        lo = y0 - r0
        s[0, i] = g[0, x, 8 + y0 : 8 + y1, :]
        s[1, i] = g[1, x, 8 + y0 : 8 + y1, :]
        keep_split(split, 0, i, u[0, x, y0:y1, :] - a0[lo : lo + cy])
        keep_split(split, 1, i, u[1, x, y0:y1, :] - a1[lo : lo + cy])

    planes(HALO, HALO + cx, middle)
    if edge is not None:
        for c in range(2):
            for k, x in enumerate((HALO, HALO + cx - 1)):
                edge[0, c, k] = f[c, x]
                edge[1, c, k] = g[c, x]
    return restrict(split, ends, own)


def rim_pair(lo, hi, fn):
    if hi > lo:
        def go(x):
            fn(x, x)
            y = lo + hi - 1 - x
            fn(2 * HALO + 1 - y, 2 * HALO - 1 - y)

        planes(lo, hi, go, width=4)


def fringe(f, g, u, t, rim, edge, halo, rows):
    for c in range(2):
        for k, x in enumerate((HALO, HALO + 1)):
            f[c, x] = edge[0, c, k]
            g[c, x] = edge[1, c, k]
    rim_pair(HALO - halo + 1, HALO, lambda k, i: smooth_plane(f, g, u, k, (rim, i), *rows))
    y0, y1 = rows

    def last(k, i):
        a0, a1 = operate_plane(g, k, (rim, i), y0, y1)
        t[0, i, y0:y1, :], t[1, i, y0:y1, :] = a0, a1

    rim_pair(HALO - halo + 2, HALO, last)


def fill(store, u, f, k, y0, y1, r0, r1, wave, layer, a):
    sq = wave * wave
    depth = layer / 3.0
    ab = sq * (pml_strength * depth * depth)
    d = 6.0 - sq
    w = jnp.where(wave > 0.0, damping / (d * d + ab * ab), 0.0)
    p, q = d * w, ab * w
    refs, i = store
    refs[0][i, y0:y1, :] = d
    refs[1][i, y0:y1, :] = ab
    refs[2][i, y0:y1, :] = p
    refs[3][i, y0:y1, :] = q
    refs[4][i, y0:y1, :] = a
    u[0, k, y0:y1, :] = r0
    u[1, k, y0:y1, :] = r1
    f[0, k, 8 + y0 : 8 + y1, :] = p * r0 - q * r1
    f[1, k, 8 + y0 : 8 + y1, :] = p * r1 + q * r0


def fill_from(store, u, f, k, buf, b, y0, y1):
    fill(store, u, f, k, y0, y1, buf[0, b], buf[1, b], buf[2, b], buf[3, b], buf[4, b].astype(jnp.int32))


def start_kernel(grid, own,
                 rhs, wave, layer, agg, ylo, yhi, xlo, xhi, cols,
                 diag, absorb, sre, sim, ids, ends, t, s, edge, out_ref,
                 n0, n1, n2, n3, n4, u, f, g, split, pad):
    cx, cy = own
    ey = cy + 2 * HALO
    refs, near = (diag, absorb, sre, sim, ids), (n0, n1, n2, n3, n4)
    mine = lambda x: (refs, x - HALO)
    low = lambda x: (near, x - HALO + NEAR)
    high = lambda x: (near, x - HALO - cx + NEAR)
    for i in range(NEAR):
        x = HALO - NEAR + i
        fill_from(low(x), u, f, x, xlo, i, 0, ey)
        x = HALO + cx + i
        fill_from(high(x), u, f, x, xhi, i, 0, ey)

    def inner(x, acc):
        i = x - HALO
        r0, r1 = rhs[0, i], rhs[1, i]
        fill_from(mine(x), u, f, x, ylo, i, 0, HALO)
        fill_from(mine(x), u, f, x, yhi, i, HALO + cy, ey)
        fill(mine(x), u, f, x, HALO, HALO + cy, r0, r1, wave[i], layer[i].astype(F32), agg[i])
        return acc + fold8(r0 * r0 + r1 * r1)

    sq = planes(HALO, HALO + cx, inner, jnp.zeros((8, 128), F32))

    def find(i):
        a = agg[i]
        lane = lanes(a.shape)
        low = jnp.zeros(a.shape, jnp.int32)
        step = a.shape[1] // 2
        while step >= 1:
            probe = low + step
            val = jnp.take_along_axis(a, probe - 1, axis=1, mode="promise_in_bounds")
            low = jnp.where(val <= lane, probe, low)
            step //= 2
        val = jnp.take_along_axis(a, low, axis=1, mode="promise_in_bounds")
        low = jnp.where(val <= lane, low + 1, low)
        ends[i] = jnp.maximum(low - 1, 0)

    planes(0, cx, find)
    g0, g1 = centre(f, g, u, t, None, (mine, low, high), 2, s, edge, split, ends, own, (0, ey), (0, ey))
    spread_rhs(g0, g1, cols, pad, out_ref, scalar_row([(40, sq)]), grid)


def start_fringe_kernel(own, got, xlo, xhi, wlo, whi, edge,
                        diag, absorb, sre, sim, ids, t, u, f, g):
    _, cy = own
    ey = cy + 2 * HALO
    rim = (diag, absorb, sre, sim, ids)
    far = HALO - NEAR

    def go(i):
        fill_from((rim, i), u, f, i, wlo, i, 0, ey)
        fill_from((rim, HALO + NEAR + i), u, f, HALO + 2 + NEAR + i, whi, i, 0, ey)

    planes(0, far, go, width=4)
    for i in range(NEAR):
        fill_from((rim, far + i), u, f, far + i, xlo, i, 0, ey)
        fill_from((rim, HALO + i), u, f, HALO + 2 + i, xhi, i, 0, ey)
    fringe(f, g, u, t, rim, edge, HALO, (0, ey))


def read_scalars(scal, j):
    hr = [pick(scal, 32 + 2 * i) for i in range(j)]
    hi = [pick(scal, 33 + 2 * i) for i in range(j)]
    sq = pick(scal, 40)
    for i in range(j):
        sq = sq - (hr[i] * hr[i] + hi[i] * hi[i])
    return hr, hi, 1.0 / jnp.sqrt(jnp.maximum(sq, 0.0) + epsilon)


def like(v, rows):
    return jnp.concatenate([v] * (rows // 8), axis=0)


def combine(scalars, new, old):
    hr, hi, inv = scalars
    a0, a1 = new
    rows = a0.shape[0]
    for i in range(len(hr)):
        b0, b1 = old(i)
        r, q = like(hr[i], rows), like(hi[i], rows)
        a0 = a0 - (r * b0 - q * b1)
        a1 = a1 - (r * b1 + q * b0)
    s = like(inv, rows)
    return a0 * s, a1 * s


def prolong_plane(pc, k, ids, i, table, own, dx):
    cy = own[1]
    ey = cy + 2 * HALO
    for dy, lo, hi in ((0, 0, HALO), (1, HALO, HALO + cy), (2, HALO + cy, ey)):
        n = dx * 3 + dy
        src = table[:, 128 * (n // 4) : 128 * (n // 4) + 128]
        index = ids[i, lo:hi, :] + 32 * (n % 4)
        pc[0, k, 8 + lo : 8 + hi, :] = take(src, index)
        pc[1, k, 8 + lo : 8 + hi, :] = take(src, index + AGG)


def image_plane(pc, k, coefs, t_in, m_old, scalars, lo, hi):
    i = coefs[1]
    a0, a1 = operate_plane(pc, k, coefs, lo, hi)
    m = combine(
        scalars,
        (t_in[0, i, lo:hi, :], t_in[1, i, lo:hi, :]),
        lambda n: (m_old[n][0, i, lo:hi, :], m_old[n][1, i, lo:hi, :]),
    )
    return m, (m[0] + a0, m[1] + a1)


def image_store(pc, u, f, k, coefs, t_in, m_old, scalars, m_out, lo, hi):
    m, (u0, u1) = image_plane(pc, k, coefs, t_in, m_old, scalars, lo, hi)
    refs, i = coefs
    if m_out is not None:
        m_out[0, i, lo:hi, :], m_out[1, i, lo:hi, :] = m
    p, q = refs[2][i, lo:hi, :], refs[3][i, lo:hi, :]
    u[0, k, lo:hi, :], u[1, k, lo:hi, :] = u0, u1
    f[0, k, 8 + lo : 8 + hi, :] = p * u0 - q * u1
    f[1, k, 8 + lo : 8 + hi, :] = p * u1 + q * u0
    return u0, u1


def y_rows(j, cy):
    halo = HALO - 2 - 2 * j
    if halo > 4:
        return 0, cy + 2 * HALO
    if halo > 0:
        return HALO - 4, HALO + cy + 4
    return HALO, HALO + cy


def step_kernel(j, grid, own, *refs):
    refs = list(refs)
    take_refs = lambda k: [refs.pop(0) for _ in range(k)]
    last = j == ITERS - 1
    rcv = refs.pop(0)
    home, rim = take_refs(5), take_refs(5)
    ends, cols, t_own, t_rim, u_in = take_refs(5)
    m_own, m_rim = take_refs(j), take_refs(0 if last else j)
    v_old, c_old = take_refs(j), take_refs(j)
    v_out, c_out, h_out, out_ref = take_refs(4)
    if not last:
        m_out, t, u_out, s_out = take_refs(4)
    mr_out = tr_out = None
    if j < ITERS - 2:
        mr_out, tr_out = take_refs(2)
    pc = refs.pop(0)
    if not last:
        u, f, split, pad = take_refs(4)
    cx, cy = own
    mine = lambda x: (home, x - HALO)
    low = lambda x: (rim, x)
    high = lambda x: (rim, x - cx)
    y0, y1 = HALO, HALO + cy
    rows = y_rows(j, cy)
    halo = HALO - 2 - 2 * j
    size = cx + 2 * HALO

    row = jnp.sum(rcv[...], axis=0, keepdims=True)
    scal = row[:, 256:384]
    h_out[...] = scal
    scalars = read_scalars(scal, j)
    hr, hi, inv = scalars
    wide = lambda v: jnp.concatenate([v[0:1]] * 3, axis=1)
    table = row
    for i in range(j):
        old = c_old[i][...]
        table = table - (wide(hr[i]) * old + wide(hi[i]) * turn_rows(old))
    table = table * wide(inv)
    c_out[...] = table

    def outside(x):
        prolong_plane(pc, x, rim[4], x, table, own, 0)
        y = 2 * HALO - 1 - x
        prolong_plane(pc, y + cx, rim[4], y, table, own, 2)

    planes(HALO - halo - 1, HALO, outside, width=4)
    planes(HALO, HALO + cx, lambda x: prolong_plane(pc, x, home[4], x - HALO, table, own, 1))

    def outer(k, c):
        image_store(pc, u, f, k, c, t_rim, m_rim, scalars, mr_out, *rows)

    pairs(HALO - halo, HALO, size, outer, low, high)

    def middle(x, acc):
        i = x - HALO
        if last:
            u0, u1 = image_plane(pc, x, mine(x), t_own, m_own, scalars, y0, y1)[1]
        else:
            u0, u1 = image_store(pc, u, f, x, mine(x), t_own, m_own, scalars, m_out, *rows)
            lo = y0 - rows[0]
            u0, u1 = u0[lo : lo + cy], u1[lo : lo + cy]
            u_out[0, i], u_out[1, i] = u0, u1
        v0, v1 = combine(scalars, (u_in[0, i], u_in[1, i]), lambda k: (v_old[k][0, i], v_old[k][1, i]))
        v_out[0, i], v_out[1, i] = v0, v1
        new = []
        for k in range(j + 1):
            b0, b1 = (v0, v1) if k == j else (v_old[k][0, i], v_old[k][1, i])
            new.append(fold8(b0 * u0 + b1 * u1))
            new.append(fold8(b0 * u1 - b1 * u0))
        new.append(fold8(u0 * u0 + u1 * u1))
        return tuple(a + b for a, b in zip(acc, new))

    zero = jnp.zeros((8, 128), F32)
    acc = planes(HALO, HALO + cx, middle, (zero,) * (2 * j + 3))
    items = [(32 + k, acc[k]) for k in range(2 * j + 2)] + [(40, acc[-1])]
    dots = scalar_row(items)
    if last:
        n = out_ref.shape[0]
        for r in range(2):
            out_ref[:, 128 * r : 128 * r + 128] = jnp.zeros((n, 128), F32)
        out_ref[:, 256:384] = jnp.broadcast_to(dots, (n, 128))
        return
    t_rows = rows if j < ITERS - 2 else (y0, y1)
    g0, g1 = centre(f, pc, u, t, tr_out, (mine, low, high), halo, s_out, None, split, ends, own, rows, t_rows)
    spread_rhs(g0, g1, cols, pad, out_ref, dots, grid)


def pack_kernel(rhs, wave, layer, agg, low, high, ints, sems):
    cy = wave.shape[1]
    copies = []
    for k, (out, y) in enumerate(((low, 0), (high, cy - HALO))):
        rows = pl.ds(y, HALO)
        for i, (src, dst) in enumerate((
            (rhs.at[:, :, rows, :], out.at[0:2]),
            (wave.at[:, rows, :], out.at[2]),
            (layer.at[:, rows, :], ints.at[2 * k]),
            (agg.at[:, rows, :], ints.at[2 * k + 1]),
        )):
            copies.append(pltpu.make_async_copy(src, dst, sems.at[4 * k + i]))
    for copy in copies:
        copy.start()
    for copy in copies:
        copy.wait()
    for k, out in enumerate((low, high)):
        out[3] = ints[2 * k].astype(F32)
        out[4] = ints[2 * k + 1].astype(F32)


def slab_kernel(rhs, wave, layer, agg, ylo, yhi, near_low, near_high, far_low, far_high):
    cx, cy = wave.shape[:2]
    y0, y1 = HALO, HALO + cy
    for out, lo, hi in (
        (near_low, 0, NEAR), (near_high, cx - NEAR, cx), (far_low, NEAR, HALO), (far_high, cx - HALO, cx - NEAR),
    ):
        out[:, :, 0:y0, :] = ylo[:, lo:hi]
        out[:, :, y1 : y1 + HALO, :] = yhi[:, lo:hi]
        out[0:2, :, y0:y1, :] = rhs[:, lo:hi]
        out[2, :, y0:y1, :] = wave[lo:hi]
        out[3, :, y0:y1, :] = layer[lo:hi].astype(F32)
        out[4, :, y0:y1, :] = agg[lo:hi].astype(F32)


def columns_kernel(inverse, out, turned):
    turned[:, 0:32] = inverse[...].T
    group = lanes(out.shape) // 32
    total = jnp.zeros(out.shape, F32)
    for r in range(4):
        part = turned[pl.ds(r, out.shape[0], stride=4), :]
        part = jnp.where(group == 0, part, 0.0)
        total = total + (part if r == 0 else pltpu.roll(part, 32 * r, 1))
    out[...] = total


def cmul(a, b):
    return a[0] * b[0] - a[1] * b[1], a[0] * b[1] + a[1] * b[0]


def finish_kernel(own, *refs):
    rcv, ids = refs[0], refs[1]
    z = refs[2 : 2 + ITERS]
    c = refs[2 + ITERS : 2 + 2 * ITERS]
    rows = refs[2 + 2 * ITERS : 2 + 3 * ITERS]
    sol, hess = refs[2 + 3 * ITERS :]
    cx, cy = own
    final = jnp.sum(rcv[:, 256:384], axis=0, keepdims=True)
    scal = [r[...] for r in rows] + [final]
    beta = jnp.sqrt(pick(scal[0], 40) + epsilon)
    upper = []
    sub = []
    for j in range(ITERS):
        row = scal[j + 1]
        col = [(pick(row, 32 + 2 * i), pick(row, 33 + 2 * i)) for i in range(j + 1)]
        sq = pick(row, 40)
        for a, b in col:
            sq = sq - (a * a + b * b)
        upper.append(col)
        sub.append(jnp.sqrt(jnp.maximum(sq, 0.0) + epsilon))
    r_i = lax.broadcasted_iota(jnp.int32, (8, 128), 0)
    c_i = lanes((8, 128))
    for comp in range(2):
        block = jnp.zeros((8, 128), F32)
        for j in range(ITERS):
            for i in range(j + 1):
                block = jnp.where((r_i == i) & (c_i == j), upper[j][i][comp], block)
            if comp == 0:
                block = jnp.where((r_i == j + 1) & (c_i == j), sub[j], block)
        hess[comp] = block[0 : ITERS + 1, 0:ITERS]
    zero = jnp.zeros((8, 128), F32)
    target = [(beta, zero)]
    rot = []
    tri = []
    for j in range(ITERS):
        col = list(upper[j])
        for i in range(j):
            cr, ci, s = rot[i]
            a, b = col[i], col[i + 1]
            up = cmul((cr, -ci), a)
            dn = cmul((cr, ci), b)
            col[i] = (up[0] + s * b[0], up[1] + s * b[1])
            col[i + 1] = (dn[0] - s * a[0], dn[1] - s * a[1])
        a = col[j]
        big = jnp.sqrt(a[0] * a[0] + a[1] * a[1] + sub[j] * sub[j])
        w = 1.0 / big
        cr, ci, s = a[0] * w, a[1] * w, sub[j] * w
        rot.append((cr, ci, s))
        g = target[j]
        target[j] = cmul((cr, -ci), g)
        target.append((-s * g[0], -s * g[1]))
        col[j] = big
        tri.append(col)
    y = [None] * ITERS
    for j in reversed(range(ITERS)):
        a0, a1 = target[j]
        for k in range(j + 1, ITERS):
            b = cmul(tri[k][j], y[k])
            a0, a1 = a0 - b[0], a1 - b[1]
        w = 1.0 / tri[j][j]
        y[j] = (a0 * w, a1 * w)
    table = jnp.zeros((1, 128), F32)
    for j in range(ITERS):
        old = c[j][:, 128:256]
        table = table + (y[j][0][0:1] * old + y[j][1][0:1] * turn(old))

    gamma = list(y)
    for j in reversed(range(ITERS)):
        w = 1.0 / (sub[j - 1] if j > 0 else beta)
        gamma[j] = (gamma[j][0] * w, gamma[j][1] * w)
        for i in range(j):
            b = cmul(upper[j - 1][i], gamma[j])
            gamma[i] = (gamma[i][0] - b[0], gamma[i][1] - b[1])

    def go(i):
        index = ids[i, HALO : HALO + cy, :]
        a0, a1 = take(table, index), take(table, index + AGG)
        for j in range(ITERS):
            b = cmul((like(gamma[j][0], cy), like(gamma[j][1], cy)), (z[j][0, i], z[j][1, i]))
            a0, a1 = a0 + b[0], a1 + b[1]
        sol[0, i], sol[1, i] = a0, a1

    planes(0, cx, go)


def shape(*dims, dtype=F32):
    return jax.ShapeDtypeStruct(dims, dtype)


def call(kernel, outs, scratch, args, flops=100_000_000, space=pltpu.VMEM):
    vm = pl.BlockSpec(memory_space=pltpu.VMEM)
    return pl.pallas_call(
        kernel,
        out_shape=outs,
        in_specs=[pl.BlockSpec(memory_space=space)] * len(args),
        out_specs=[vm] * len(outs),
        scratch_shapes=scratch,
        compiler_params=pltpu.CompilerParams(vmem_limit_bytes=VLIMIT),
        cost_estimate=pl.CostEstimate(flops=flops, bytes_accessed=1_000_000, transcendentals=0),
    )(*args)


def exchange(x):
    return lax.all_to_all(x, AXES, 0, 0, tiled=True)


def program(right_side, wavenumber, pml_layer, aggregate, coarse_inverse):
    gx, gy = lax.axis_size("gx"), lax.axis_size("gy")
    n = gx * gy
    cx, cy, cz = wavenumber.shape
    own = (cx, cy)
    ex, ey = cx + 2 * HALO, cy + 2 * HALO
    grid = (gx, gy)
    margin = -(-(gy + 1) // 8) * 8

    def swap(low, high, axis):
        count = lax.axis_size(axis)
        up = [(i, i + 1) for i in range(count - 1)]
        down = [(b, a) for a, b in up]
        low_in = lax.ppermute(high, axis, up)
        high_in = lax.ppermute(low, axis, down)
        return low_in, high_in

    strip = shape(5, cx, HALO, cz)
    low, high = call(
        pack_kernel, [strip, strip],
        [pltpu.VMEM((4, cx, HALO, cz), jnp.int32), pltpu.SemaphoreType.DMA((8,))],
        [pltpu.with_memory_space_constraint(x, pltpu.HBM) for x in (right_side, wavenumber, pml_layer, aggregate)],
        space=pltpu.HBM,
    )
    ylo, yhi = swap(low, high, "gy")
    (inverse,) = call(
        columns_kernel, [shape(4 * n, 128)], [pltpu.VMEM((AGG * n, 128), F32)],
        [coarse_inverse.reshape(2 * AGG, AGG * n)],
    )
    cols = exchange(inverse)
    right_side, wavenumber, pml_layer, aggregate, ylo, yhi, cols = lax.optimization_barrier(
        (right_side, wavenumber, pml_layer, aggregate, ylo, yhi, cols)
    )
    near, far = shape(5, NEAR, ey, cz), shape(5, HALO - NEAR, ey, cz)
    near_low, near_high, far_low, far_high = call(
        slab_kernel, [near, near, far, far], [],
        [right_side, wavenumber, pml_layer, aggregate, ylo, yhi],
    )
    xlo, xhi = swap(near_low, near_high, "gx")
    wlo, whi = swap(far_low, far_high, "gx")

    I32 = jnp.int32
    home = [shape(cx, ey, cz)] * 4 + [shape(cx, ey, cz, dtype=I32)]
    rim = [shape(2 * HALO, ey, cz)] * 4 + [shape(2 * HALO, ey, cz, dtype=I32)]
    home2, rim2 = shape(2, cx, ey, cz), shape(2, 2 * HALO, ey, cz)
    mine = shape(2, cx, cy, cz)
    chunk = shape(n, 384)
    edges = shape(2, 2, 2, ey + 16, cz)
    vmem = lambda *dims, dtype=F32: pltpu.VMEM(dims, dtype)
    tall = vmem(2, ex, ey + 16, cz)
    flat = vmem(2, ex, ey, cz)
    short_tall = vmem(2, 2 * HALO + 2, ey + 16, cz)
    short_flat = vmem(2, 2 * HALO + 2, ey, cz)
    pad = vmem(n + 2 * margin, 128)
    split = vmem(2, cx, cy, 256, dtype=jnp.bfloat16)
    near = [vmem(2 * NEAR, ey, cz)] * 4 + [vmem(2 * NEAR, ey, cz, dtype=I32)]

    *own_coefs, ends, t_own, s, edge, send = call(
        functools.partial(start_kernel, grid, own),
        home + [shape(cx, cy, cz, dtype=I32), home2, mine, edges, chunk],
        near + [flat, tall, tall, split, pad],
        [right_side, wavenumber, pml_layer, aggregate, ylo, yhi, xlo, xhi, cols],
    )
    got = exchange(send)
    *rim_coefs, t_rim = call(
        functools.partial(start_fringe_kernel, own),
        rim + [rim2],
        [short_flat, short_tall, short_tall],
        [got, xlo, xhi, wlo, whi, edge],
    )
    u = right_side
    ms, mrs, vs, ss, cs, hs = [], [], [], [s], [], []
    for j in range(ITERS):
        last = j == ITERS - 1
        args = [got] + own_coefs + rim_coefs + [ends, cols, t_own, t_rim, u] + ms + ([] if last else mrs) + vs + cs
        outs = [mine, shape(1, 384), shape(1, 128), chunk]
        scratch = [tall]
        if not last:
            outs += [home2, home2, mine, mine]
            if j < ITERS - 2:
                outs += [rim2, rim2]
            scratch += [flat, tall, split, pad]
        v, c, h, send, *rest = call(functools.partial(step_kernel, j, grid, own), outs, scratch, args)
        got = exchange(send)
        if not last:
            m, t_own, u, s = rest[:4]
            ms.append(m)
            ss.append(s)
            if j < ITERS - 2:
                mrs.append(rest[4])
                t_rim = rest[5]
        vs.append(v)
        cs.append(c)
        hs.append(h)
    sol, hess = call(
        functools.partial(finish_kernel, own),
        [mine, shape(2, ITERS + 1, ITERS)],
        [],
        [got, own_coefs[4]] + ss + cs + hs,
    )
    return sol, hess


def solution(mesh):
    return jax.shard_map(
        program,
        mesh=mesh,
        in_specs=(
            P(None, "gx", "gy", None),
            P("gx", "gy", None),
            P("gx", "gy", None),
            P("gx", "gy", None),
            P(None, ("gx", "gy"), None),
        ),
        out_specs=(P(None, "gx", "gy", None), P()),
        check_vma=False,
    )
```

```python
import functools

import jax
import jax.numpy as jnp
from jax import lax
from jax.experimental import pallas as pl
from jax.experimental.pallas import tpu as pltpu
from jax.sharding import PartitionSpec as P


ITERS = 4
HALO = 2 * ITERS
AXES = ("gx", "gy")
AGG = 16
damping = 0.8
pml_strength = 3.0
epsilon = 1e-06
F32 = jnp.float32
VLIMIT = 16 * 1024 * 1024


def lanes(shape):
    return lax.broadcasted_iota(jnp.int32, shape, len(shape) - 1)


def turn(x):
    odd = (lanes(x.shape) // AGG) % 2 == 1
    return jnp.where(odd, pltpu.roll(x, AGG, 1), -pltpu.roll(x, x.shape[1] - AGG, 1))


def turn_rows(x):
    parts = [turn(x[:, i : i + 128]) for i in range(0, x.shape[1], 128)]
    return jnp.concatenate(parts, axis=1)


def pick(row, lane):
    return jnp.broadcast_to(row[:, lane : lane + 1], (8, 128))


def take(table, index):
    rows = index.shape[0]
    src = jnp.broadcast_to(table, (rows, 128))
    return jnp.take_along_axis(src, index, axis=1, mode="promise_in_bounds")


def planes(lo, hi, fn, carry=None, width=8):
    count = hi - lo
    step = max(d for d in range(1, count + 1) if count % d == 0 and d <= width + width // 2)
    if step * 2 < width and count > width:
        step = width
    whole = count // step * step

    def go(i, c):
        for k in range(step):
            x = lo + i * step + k
            if carry is None:
                fn(x)
            else:
                c = fn(x, c)
        return c

    c = 0 if carry is None else carry
    if whole // step == 1:
        c = go(0, c)
    else:
        c = lax.fori_loop(0, whole // step, go, c)
    for x in range(lo + whole, hi):
        if carry is None:
            fn(x)
        else:
            c = fn(x, c)
    return c


def stencil(ref, c, x, y0, y1):
    mid = ref[c, x, 8 + y0 : 8 + y1, :]
    total = (
        ref[c, x - 1, 8 + y0 : 8 + y1, :]
        + ref[c, x + 1, 8 + y0 : 8 + y1, :]
        + ref[c, x, 7 + y0 : 7 + y1, :]
        + ref[c, x, 9 + y0 : 9 + y1, :]
    )
    lane = lanes(mid.shape)
    last = mid.shape[-1] - 1
    total = total + jnp.where(lane == 0, 0.0, pltpu.roll(mid, 1, 1))
    total = total + jnp.where(lane == last, 0.0, pltpu.roll(mid, last, 1))
    return mid, total


def operate_plane(ref, k, coefs, y0, y1):
    refs, i = coefs
    d = refs[0][i, y0:y1, :]
    a = refs[1][i, y0:y1, :]
    m0, t0 = stencil(ref, 0, k, y0, y1)
    m1, t1 = stencil(ref, 1, k, y0, y1)
    return d * m0 - t0 + a * m1, d * m1 - t1 - a * m0


def fold8(x):
    out = x[0:8]
    for i in range(8, x.shape[0], 8):
        out = out + x[i : i + 8]
    return out


def keep_split(ref, c, i, x):
    top = x.astype(jnp.bfloat16)
    ref[c, i, :, 0:128] = top
    ref[c, i, :, 128:256] = (x - top.astype(F32)).astype(jnp.bfloat16)


def restrict(split, ends, own):
    cx, cy = own
    r = lax.broadcasted_iota(jnp.int32, (256, 128), 0) % 128
    ones = jnp.where(r <= lanes((256, 128)), 1.0, 0.0).astype(jnp.bfloat16)
    per = 16
    out = []
    for c in range(2):
        acc = jnp.zeros((8, 128), F32)
        for i in range(0, cx, per):
            block = split[c, i : i + per].reshape(cy * per, 256)
            sums = jnp.dot(block, ones, preferred_element_type=F32)
            for k in range(per):
                part = sums[cy * k : cy * (k + 1)]
                acc = acc + fold8(jnp.take_along_axis(part, ends[i + k], axis=1, mode="promise_in_bounds"))
        out.append(acc)
    return out


def spread_rhs(g0, g1, cols_ref, pad_ref, out_ref, scalars, grid):
    gx, gy = grid
    n = gx * gy
    lane = lanes((8, 128))
    acc = None
    for c, g in enumerate((g0, g1)):
        total = jnp.broadcast_to(jnp.sum(g, axis=0, keepdims=True), (8, 128))
        for q in range(4):
            source = lane // 32 + 4 * q
            below = jnp.take_along_axis(total, jnp.maximum(source - 1, 0), axis=1, mode="promise_in_bounds")
            weight = jnp.take_along_axis(total, source, axis=1, mode="promise_in_bounds")
            weight = weight - jnp.where(source == 0, 0.0, below)
            term = cols_ref[pl.ds((c * 4 + q) * n, n), :] * weight[0:1]
            acc = term if acc is None else acc + term
    whole = (acc + pltpu.roll(acc, 64, 1)) + (pltpu.roll(acc, 32, 1) + pltpu.roll(acc, 96, 1))
    margin = (pad_ref.shape[0] - n) // 2
    pad_ref[0:margin, :] = jnp.zeros((margin, 128), F32)
    pad_ref[margin + n : 2 * margin + n, :] = jnp.zeros((margin, 128), F32)
    pad_ref[margin : margin + n, :] = whole
    place = lax.broadcasted_iota(jnp.int32, (n, 128), 0) % gy
    group = lanes((n, 128)) // 32
    outs = [jnp.zeros((n, 128), F32) for _ in range(3)]
    for dx in (-1, 0, 1):
        for dy in (-1, 0, 1):
            k = (dx + 1) * 3 + dy + 1
            start = margin + dx * gy + dy
            piece = pad_ref[start : start + n, :]
            ok = (group == k % 4) & (place + dy >= 0) & (place + dy < gy)
            outs[k // 4] = jnp.where(ok, piece, outs[k // 4])
    outs[2] = outs[2] + jnp.broadcast_to(scalars, (n, 128))
    for r in range(3):
        out_ref[:, 128 * r : 128 * (r + 1)] = outs[r]


def scalar_row(items):
    lane = lanes((1, 128))
    row = jnp.zeros((1, 128), F32)
    for where, acc in items:
        s = jnp.sum(jnp.sum(acc, axis=0, keepdims=True), axis=1, keepdims=True)
        row = jnp.where(lane == where, jnp.broadcast_to(s, (1, 128)), row)
    return row


def smooth_plane(f, g, u, k, coefs, y0, y1):
    a0, a1 = operate_plane(f, k, coefs, y0, y1)
    e0, e1 = u[0, k, y0:y1, :] - a0, u[1, k, y0:y1, :] - a1
    refs, i = coefs
    p, q = refs[2][i, y0:y1, :], refs[3][i, y0:y1, :]
    g[0, k, 8 + y0 : 8 + y1, :] = f[0, k, 8 + y0 : 8 + y1, :] + (p * e0 - q * e1)
    g[1, k, 8 + y0 : 8 + y1, :] = f[1, k, 8 + y0 : 8 + y1, :] + (p * e1 + q * e0)


def pairs(lo, hi, size, fn, low, high):
    if hi > lo:
        def go(x):
            fn(x, low(x))
            y = size - 1 - x
            fn(y, high(y))

        planes(lo, hi, go, width=4)


def centre(f, g, u, t, t_rim, places, halo, s, split, ends, own, rows, t_rows):
    mine, low, high = places
    cx, cy = own
    size = cx + 2 * HALO
    y0, y1 = HALO, HALO + cy
    r0, r1 = t_rows
    pairs(HALO - halo + 1, HALO, size, lambda k, c: smooth_plane(f, g, u, k, c, *rows), low, high)
    planes(HALO, HALO + cx, lambda x: smooth_plane(f, g, u, x, mine(x), *rows))

    def outer(k, c):
        a0, a1 = operate_plane(g, k, c, r0, r1)
        t_rim[0, c[1], r0:r1, :], t_rim[1, c[1], r0:r1, :] = a0, a1

    pairs(HALO - halo + 2, HALO, size, outer, low, high)

    def middle(x):
        i = x - HALO
        a0, a1 = operate_plane(g, x, mine(x), r0, r1)
        t[0, i, r0:r1, :], t[1, i, r0:r1, :] = a0, a1
        lo = y0 - r0
        s[0, i] = g[0, x, 8 + y0 : 8 + y1, :]
        s[1, i] = g[1, x, 8 + y0 : 8 + y1, :]
        keep_split(split, 0, i, u[0, x, y0:y1, :] - a0[lo : lo + cy])
        keep_split(split, 1, i, u[1, x, y0:y1, :] - a1[lo : lo + cy])

    planes(HALO, HALO + cx, middle)
    return restrict(split, ends, own)


def fill(store, y0, y1, wave, layer, a):
    sq = wave * wave
    ab = sq * (layer * layer * (pml_strength / 9.0))
    d = 6.0 - sq
    w = jnp.where(wave > 0.0, damping * pl.reciprocal(d * d + ab * ab), 0.0)
    refs, i = store
    refs[0][i, y0:y1, :] = d
    refs[1][i, y0:y1, :] = ab
    refs[2][i, y0:y1, :] = d * w
    refs[3][i, y0:y1, :] = ab * w
    refs[4][i, y0:y1, :] = a


def own_kernel(own, rhs, wave, layer, agg, ylo, yhi, diag, absorb, sre, sim, ids, ends, sq_out):
    cx, cy = own
    ey = cy + 2 * HALO
    home = (diag, absorb, sre, sim, ids)

    def inner(i, acc):
        store = (home, i)
        fill(store, 0, HALO, ylo[2, i], ylo[3, i], ylo[4, i].astype(jnp.int32))
        fill(store, HALO + cy, ey, yhi[2, i], yhi[3, i], yhi[4, i].astype(jnp.int32))
        fill(store, HALO, HALO + cy, wave[i], layer[i].astype(F32), agg[i])
        r0, r1 = rhs[0, i], rhs[1, i]
        return acc + fold8(r0 * r0 + r1 * r1)

    sq = planes(0, cx, inner, jnp.zeros((8, 128), F32))
    sq_out[...] = scalar_row([(40, sq)])

    def find(i):
        a = agg[i]
        lane = lanes(a.shape)
        low = jnp.zeros(a.shape, jnp.int32)
        step = a.shape[1] // 2
        while step >= 1:
            probe = low + step
            val = jnp.take_along_axis(a, probe - 1, axis=1, mode="promise_in_bounds")
            low = jnp.where(val <= lane, probe, low)
            step //= 2
        val = jnp.take_along_axis(a, low, axis=1, mode="promise_in_bounds")
        low = jnp.where(val <= lane, low + 1, low)
        ends[i] = jnp.maximum(low - 1, 0)

    planes(0, cx, find)


def start_kernel(grid, own, *refs):
    rhs, ylo, yhi, xlo, xhi, clo, chi, cols, ends, sq = refs[:10]
    home, rim = refs[10:15], refs[15:20]
    t, t_rim, s, out_ref, u, f, g, split, pad = refs[20:]
    cx, cy = own
    ey = cy + 2 * HALO
    y0, y1 = HALO, HALO + cy
    mine = lambda x: (home, x - HALO)
    low = lambda x: (rim, x)
    high = lambda x: (rim, x - cx)

    def first(place, k, lo, hi, r0, r1):
        refs, i = place
        p, q = refs[2][i, lo:hi, :], refs[3][i, lo:hi, :]
        u[0, k, lo:hi, :] = r0
        u[1, k, lo:hi, :] = r1
        f[0, k, 8 + lo : 8 + hi, :] = p * r0 - q * r1
        f[1, k, 8 + lo : 8 + hi, :] = p * r1 + q * r0

    for k in range(HALO):
        for buf, corner, i, x in ((xlo, clo, HALO - 1 - k, HALO - 1 - k), (xhi, chi, k, HALO + cx + k)):
            place = low(x) if x < HALO else high(x)
            below, above = corner_plane(corner, k)
            for src, lo, hi in ((below, 0, y0), (buf[:, i], y0, y1), (above, y1, ey)):
                fill(place, lo, hi, src[2], src[3], src[4].astype(jnp.int32))
                first(place, x, lo, hi, src[0], src[1])

    def inner(x):
        i = x - HALO
        first(mine(x), x, 0, y0, ylo[0, i], ylo[1, i])
        first(mine(x), x, y0, y1, rhs[0, i], rhs[1, i])
        first(mine(x), x, y1, ey, yhi[0, i], yhi[1, i])

    planes(HALO, HALO + cx, inner)
    g0, g1 = centre(f, g, u, t, t_rim, (mine, low, high), HALO, s, split, ends, own, (0, ey), (0, ey))
    spread_rhs(g0, g1, cols, pad, out_ref, sq[...], grid)


def read_scalars(raw, olds, j):
    h = []
    for i in range(j):
        a0, a1 = pick(raw, 32 + 2 * i), pick(raw, 33 + 2 * i)
        for k in range(i):
            b0, b1 = pick(olds[i], 32 + 2 * k), pick(olds[i], 33 + 2 * k)
            a0, a1 = a0 - (b0 * h[k][0] + b1 * h[k][1]), a1 - (b0 * h[k][1] - b1 * h[k][0])
        inv = pick(olds[i], 41)
        h.append((a0 * inv, a1 * inv))
    sq = pick(raw, 40)
    for a0, a1 in h:
        sq = sq - (a0 * a0 + a1 * a1)
    length = jnp.sqrt(jnp.maximum(sq, 0.0) + epsilon)
    return h, length


def write_scalars(out, h, length, inv):
    lane = lanes((1, 128))
    row = jnp.where(lane == 40, length[0:1], inv[0:1])
    for k, pair in enumerate(h):
        for c in range(2):
            row = jnp.where(lane == 32 + 2 * k + c, pair[c][0:1], row)
    out[...] = row


def like(v, rows):
    return jnp.concatenate([v] * (rows // 8), axis=0)


def combine(scalars, new, old):
    h, inv = scalars
    a0, a1 = new
    rows = a0.shape[0]
    for i in range(len(h)):
        b0, b1 = old(i)
        r, q = like(h[i][0], rows), like(h[i][1], rows)
        a0 = a0 - (r * b0 - q * b1)
        a1 = a1 - (r * b1 + q * b0)
    s = like(inv, rows)
    return a0 * s, a1 * s


def splats(row, first):
    return [pick(row, first + k) for k in range(AGG)]


def marks(index):
    return [(index & 1) == 1, (index & 3) >= 2, (index & 7) >= 4, index >= 8]


def choose(values, bits):
    rows = bits[0].shape[0]
    level = [like(v, rows) for v in values]
    for bit in bits:
        level = [jnp.where(bit, level[k + 1], level[k]) for k in range(0, len(level), 2)]
    return level[0]


def prolong_plane(pc, k, ids, i, table, own, dx, values=None):
    cy = own[1]
    ey = cy + 2 * HALO
    for dy, lo, hi in ((0, 0, HALO), (1, HALO, HALO + cy), (2, HALO + cy, ey)):
        n = dx * 3 + dy
        if values is not None and dy == 1:
            bits = marks(ids[i, lo:hi, :])
            for c in range(2):
                pc[c, k, 8 + lo : 8 + hi, :] = choose(values[c], bits)
            continue
        src = table[:, 128 * (n // 4) : 128 * (n // 4) + 128]
        index = ids[i, lo:hi, :] + 32 * (n % 4)
        pc[0, k, 8 + lo : 8 + hi, :] = take(src, index)
        pc[1, k, 8 + lo : 8 + hi, :] = take(src, index + AGG)


def image_plane(pc, k, coefs, t_in, m_old, scalars, lo, hi):
    i = coefs[1]
    a0, a1 = operate_plane(pc, k, coefs, lo, hi)
    m = combine(
        scalars,
        (t_in[0, i, lo:hi, :], t_in[1, i, lo:hi, :]),
        lambda n: (m_old[n][0, i, lo:hi, :], m_old[n][1, i, lo:hi, :]),
    )
    return m, (m[0] + a0, m[1] + a1)


def image_store(pc, u, f, k, coefs, t_in, m_old, scalars, m_out, lo, hi):
    m, (u0, u1) = image_plane(pc, k, coefs, t_in, m_old, scalars, lo, hi)
    refs, i = coefs
    if m_out is not None:
        m_out[0, i, lo:hi, :], m_out[1, i, lo:hi, :] = m
    p, q = refs[2][i, lo:hi, :], refs[3][i, lo:hi, :]
    u[0, k, lo:hi, :], u[1, k, lo:hi, :] = u0, u1
    f[0, k, 8 + lo : 8 + hi, :] = p * u0 - q * u1
    f[1, k, 8 + lo : 8 + hi, :] = p * u1 + q * u0
    return u0, u1


def y_rows(j, cy):
    halo = HALO - 2 - 2 * j
    if halo > 4:
        return 0, cy + 2 * HALO
    if halo > 0:
        return HALO - 4, HALO + cy + 4
    return HALO, HALO + cy


def step_kernel(j, grid, own, *refs):
    refs = list(refs)
    take_refs = lambda k: [refs.pop(0) for _ in range(k)]
    last = j == ITERS - 1
    rcv = refs.pop(0)
    home, rim = take_refs(5), take_refs(5)
    ends, cols, t_own, t_rim = take_refs(4)
    m_own, m_rim = take_refs(j), take_refs(0 if last else j)
    u_in, c_old, h_old = take_refs(j + 1), take_refs(j), take_refs(j)
    c_out, h_out, out_ref = take_refs(3)
    if not last:
        m_out, t, u_out, s_out = take_refs(4)
    mr_out = tr_out = None
    if j < ITERS - 2:
        mr_out, tr_out = take_refs(2)
    pc = refs.pop(0)
    if not last:
        u, f, split, pad = take_refs(4)
    cx, cy = own
    mine = lambda x: (home, x - HALO)
    low = lambda x: (rim, x)
    high = lambda x: (rim, x - cx)
    y0, y1 = HALO, HALO + cy
    rows = y_rows(j, cy)
    halo = HALO - 2 - 2 * j
    size = cx + 2 * HALO

    row = jnp.sum(rcv[...], axis=0, keepdims=True)
    h, length = read_scalars(row[:, 256:384], [r[...] for r in h_old], j)
    inv = 1.0 / length
    write_scalars(h_out, h, length, inv)
    scalars = h, inv
    wide = lambda v: jnp.concatenate([v[0:1]] * 3, axis=1)
    table = row
    for i in range(j):
        old = c_old[i][...]
        table = table - (wide(h[i][0]) * old + wide(h[i][1]) * turn_rows(old))
    table = table * wide(inv)
    c_out[...] = table

    def outside(x):
        prolong_plane(pc, x, rim[4], x, table, own, 0)
        y = 2 * HALO - 1 - x
        prolong_plane(pc, y + cx, rim[4], y, table, own, 2)

    planes(HALO - halo - 1, HALO, outside, width=4)
    values = [splats(table[:, 128:256], AGG * c) for c in range(2)]
    planes(HALO, HALO + cx, lambda x: prolong_plane(pc, x, home[4], x - HALO, table, own, 1, values))

    def outer(k, c):
        image_store(pc, u, f, k, c, t_rim, m_rim, scalars, mr_out, *rows)

    pairs(HALO - halo, HALO, size, outer, low, high)

    def middle(x, acc):
        i = x - HALO
        if last:
            u0, u1 = image_plane(pc, x, mine(x), t_own, m_own, scalars, y0, y1)[1]
        else:
            u0, u1 = image_store(pc, u, f, x, mine(x), t_own, m_own, scalars, m_out, *rows)
            lo = y0 - rows[0]
            u0, u1 = u0[lo : lo + cy], u1[lo : lo + cy]
            u_out[0, i], u_out[1, i] = u0, u1
        new = []
        for k in range(j + 1):
            b0, b1 = u_in[k][0, i], u_in[k][1, i]
            new.append(fold8(b0 * u0 + b1 * u1))
            new.append(fold8(b0 * u1 - b1 * u0))
        new.append(fold8(u0 * u0 + u1 * u1))
        return tuple(a + b for a, b in zip(acc, new))

    zero = jnp.zeros((8, 128), F32)
    acc = planes(HALO, HALO + cx, middle, (zero,) * (2 * j + 3))
    items = [(32 + k, acc[k]) for k in range(2 * j + 2)] + [(40, acc[-1])]
    dots = scalar_row(items)
    if last:
        n = out_ref.shape[0]
        for r in range(2):
            out_ref[:, 128 * r : 128 * r + 128] = jnp.zeros((n, 128), F32)
        out_ref[:, 256:384] = jnp.broadcast_to(dots, (n, 128))
        return
    t_rows = rows if j < ITERS - 2 else (y0, y1)
    g0, g1 = centre(f, pc, u, t, tr_out, (mine, low, high), halo, s_out, split, ends, own, rows, t_rows)
    spread_rhs(g0, g1, cols, pad, out_ref, dots, grid)


def pack_kernel(rhs, wave, layer, agg, ylow, yhigh, xlow, xhigh, yint, xint, sems):
    cx, cy = wave.shape[:2]
    every = slice(None)
    cuts = (
        (ylow, yint, 0, every, pl.ds(0, HALO)),
        (yhigh, yint, 2, every, pl.ds(cy - HALO, HALO)),
        (xlow, xint, 0, pl.ds(0, HALO), every),
        (xhigh, xint, 2, pl.ds(cx - HALO, HALO), every),
    )
    copies = []
    for k, (out, ints, slot, xs, ys) in enumerate(cuts):
        for i, (src, dst) in enumerate((
            (rhs.at[:, xs, ys, :], out.at[0:2]),
            (wave.at[xs, ys, :], out.at[2]),
            (layer.at[xs, ys, :], ints.at[slot]),
            (agg.at[xs, ys, :], ints.at[slot + 1]),
        )):
            copies.append(pltpu.make_async_copy(src, dst, sems.at[4 * k + i]))
    for copy in copies:
        copy.start()
    for copy in copies:
        copy.wait()
    for out, ints, slot, _, _ in cuts:
        out[3] = ints[slot].astype(F32)
        out[4] = ints[slot + 1].astype(F32)


def corner_kernel(ylo, yhi, low, high):
    cx = ylo.shape[1]
    row = lax.broadcasted_iota(jnp.int32, (5, HALO, ylo.shape[3]), 1)
    for out, plane in ((low, lambda k: k), (high, lambda k: cx - 1 - k)):
        for p in range(HALO // 2):
            a, b = plane(p), plane(HALO - 2 - p)
            out[:, p, 0:HALO, :] = jnp.where(row > p, ylo[:, a], pltpu.roll(ylo[:, b], p + 1, 1))
            out[:, p, HALO : 2 * HALO, :] = jnp.where(
                row < HALO - 1 - p, yhi[:, a], pltpu.roll(yhi[:, b], HALO - 1 - p, 1)
            )


def corner_plane(buf, k):
    if k == HALO - 1:
        zero = jnp.zeros((5, HALO, buf.shape[3]), F32)
        return zero, zero
    p = min(k, HALO - 2 - k)
    below, above = buf[:, p, 0:HALO, :], buf[:, p, HALO : 2 * HALO, :]
    if k != p:
        below, above = pltpu.roll(below, HALO - 1 - p, 1), pltpu.roll(above, p + 1, 1)
    return below, above


def columns_kernel(inverse, out, turned):
    turned[:, 0:32] = inverse[...].T
    group = lanes(out.shape) // 32
    total = jnp.zeros(out.shape, F32)
    for r in range(4):
        part = turned[pl.ds(r, out.shape[0], stride=4), :]
        part = jnp.where(group == 0, part, 0.0)
        total = total + (part if r == 0 else pltpu.roll(part, 32 * r, 1))
    out[...] = total


def arrange_kernel(got, out):
    n = got.shape[0] // 4
    for q in range(4):
        rows = got[pl.ds(q, n, stride=4), :]
        out[q * n : (q + 1) * n, :] = rows
        out[(4 + q) * n : (5 + q) * n, :] = turn(rows)


def cmul(a, b):
    return a[0] * b[0] - a[1] * b[1], a[0] * b[1] + a[1] * b[0]


def finish_kernel(own, *refs):
    rcv, ids = refs[0], refs[1]
    z = refs[2 : 2 + ITERS]
    c = refs[2 + ITERS : 2 + 2 * ITERS]
    rows = refs[2 + 2 * ITERS : 2 + 3 * ITERS]
    sol, hess = refs[2 + 3 * ITERS :]
    cx, cy = own
    final = jnp.sum(rcv[:, 256:384], axis=0, keepdims=True)
    scal = [r[...] for r in rows]
    beta = pick(scal[0], 40)
    upper, sub = [], []
    for j in range(1, ITERS):
        upper.append([(pick(scal[j], 32 + 2 * i), pick(scal[j], 33 + 2 * i)) for i in range(j)])
        sub.append(pick(scal[j], 40))
    h, length = read_scalars(final, scal, ITERS)
    upper.append(h)
    sub.append(length)
    r_i = lax.broadcasted_iota(jnp.int32, (8, 128), 0)
    c_i = lanes((8, 128))
    for comp in range(2):
        block = jnp.zeros((8, 128), F32)
        for j in range(ITERS):
            for i in range(j + 1):
                block = jnp.where((r_i == j) & (c_i == i), upper[j][i][comp], block)
            if comp == 0:
                block = jnp.where((r_i == j) & (c_i == j + 1), sub[j], block)
        hess[comp] = block[0:ITERS, 0 : ITERS + 1]
    zero = jnp.zeros((8, 128), F32)
    target = [(beta, zero)]
    rot = []
    tri = []
    for j in range(ITERS):
        col = list(upper[j])
        for i in range(j):
            cr, ci, s = rot[i]
            a, b = col[i], col[i + 1]
            up = cmul((cr, -ci), a)
            dn = cmul((cr, ci), b)
            col[i] = (up[0] + s * b[0], up[1] + s * b[1])
            col[i + 1] = (dn[0] - s * a[0], dn[1] - s * a[1])
        a = col[j]
        big = jnp.sqrt(a[0] * a[0] + a[1] * a[1] + sub[j] * sub[j])
        w = 1.0 / big
        cr, ci, s = a[0] * w, a[1] * w, sub[j] * w
        rot.append((cr, ci, s))
        g = target[j]
        target[j] = cmul((cr, -ci), g)
        target.append((-s * g[0], -s * g[1]))
        col[j] = big
        tri.append(col)
    y = [None] * ITERS
    for j in reversed(range(ITERS)):
        a0, a1 = target[j]
        for k in range(j + 1, ITERS):
            b = cmul(tri[k][j], y[k])
            a0, a1 = a0 - b[0], a1 - b[1]
        w = 1.0 / tri[j][j]
        y[j] = (a0 * w, a1 * w)
    table = jnp.zeros((1, 128), F32)
    for j in range(ITERS):
        old = c[j][:, 128:256]
        table = table + (y[j][0][0:1] * old + y[j][1][0:1] * turn(old))

    gamma = list(y)
    for j in reversed(range(ITERS)):
        w = 1.0 / (sub[j - 1] if j > 0 else beta)
        gamma[j] = (gamma[j][0] * w, gamma[j][1] * w)
        for i in range(j):
            b = cmul(upper[j - 1][i], gamma[j])
            gamma[i] = (gamma[i][0] - b[0], gamma[i][1] - b[1])

    values = splats(table, AGG)

    def go(i):
        index = ids[i, HALO : HALO + cy, :]
        a0, a1 = take(table, index), choose(values, marks(index))
        for j in range(ITERS):
            b = cmul((like(gamma[j][0], cy), like(gamma[j][1], cy)), (z[j][0, i], z[j][1, i]))
            a0, a1 = a0 + b[0], a1 + b[1]
        sol[0, i], sol[1, i] = a0, a1

    planes(0, cx, go)


def shape(*dims, dtype=F32):
    return jax.ShapeDtypeStruct(dims, dtype)


def call(kernel, outs, scratch, args, flops=100_000_000, space=pltpu.VMEM):
    vm = pl.BlockSpec(memory_space=pltpu.VMEM)
    return pl.pallas_call(
        kernel,
        out_shape=outs,
        in_specs=[pl.BlockSpec(memory_space=space)] * len(args),
        out_specs=[vm] * len(outs),
        scratch_shapes=scratch,
        compiler_params=pltpu.CompilerParams(vmem_limit_bytes=VLIMIT),
        cost_estimate=pl.CostEstimate(flops=flops, bytes_accessed=1_000_000, transcendentals=0),
    )(*args)


def exchange(x):
    return lax.all_to_all(x, AXES, 0, 0, tiled=True)


def program(right_side, wavenumber, pml_layer, aggregate, coarse_inverse):
    gx, gy = lax.axis_size("gx"), lax.axis_size("gy")
    n = gx * gy
    cx, cy, cz = wavenumber.shape
    own = (cx, cy)
    ex, ey = cx + 2 * HALO, cy + 2 * HALO
    grid = (gx, gy)
    margin = -(-(gy + 1) // 8) * 8

    def swap(low, high, axis):
        count = lax.axis_size(axis)
        up = [(i, i + 1) for i in range(count - 1)]
        down = [(b, a) for a, b in up]
        low_in = lax.ppermute(high, axis, up)
        high_in = lax.ppermute(low, axis, down)
        return low_in, high_in

    strip, slab = shape(5, cx, HALO, cz), shape(5, HALO, cy, cz)
    ylow, yhigh, xlow, xhigh = call(
        pack_kernel, [strip, strip, slab, slab],
        [pltpu.VMEM((4, cx, HALO, cz), jnp.int32), pltpu.VMEM((4, HALO, cy, cz), jnp.int32), pltpu.SemaphoreType.DMA((16,))],
        [pltpu.with_memory_space_constraint(x, pltpu.HBM) for x in (right_side, wavenumber, pml_layer, aggregate)],
        space=pltpu.HBM,
    )
    ylo, yhi = swap(ylow, yhigh, "gy")
    xlo, xhi = swap(xlow, xhigh, "gx")
    (inverse,) = call(
        columns_kernel, [shape(4 * n, 128)], [pltpu.VMEM((AGG * n, 128), F32)],
        [coarse_inverse.reshape(2 * AGG, AGG * n)],
    )
    cols = exchange(inverse)
    right_side, wavenumber, pml_layer, aggregate, ylo, yhi, cols = lax.optimization_barrier(
        (right_side, wavenumber, pml_layer, aggregate, ylo, yhi, cols)
    )
    corner = shape(5, HALO // 2, 2 * HALO, cz)
    clow, chigh = call(corner_kernel, [corner, corner], [], [ylo, yhi])
    clo, chi = swap(clow, chigh, "gx")
    (cols,) = call(arrange_kernel, [shape(8 * n, 128)], [], [cols])
    I32 = jnp.int32
    home = [shape(cx, ey, cz)] * 4 + [shape(cx, ey, cz, dtype=I32)]
    rim = [shape(2 * HALO, ey, cz)] * 4 + [shape(2 * HALO, ey, cz, dtype=I32)]
    home2, rim2 = shape(2, cx, ey, cz), shape(2, 2 * HALO, ey, cz)
    mine = shape(2, cx, cy, cz)
    chunk = shape(n, 384)
    vmem = lambda *dims, dtype=F32: pltpu.VMEM(dims, dtype)
    tall = vmem(2, ex, ey + 16, cz)
    flat = vmem(2, ex, ey, cz)
    pad = vmem(n + 2 * margin, 128)
    split = vmem(2, cx, cy, 256, dtype=jnp.bfloat16)

    *own_coefs, ends, sq = call(
        functools.partial(own_kernel, own),
        home + [shape(cx, cy, cz, dtype=I32), shape(1, 128)], [],
        [right_side, wavenumber, pml_layer, aggregate, ylo, yhi],
    )
    res = call(
        functools.partial(start_kernel, grid, own),
        rim + [home2, rim2, mine, chunk],
        [flat, tall, tall, split, pad],
        [right_side, ylo, yhi, xlo, xhi, clo, chi, cols, ends, sq] + own_coefs,
    )
    rim_coefs = list(res[:5])
    t_own, t_rim, s, send = res[5:]
    got = exchange(send)
    ms, mrs, us, ss, cs, hs = [], [], [right_side], [s], [], []
    for j in range(ITERS):
        last = j == ITERS - 1
        args = [got] + own_coefs + rim_coefs + [ends, cols, t_own, t_rim] + ms + ([] if last else mrs) + us + cs + hs
        outs = [shape(1, 384), shape(1, 128), chunk]
        scratch = [tall]
        if not last:
            outs += [home2, home2, mine, mine]
            if j < ITERS - 2:
                outs += [rim2, rim2]
            scratch += [flat, tall, split, pad]
        c, h, send, *rest = call(functools.partial(step_kernel, j, grid, own), outs, scratch, args)
        got = exchange(send)
        if not last:
            m, t_own, u, s = rest[:4]
            us.append(u)
            ms.append(m)
            ss.append(s)
            if j < ITERS - 2:
                mrs.append(rest[4])
                t_rim = rest[5]
        cs.append(c)
        hs.append(h)
    sol, hess = call(
        functools.partial(finish_kernel, own),
        [mine, shape(2, ITERS, ITERS + 1)],
        [],
        [got, own_coefs[4]] + ss + cs + hs,
    )
    return sol, jnp.swapaxes(hess, 1, 2)


def solution(mesh):
    return jax.shard_map(
        program,
        mesh=mesh,
        in_specs=(
            P(None, "gx", "gy", None),
            P("gx", "gy", None),
            P("gx", "gy", None),
            P("gx", "gy", None),
            P(None, ("gx", "gy"), None),
        ),
        out_specs=(P(None, "gx", "gy", None), P()),
        check_vma=False,
    )
```

```python
import functools

import jax
import jax.numpy as jnp
from jax import lax
from jax.experimental import pallas as pl
from jax.experimental.pallas import tpu as pltpu
from jax.sharding import PartitionSpec as P


ITERS = 4
HALO = 2 * ITERS
GROUP = 4
AXES = ("gx", "gy")
AGG = 16
damping = 0.8
pml_strength = 3.0
epsilon = 1e-06
F32 = jnp.float32
VLIMIT = 16 * 1024 * 1024


def lanes(shape):
    return lax.broadcasted_iota(jnp.int32, shape, len(shape) - 1)


def turn(x):
    odd = (lanes(x.shape) // AGG) % 2 == 1
    return jnp.where(odd, pltpu.roll(x, AGG, 1), -pltpu.roll(x, x.shape[1] - AGG, 1))


def turn_rows(x):
    parts = [turn(x[:, i : i + 128]) for i in range(0, x.shape[1], 128)]
    return jnp.concatenate(parts, axis=1)


def pick(row, lane):
    return jnp.broadcast_to(row[:, lane : lane + 1], (8, 128))


def take(table, index):
    rows = index.shape[0]
    src = jnp.broadcast_to(table, (rows, 128))
    return jnp.take_along_axis(src, index, axis=1, mode="promise_in_bounds")


def planes(lo, hi, fn, carry=None, width=16):
    count = hi - lo
    step = max(d for d in range(1, count + 1) if count % d == 0 and d <= width + width // 2)
    if step * 2 < width and count > width:
        step = width
    whole = count // step * step

    def go(i, c):
        for k in range(step):
            x = lo + i * step + k
            if carry is None:
                fn(x)
            else:
                c = fn(x, c)
        return c

    c = 0 if carry is None else carry
    if whole // step == 1:
        c = go(0, c)
    else:
        c = lax.fori_loop(0, whole // step, go, c)
    for x in range(lo + whole, hi):
        if carry is None:
            fn(x)
        else:
            c = fn(x, c)
    return c


def stencil(ref, c, x, y0, y1):
    mid = ref[c, x, 8 + y0 : 8 + y1, :]
    lane = lanes(mid.shape)
    last = mid.shape[-1] - 1
    total = jnp.where(lane == 0, 0.0, pltpu.roll(mid, 1, 1)) + jnp.where(lane == last, 0.0, pltpu.roll(mid, last, 1))
    total = total + (ref[c, x - 1, 8 + y0 : 8 + y1, :] + ref[c, x + 1, 8 + y0 : 8 + y1, :])
    return mid, total + (ref[c, x, 7 + y0 : 7 + y1, :] + ref[c, x, 9 + y0 : 9 + y1, :])


def operate_plane(ref, k, coefs, y0, y1):
    refs, i = coefs
    d = refs[0][i, y0:y1, :]
    a = refs[1][i, y0:y1, :]
    m0, t0 = stencil(ref, 0, k, y0, y1)
    m1, t1 = stencil(ref, 1, k, y0, y1)
    return d * m0 - t0 + a * m1, d * m1 - t1 - a * m0


def fold8(x):
    out = x[0:8]
    for i in range(8, x.shape[0], 8):
        out = out + x[i : i + 8]
    return out


def halves(x):
    top = x.astype(jnp.bfloat16)
    return jnp.concatenate([top, (x - top.astype(F32)).astype(jnp.bfloat16)], axis=1)


def below_ones():
    r = lax.broadcasted_iota(jnp.int32, (256, 128), 0) % 128
    return jnp.where(r <= lanes((256, 128)), 1.0, 0.0).astype(jnp.bfloat16)


def restrict(parts, ends, i, ones, acc):
    cy = parts[0][0].shape[0]
    sums = jnp.dot(
        jnp.concatenate([p for pair in parts for p in pair], axis=0), ones, preferred_element_type=F32
    )
    acc = list(acc)
    for k in range(len(parts)):
        index = ends[i + k]
        for c in range(2):
            part = sums[cy * (2 * k + c) : cy * (2 * k + c + 1)]
            acc[c] = acc[c] + fold8(jnp.take_along_axis(part, index, axis=1, mode="promise_in_bounds"))
    return tuple(acc)


def spread_rhs(g0, g1, cols_ref, pad_ref, out_ref, scalars, grid):
    gx, gy = grid
    n = gx * gy
    lane = lanes((8, 128))
    acc = None
    for c, g in enumerate((g0, g1)):
        total = jnp.broadcast_to(jnp.sum(g, axis=0, keepdims=True), (8, 128))
        for q in range(4):
            source = lane // 32 + 4 * q
            below = jnp.take_along_axis(total, jnp.maximum(source - 1, 0), axis=1, mode="promise_in_bounds")
            weight = jnp.take_along_axis(total, source, axis=1, mode="promise_in_bounds")
            weight = weight - jnp.where(source == 0, 0.0, below)
            term = cols_ref[pl.ds((c * 4 + q) * n, n), :] * weight[0:1]
            acc = term if acc is None else acc + term
    whole = (acc + pltpu.roll(acc, 64, 1)) + (pltpu.roll(acc, 32, 1) + pltpu.roll(acc, 96, 1))
    margin = (pad_ref.shape[0] - n) // 2
    pad_ref[0:margin, :] = jnp.zeros((margin, 128), F32)
    pad_ref[margin + n : 2 * margin + n, :] = jnp.zeros((margin, 128), F32)
    pad_ref[margin : margin + n, :] = whole
    place = lax.broadcasted_iota(jnp.int32, (n, 128), 0) % gy
    group = lanes((n, 128)) // 32
    outs = [jnp.zeros((n, 128), F32) for _ in range(3)]
    for dx in (-1, 0, 1):
        for dy in (-1, 0, 1):
            k = (dx + 1) * 3 + dy + 1
            start = margin + dx * gy + dy
            piece = pad_ref[start : start + n, :]
            ok = (group == k % 4) & (place + dy >= 0) & (place + dy < gy)
            outs[k // 4] = jnp.where(ok, piece, outs[k // 4])
    outs[2] = outs[2] + jnp.broadcast_to(scalars, (n, 128))
    for r in range(3):
        out_ref[:, 128 * r : 128 * (r + 1)] = outs[r]


def scalar_row(items):
    lane = lanes((1, 128))
    row = jnp.zeros((1, 128), F32)
    for where, acc in items:
        s = jnp.sum(jnp.sum(acc, axis=0, keepdims=True), axis=1, keepdims=True)
        row = jnp.where(lane == where, jnp.broadcast_to(s, (1, 128)), row)
    return row


def smooth_plane(f, g, u, k, coefs, y0, y1):
    a0, a1 = operate_plane(f, k, coefs, y0, y1)
    e0, e1 = u[0, k, y0:y1, :] - a0, u[1, k, y0:y1, :] - a1
    refs, i = coefs
    p, q = refs[2][i, y0:y1, :], refs[3][i, y0:y1, :]
    g[0, k, 8 + y0 : 8 + y1, :] = f[0, k, 8 + y0 : 8 + y1, :] + (p * e0 - q * e1)
    g[1, k, 8 + y0 : 8 + y1, :] = f[1, k, 8 + y0 : 8 + y1, :] + (p * e1 + q * e0)


def window(halo, cy):
    if halo > 4:
        return 0, cy + 2 * HALO
    if halo > 0:
        return HALO - 4, HALO + cy + 4
    return HALO, HALO + cy


def pairs(lo, size, fn, low, high):
    for x in range(lo, HALO):
        y = size - 1 - x
        fn(x, low(x), HALO - x)
        fn(y, high(y), HALO - x)


def centre(f, g, u, t, t_rim, places, halo, s, ends, own, rows, t_rows):
    mine, low, high = places
    cx, cy = own
    size = cx + 2 * HALO
    y0, y1 = HALO, HALO + cy
    r0, r1 = t_rows
    pairs(
        HALO - halo + 1, size,
        lambda k, c, far: smooth_plane(f, g, u, k, c, *window(halo - 1 - far, cy)), low, high,
    )
    planes(HALO, HALO + cx, lambda x: smooth_plane(f, g, u, x, mine(x), *rows))

    def outer(k, c, far):
        q0, q1 = window(halo - 2 - far, cy)
        a0, a1 = operate_plane(g, k, c, q0, q1)
        t_rim[0, c[1], q0:q1, :], t_rim[1, c[1], q0:q1, :] = a0, a1

    pairs(HALO - halo + 2, size, outer, low, high)

    ones = below_ones()

    def middle(b, acc):
        parts = []
        for k in range(GROUP):
            i = b * GROUP + k
            x = HALO + i
            a0, a1 = operate_plane(g, x, mine(x), r0, r1)
            t[0, i, r0:r1, :], t[1, i, r0:r1, :] = a0, a1
            lo = y0 - r0
            s[0, i] = g[0, x, 8 + y0 : 8 + y1, :]
            s[1, i] = g[1, x, 8 + y0 : 8 + y1, :]
            parts.append((
                halves(u[0, x, y0:y1, :] - a0[lo : lo + cy]), halves(u[1, x, y0:y1, :] - a1[lo : lo + cy])
            ))
        return restrict(parts, ends, b * GROUP, ones, acc)

    zero = jnp.zeros((8, 128), F32)
    return planes(0, cx // GROUP, middle, (zero, zero), width=16 // GROUP)


def fill(store, y0, y1, wave, layer, a):
    sq = wave * wave
    ab = sq * (layer * layer * (pml_strength / 9.0))
    d = 6.0 - sq
    w = jnp.where(wave > 0.0, damping * pl.reciprocal(d * d + ab * ab), 0.0)
    refs, i = store
    refs[0][i, y0:y1, :] = d
    refs[1][i, y0:y1, :] = ab
    refs[2][i, y0:y1, :] = d * w
    refs[3][i, y0:y1, :] = ab * w
    refs[4][i, y0:y1, :] = a


def own_kernel(own, rhs, wave, layer, agg, ylo, yhi, diag, absorb, sre, sim, ids, ends, sq_out):
    cx, cy = own
    ey = cy + 2 * HALO
    home = (diag, absorb, sre, sim, ids)

    def inner(i, acc):
        store = (home, i)
        fill(store, 0, HALO, ylo[2, i], ylo[3, i], ylo[4, i].astype(jnp.int32))
        fill(store, HALO + cy, ey, yhi[2, i], yhi[3, i], yhi[4, i].astype(jnp.int32))
        fill(store, HALO, HALO + cy, wave[i], layer[i].astype(F32), agg[i])
        r0, r1 = rhs[0, i], rhs[1, i]
        return acc + fold8(r0 * r0 + r1 * r1)

    sq = planes(0, cx, inner, jnp.zeros((8, 128), F32), width=8)
    sq_out[...] = scalar_row([(40, sq)])

    def find(i):
        a = agg[i]
        lane = lanes(a.shape)
        low = jnp.zeros(a.shape, jnp.int32)
        step = a.shape[1] // 2
        while step >= 1:
            probe = low + step
            val = jnp.take_along_axis(a, probe - 1, axis=1, mode="promise_in_bounds")
            low = jnp.where(val <= lane, probe, low)
            step //= 2
        val = jnp.take_along_axis(a, low, axis=1, mode="promise_in_bounds")
        low = jnp.where(val <= lane, low + 1, low)
        ends[i] = jnp.maximum(low - 1, 0)

    planes(0, cx, find, width=8)


def start_kernel(grid, own, *refs):
    rhs, ylo, yhi, xlo, xhi, clo, chi, cols, ends, sq = refs[:10]
    home, rim = refs[10:15], refs[15:20]
    t, t_rim, s, out_ref, u, f, g, pad = refs[20:]
    cx, cy = own
    ey = cy + 2 * HALO
    y0, y1 = HALO, HALO + cy
    mine = lambda x: (home, x - HALO)
    low = lambda x: (rim, x)
    high = lambda x: (rim, x - cx)

    def first(place, k, lo, hi, r0, r1):
        refs, i = place
        p, q = refs[2][i, lo:hi, :], refs[3][i, lo:hi, :]
        u[0, k, lo:hi, :] = r0
        u[1, k, lo:hi, :] = r1
        f[0, k, 8 + lo : 8 + hi, :] = p * r0 - q * r1
        f[1, k, 8 + lo : 8 + hi, :] = p * r1 + q * r0

    for k in range(HALO):
        for buf, corner, i, x in ((xlo, clo, HALO - 1 - k, HALO - 1 - k), (xhi, chi, k, HALO + cx + k)):
            place = low(x) if x < HALO else high(x)
            below, above = corner_plane(corner, k)
            for src, lo, hi in ((below, 0, y0), (buf[:, i], y0, y1), (above, y1, ey)):
                fill(place, lo, hi, src[2], src[3], src[4].astype(jnp.int32))
                first(place, x, lo, hi, src[0], src[1])

    def inner(x):
        i = x - HALO
        first(mine(x), x, 0, y0, ylo[0, i], ylo[1, i])
        first(mine(x), x, y0, y1, rhs[0, i], rhs[1, i])
        first(mine(x), x, y1, ey, yhi[0, i], yhi[1, i])

    planes(HALO, HALO + cx, inner)
    g0, g1 = centre(f, g, u, t, t_rim, (mine, low, high), HALO, s, ends, own, (0, ey), (0, ey))
    spread_rhs(g0, g1, cols, pad, out_ref, sq[...], grid)


def read_scalars(raw, olds, j):
    h = []
    for i in range(j):
        a0, a1 = pick(raw, 32 + 2 * i), pick(raw, 33 + 2 * i)
        for k in range(i):
            b0, b1 = pick(olds[i], 32 + 2 * k), pick(olds[i], 33 + 2 * k)
            a0, a1 = a0 - (b0 * h[k][0] + b1 * h[k][1]), a1 - (b0 * h[k][1] - b1 * h[k][0])
        inv = pick(olds[i], 41)
        h.append((a0 * inv, a1 * inv))
    sq = pick(raw, 40)
    for a0, a1 in h:
        sq = sq - (a0 * a0 + a1 * a1)
    length = jnp.sqrt(jnp.maximum(sq, 0.0) + epsilon)
    return h, length


def write_scalars(out, h, length, inv):
    lane = lanes((1, 128))
    row = jnp.where(lane == 40, length[0:1], inv[0:1])
    for k, pair in enumerate(h):
        for c in range(2):
            row = jnp.where(lane == 32 + 2 * k + c, pair[c][0:1], row)
    out[...] = row


def like(v, rows):
    return jnp.concatenate([v] * (rows // 8), axis=0)


def combine(scalars, new, old):
    h, inv = scalars
    a0, a1 = new
    rows = a0.shape[0]
    for i in range(len(h)):
        b0, b1 = old(i)
        r, q = like(h[i][0], rows), like(h[i][1], rows)
        a0 = a0 - (r * b0 - q * b1)
        a1 = a1 - (r * b1 + q * b0)
    s = like(inv, rows)
    return a0 * s, a1 * s


def splats(row, first):
    return [pick(row, first + k) for k in range(AGG)]


def marks(index):
    return [(index & 1) == 1, (index & 3) >= 2, (index & 7) >= 4, index >= 8]


def choose(values, bits):
    rows = bits[0].shape[0]
    level = [like(v, rows) for v in values]
    for bit in bits:
        level = [jnp.where(bit, level[k + 1], level[k]) for k in range(0, len(level), 2)]
    return level[0]


def prolong_plane(pc, k, ids, i, table, own, dx, values=None, wide_y=True):
    cy = own[1]
    ey = cy + 2 * HALO
    for dy, lo, hi in ((0, 0, HALO), (1, HALO, HALO + cy), (2, HALO + cy, ey)):
        n = dx * 3 + dy
        if dy != 1 and not wide_y:
            continue
        if values is not None and dy == 1:
            bits = marks(ids[i, lo:hi, :])
            for c in range(2):
                pc[c, k, 8 + lo : 8 + hi, :] = choose(values[c], bits)
            continue
        src = table[:, 128 * (n // 4) : 128 * (n // 4) + 128]
        index = ids[i, lo:hi, :] + 32 * (n % 4)
        pc[0, k, 8 + lo : 8 + hi, :] = take(src, index)
        pc[1, k, 8 + lo : 8 + hi, :] = take(src, index + AGG)


def image_plane(pc, k, coefs, t_in, m_old, scalars, lo, hi):
    i = coefs[1]
    a0, a1 = operate_plane(pc, k, coefs, lo, hi)
    m = combine(
        scalars,
        (t_in[0, i, lo:hi, :], t_in[1, i, lo:hi, :]),
        lambda n: (m_old[n][0, i, lo:hi, :], m_old[n][1, i, lo:hi, :]),
    )
    return m, (m[0] + a0, m[1] + a1)


def image_store(pc, u, f, k, coefs, t_in, m_old, scalars, m_out, lo, hi):
    m, (u0, u1) = image_plane(pc, k, coefs, t_in, m_old, scalars, lo, hi)
    refs, i = coefs
    if m_out is not None:
        m_out[0, i, lo:hi, :], m_out[1, i, lo:hi, :] = m
    p, q = refs[2][i, lo:hi, :], refs[3][i, lo:hi, :]
    u[0, k, lo:hi, :], u[1, k, lo:hi, :] = u0, u1
    f[0, k, 8 + lo : 8 + hi, :] = p * u0 - q * u1
    f[1, k, 8 + lo : 8 + hi, :] = p * u1 + q * u0
    return u0, u1


def step_kernel(j, grid, own, *refs):
    refs = list(refs)
    take_refs = lambda k: [refs.pop(0) for _ in range(k)]
    last = j == ITERS - 1
    rcv = refs.pop(0)
    home, rim = take_refs(5), take_refs(5)
    ends, cols, t_own, t_rim = take_refs(4)
    m_own, m_rim = take_refs(j), take_refs(0 if last else j)
    u_in, c_old, h_old = take_refs(j + 1), take_refs(j), take_refs(j)
    c_out, h_out, out_ref = take_refs(3)
    if not last:
        m_out, t, u_out, s_out = take_refs(4)
    mr_out = tr_out = None
    if j < ITERS - 2:
        mr_out, tr_out = take_refs(2)
    pc = refs.pop(0)
    if not last:
        u, f, pad = take_refs(3)
    cx, cy = own
    mine = lambda x: (home, x - HALO)
    low = lambda x: (rim, x)
    high = lambda x: (rim, x - cx)
    y0, y1 = HALO, HALO + cy
    halo = HALO - 2 - 2 * j
    rows = window(halo, cy)
    size = cx + 2 * HALO

    row = jnp.sum(rcv[...], axis=0, keepdims=True)
    h, length = read_scalars(row[:, 256:384], [r[...] for r in h_old], j)
    inv = 1.0 / length
    write_scalars(h_out, h, length, inv)
    scalars = h, inv
    wide = lambda v: jnp.concatenate([v[0:1]] * 3, axis=1)
    table = row
    for i in range(j):
        old = c_old[i][...]
        table = table - (wide(h[i][0]) * old + wide(h[i][1]) * turn_rows(old))
    table = table * wide(inv)
    c_out[...] = table

    for x in range(HALO - halo - 1, HALO):
        y = 2 * HALO - 1 - x
        wide_y = halo + 1 - (HALO - x) > 0
        prolong_plane(pc, x, rim[4], x, table, own, 0, wide_y=wide_y)
        prolong_plane(pc, y + cx, rim[4], y, table, own, 2, wide_y=wide_y)
    values = [splats(table[:, 128:256], AGG * c) for c in range(2)]
    planes(HALO, HALO + cx, lambda x: prolong_plane(pc, x, home[4], x - HALO, table, own, 1, values))

    def outer(k, c, far):
        image_store(pc, u, f, k, c, t_rim, m_rim, scalars, mr_out, *window(halo - far, cy))

    pairs(HALO - halo, size, outer, low, high)

    def middle(x, acc):
        i = x - HALO
        if last:
            u0, u1 = image_plane(pc, x, mine(x), t_own, m_own, scalars, y0, y1)[1]
        else:
            u0, u1 = image_store(pc, u, f, x, mine(x), t_own, m_own, scalars, m_out, *rows)
            lo = y0 - rows[0]
            u0, u1 = u0[lo : lo + cy], u1[lo : lo + cy]
            u_out[0, i], u_out[1, i] = u0, u1
        new = []
        for k in range(j + 1):
            b0, b1 = u_in[k][0, i], u_in[k][1, i]
            new.append(fold8(b0 * u0 + b1 * u1))
            new.append(fold8(b0 * u1 - b1 * u0))
        new.append(fold8(u0 * u0 + u1 * u1))
        return tuple(a + b for a, b in zip(acc, new))

    zero = jnp.zeros((8, 128), F32)
    acc = planes(HALO, HALO + cx, middle, (zero,) * (2 * j + 3))
    items = [(32 + k, acc[k]) for k in range(2 * j + 2)] + [(40, acc[-1])]
    dots = scalar_row(items)
    if last:
        n = out_ref.shape[0]
        for r in range(2):
            out_ref[:, 128 * r : 128 * r + 128] = jnp.zeros((n, 128), F32)
        out_ref[:, 256:384] = jnp.broadcast_to(dots, (n, 128))
        return
    t_rows = rows if j < ITERS - 2 else (y0, y1)
    g0, g1 = centre(f, pc, u, t, tr_out, (mine, low, high), halo, s_out, ends, own, rows, t_rows)
    spread_rhs(g0, g1, cols, pad, out_ref, dots, grid)


def pack_kernel(rhs, wave, layer, agg, ylow, yhigh, xlow, xhigh, yint, xint, sems):
    cx, cy = wave.shape[:2]
    every = slice(None)
    cuts = (
        (ylow, yint, 0, every, pl.ds(0, HALO)),
        (yhigh, yint, 2, every, pl.ds(cy - HALO, HALO)),
        (xlow, xint, 0, pl.ds(0, HALO), every),
        (xhigh, xint, 2, pl.ds(cx - HALO, HALO), every),
    )
    copies = []
    for k, (out, ints, slot, xs, ys) in enumerate(cuts):
        for i, (src, dst) in enumerate((
            (rhs.at[:, xs, ys, :], out.at[0:2]),
            (wave.at[xs, ys, :], out.at[2]),
            (layer.at[xs, ys, :], ints.at[slot]),
            (agg.at[xs, ys, :], ints.at[slot + 1]),
        )):
            copies.append(pltpu.make_async_copy(src, dst, sems.at[4 * k + i]))
    for copy in copies:
        copy.start()
    for copy in copies:
        copy.wait()
    for out, ints, slot, _, _ in cuts:
        out[3] = ints[slot].astype(F32)
        out[4] = ints[slot + 1].astype(F32)


def corner_kernel(ylo, yhi, low, high):
    cx = ylo.shape[1]
    row = lax.broadcasted_iota(jnp.int32, (5, HALO, ylo.shape[3]), 1)
    for out, plane in ((low, lambda k: k), (high, lambda k: cx - 1 - k)):
        for p in range(HALO // 2):
            a, b = plane(p), plane(HALO - 2 - p)
            out[:, p, 0:HALO, :] = jnp.where(row > p, ylo[:, a], pltpu.roll(ylo[:, b], p + 1, 1))
            out[:, p, HALO : 2 * HALO, :] = jnp.where(
                row < HALO - 1 - p, yhi[:, a], pltpu.roll(yhi[:, b], HALO - 1 - p, 1)
            )


def corner_plane(buf, k):
    if k == HALO - 1:
        zero = jnp.zeros((5, HALO, buf.shape[3]), F32)
        return zero, zero
    p = min(k, HALO - 2 - k)
    below, above = buf[:, p, 0:HALO, :], buf[:, p, HALO : 2 * HALO, :]
    if k != p:
        below, above = pltpu.roll(below, HALO - 1 - p, 1), pltpu.roll(above, p + 1, 1)
    return below, above


def columns_kernel(inverse, out, turned):
    turned[:, 0:32] = inverse[...].T
    group = lanes(out.shape) // 32
    total = jnp.zeros(out.shape, F32)
    for r in range(4):
        part = turned[pl.ds(r, out.shape[0], stride=4), :]
        part = jnp.where(group == 0, part, 0.0)
        total = total + (part if r == 0 else pltpu.roll(part, 32 * r, 1))
    out[...] = total


def arrange_kernel(got, out):
    n = got.shape[0] // 4
    for q in range(4):
        rows = got[pl.ds(q, n, stride=4), :]
        out[q * n : (q + 1) * n, :] = rows
        out[(4 + q) * n : (5 + q) * n, :] = turn(rows)


def cmul(a, b):
    return a[0] * b[0] - a[1] * b[1], a[0] * b[1] + a[1] * b[0]


def finish_kernel(own, *refs):
    rcv, ids = refs[0], refs[1]
    z = refs[2 : 2 + ITERS]
    c = refs[2 + ITERS : 2 + 2 * ITERS]
    rows = refs[2 + 2 * ITERS : 2 + 3 * ITERS]
    sol, hess = refs[2 + 3 * ITERS :]
    cx, cy = own
    final = jnp.sum(rcv[:, 256:384], axis=0, keepdims=True)
    scal = [r[...] for r in rows]
    beta = pick(scal[0], 40)
    upper, sub = [], []
    for j in range(1, ITERS):
        upper.append([(pick(scal[j], 32 + 2 * i), pick(scal[j], 33 + 2 * i)) for i in range(j)])
        sub.append(pick(scal[j], 40))
    h, length = read_scalars(final, scal, ITERS)
    upper.append(h)
    sub.append(length)
    r_i = lax.broadcasted_iota(jnp.int32, (8, 128), 0)
    c_i = lanes((8, 128))
    for comp in range(2):
        block = jnp.zeros((8, 128), F32)
        for j in range(ITERS):
            for i in range(j + 1):
                block = jnp.where((r_i == j) & (c_i == i), upper[j][i][comp], block)
            if comp == 0:
                block = jnp.where((r_i == j) & (c_i == j + 1), sub[j], block)
        hess[comp] = block[0:ITERS, 0 : ITERS + 1]
    zero = jnp.zeros((8, 128), F32)
    target = [(beta, zero)]
    rot = []
    tri = []
    for j in range(ITERS):
        col = list(upper[j])
        for i in range(j):
            cr, ci, s = rot[i]
            a, b = col[i], col[i + 1]
            up = cmul((cr, -ci), a)
            dn = cmul((cr, ci), b)
            col[i] = (up[0] + s * b[0], up[1] + s * b[1])
            col[i + 1] = (dn[0] - s * a[0], dn[1] - s * a[1])
        a = col[j]
        big = jnp.sqrt(a[0] * a[0] + a[1] * a[1] + sub[j] * sub[j])
        w = 1.0 / big
        cr, ci, s = a[0] * w, a[1] * w, sub[j] * w
        rot.append((cr, ci, s))
        g = target[j]
        target[j] = cmul((cr, -ci), g)
        target.append((-s * g[0], -s * g[1]))
        col[j] = big
        tri.append(col)
    y = [None] * ITERS
    for j in reversed(range(ITERS)):
        a0, a1 = target[j]
        for k in range(j + 1, ITERS):
            b = cmul(tri[k][j], y[k])
            a0, a1 = a0 - b[0], a1 - b[1]
        w = 1.0 / tri[j][j]
        y[j] = (a0 * w, a1 * w)
    table = jnp.zeros((1, 128), F32)
    for j in range(ITERS):
        old = c[j][:, 128:256]
        table = table + (y[j][0][0:1] * old + y[j][1][0:1] * turn(old))

    gamma = list(y)
    for j in reversed(range(ITERS)):
        w = 1.0 / (sub[j - 1] if j > 0 else beta)
        gamma[j] = (gamma[j][0] * w, gamma[j][1] * w)
        for i in range(j):
            b = cmul(upper[j - 1][i], gamma[j])
            gamma[i] = (gamma[i][0] - b[0], gamma[i][1] - b[1])

    values = splats(table, AGG)

    def go(i):
        index = ids[i, HALO : HALO + cy, :]
        a0, a1 = take(table, index), choose(values, marks(index))
        for j in range(ITERS):
            b = cmul((like(gamma[j][0], cy), like(gamma[j][1], cy)), (z[j][0, i], z[j][1, i]))
            a0, a1 = a0 + b[0], a1 + b[1]
        sol[0, i], sol[1, i] = a0, a1

    planes(0, cx, go)


def shape(*dims, dtype=F32):
    return jax.ShapeDtypeStruct(dims, dtype)


def call(kernel, outs, scratch, args, flops=100_000_000, space=pltpu.VMEM):
    return pl.pallas_call(
        kernel,
        out_shape=outs,
        in_specs=[pl.BlockSpec(memory_space=space)] * len(args),
        out_specs=[pl.BlockSpec(memory_space=pltpu.VMEM)] * len(outs),
        scratch_shapes=scratch,
        compiler_params=pltpu.CompilerParams(vmem_limit_bytes=VLIMIT),
        cost_estimate=pl.CostEstimate(flops=flops, bytes_accessed=1_000_000, transcendentals=0),
    )(*args)


def exchange(x):
    return lax.all_to_all(x, AXES, 0, 0, tiled=True)


def program(right_side, wavenumber, pml_layer, aggregate, coarse_inverse):
    gx, gy = lax.axis_size("gx"), lax.axis_size("gy")
    n = gx * gy
    cx, cy, cz = wavenumber.shape
    own = (cx, cy)
    ex, ey = cx + 2 * HALO, cy + 2 * HALO
    grid = (gx, gy)
    margin = -(-(gy + 1) // 8) * 8

    def swap(low, high, axis):
        count = lax.axis_size(axis)
        up = [(i, i + 1) for i in range(count - 1)]
        down = [(b, a) for a, b in up]
        low_in = lax.ppermute(high, axis, up)
        high_in = lax.ppermute(low, axis, down)
        return low_in, high_in

    strip, slab = shape(5, cx, HALO, cz), shape(5, HALO, cy, cz)
    ylow, yhigh, xlow, xhigh = call(
        pack_kernel, [strip, strip, slab, slab],
        [pltpu.VMEM((4, cx, HALO, cz), jnp.int32), pltpu.VMEM((4, HALO, cy, cz), jnp.int32), pltpu.SemaphoreType.DMA((16,))],
        [pltpu.with_memory_space_constraint(x, pltpu.HBM) for x in (right_side, wavenumber, pml_layer, aggregate)],
        space=pltpu.HBM,
    )
    ylo, yhi = swap(ylow, yhigh, "gy")
    xlo, xhi = swap(xlow, xhigh, "gx")
    (inverse,) = call(
        columns_kernel, [shape(4 * n, 128)], [pltpu.VMEM((AGG * n, 128), F32)],
        [coarse_inverse.reshape(2 * AGG, AGG * n)],
    )
    cols = exchange(inverse)
    right_side, wavenumber, pml_layer, aggregate, ylo, yhi, cols = lax.optimization_barrier(
        (right_side, wavenumber, pml_layer, aggregate, ylo, yhi, cols)
    )
    corner = shape(5, HALO // 2, 2 * HALO, cz)
    clow, chigh = call(corner_kernel, [corner, corner], [], [ylo, yhi])
    clo, chi = swap(clow, chigh, "gx")
    (cols,) = call(arrange_kernel, [shape(8 * n, 128)], [], [cols])
    I32 = jnp.int32
    home = [shape(cx, ey, cz)] * 4 + [shape(cx, ey, cz, dtype=I32)]
    rim = [shape(2 * HALO, ey, cz)] * 4 + [shape(2 * HALO, ey, cz, dtype=I32)]
    home2, rim2 = shape(2, cx, ey, cz), shape(2, 2 * HALO, ey, cz)
    mine = shape(2, cx, cy, cz)
    chunk = shape(n, 384)
    vmem = lambda *dims, dtype=F32: pltpu.VMEM(dims, dtype)
    tall = vmem(2, ex, ey + 16, cz)
    flat = vmem(2, ex, ey, cz)
    pad = vmem(n + 2 * margin, 128)

    *own_coefs, ends, sq = call(
        functools.partial(own_kernel, own),
        home + [shape(cx, cy, cz, dtype=I32), shape(1, 128)], [],
        [right_side, wavenumber, pml_layer, aggregate, ylo, yhi],
    )
    res = call(
        functools.partial(start_kernel, grid, own),
        rim + [home2, rim2, mine, chunk],
        [flat, tall, tall, pad],
        [right_side, ylo, yhi, xlo, xhi, clo, chi, cols, ends, sq] + own_coefs,
    )
    rim_coefs = list(res[:5])
    t_own, t_rim, s, send = res[5:]
    got = exchange(send)
    ms, mrs, us, ss, cs, hs = [], [], [right_side], [s], [], []
    for j in range(ITERS):
        last = j == ITERS - 1
        args = [got] + own_coefs + rim_coefs + [ends, cols, t_own, t_rim] + ms + ([] if last else mrs) + us + cs + hs
        outs = [shape(1, 384), shape(1, 128), chunk]
        scratch = [tall]
        if not last:
            outs += [home2, home2, mine, mine]
            if j < ITERS - 2:
                outs += [rim2, rim2]
            scratch += [flat, tall, pad]
        c, h, send, *rest = call(functools.partial(step_kernel, j, grid, own), outs, scratch, args)
        got = exchange(send)
        if not last:
            m, t_own, u, s = rest[:4]
            us.append(u)
            ms.append(m)
            ss.append(s)
            if j < ITERS - 2:
                mrs.append(rest[4])
                t_rim = rest[5]
        cs.append(c)
        hs.append(h)
    sol, hess = call(
        functools.partial(finish_kernel, own),
        [mine, shape(2, ITERS, ITERS + 1)],
        [],
        [got, own_coefs[4]] + ss + cs + hs,
    )
    return sol, jnp.swapaxes(hess, 1, 2)


def solution(mesh):
    return jax.shard_map(
        program,
        mesh=mesh,
        in_specs=(
            P(None, "gx", "gy", None),
            P("gx", "gy", None),
            P("gx", "gy", None),
            P("gx", "gy", None),
            P(None, ("gx", "gy"), None),
        ),
        out_specs=(P(None, "gx", "gy", None), P()),
        check_vma=False,
    )
```

```python
import functools

import jax
import jax.numpy as jnp
from jax import lax
from jax.experimental import pallas as pl
from jax.experimental.pallas import tpu as pltpu
from jax.sharding import PartitionSpec as P


ITERS = 4
HALO = 2 * ITERS
GROUP = 4
AXES = ("gx", "gy")
AGG = 16
damping = 0.8
pml_strength = 3.0
epsilon = 1e-06
F32 = jnp.float32
VLIMIT = 16 * 1024 * 1024


def lanes(shape):
    return lax.broadcasted_iota(jnp.int32, shape, len(shape) - 1)


def turn(x):
    odd = (lanes(x.shape) // AGG) % 2 == 1
    return jnp.where(odd, pltpu.roll(x, AGG, 1), -pltpu.roll(x, x.shape[1] - AGG, 1))


def turn_rows(x):
    parts = [turn(x[:, i : i + 128]) for i in range(0, x.shape[1], 128)]
    return jnp.concatenate(parts, axis=1)


def pick(row, lane):
    return jnp.broadcast_to(row[:, lane : lane + 1], (8, 128))


def take(table, index):
    rows = index.shape[0]
    src = jnp.broadcast_to(table, (rows, 128))
    return jnp.take_along_axis(src, index, axis=1, mode="promise_in_bounds")


def planes(lo, hi, fn, carry=None, width=16):
    count = hi - lo
    step = max(d for d in range(1, count + 1) if count % d == 0 and d <= width + width // 2)
    if step * 2 < width and count > width:
        step = width
    whole = count // step * step

    def go(i, c):
        for k in range(step):
            x = lo + i * step + k
            if carry is None:
                fn(x)
            else:
                c = fn(x, c)
        return c

    c = 0 if carry is None else carry
    if whole // step == 1:
        c = go(0, c)
    else:
        c = lax.fori_loop(0, whole // step, go, c)
    for x in range(lo + whole, hi):
        if carry is None:
            fn(x)
        else:
            c = fn(x, c)
    return c


def stencil(ref, c, x, y0, y1):
    mid = ref[c, x, 8 + y0 : 8 + y1, :]
    lane = lanes(mid.shape)
    last = mid.shape[-1] - 1
    total = jnp.where(lane == 0, 0.0, pltpu.roll(mid, 1, 1)) + jnp.where(lane == last, 0.0, pltpu.roll(mid, last, 1))
    total = total + (ref[c, x - 1, 8 + y0 : 8 + y1, :] + ref[c, x + 1, 8 + y0 : 8 + y1, :])
    return mid, total + (ref[c, x, 7 + y0 : 7 + y1, :] + ref[c, x, 9 + y0 : 9 + y1, :])


def operate_plane(ref, k, coefs, y0, y1):
    refs, i = coefs
    d = refs[0][i, y0:y1, :]
    a = refs[1][i, y0:y1, :]
    m0, t0 = stencil(ref, 0, k, y0, y1)
    m1, t1 = stencil(ref, 1, k, y0, y1)
    return d * m0 - t0 + a * m1, d * m1 - t1 - a * m0


def fold8(x):
    out = x[0:8]
    for i in range(8, x.shape[0], 8):
        out = out + x[i : i + 8]
    return out


def halves(x):
    top = x.astype(jnp.bfloat16)
    return jnp.concatenate([top, (x - top.astype(F32)).astype(jnp.bfloat16)], axis=1)


def below_ones():
    r = lax.broadcasted_iota(jnp.int32, (256, 128), 0) % 128
    return jnp.where(r <= lanes((256, 128)), 1.0, 0.0).astype(jnp.bfloat16)


def restrict(parts, ends, where, ones, acc):
    cy = parts[0][0].shape[0]
    sums = jnp.dot(
        jnp.concatenate([p for pair in parts for p in pair], axis=0), ones, preferred_element_type=F32
    )
    acc = list(acc)
    for k in range(len(parts)):
        index = ends[where[k]]
        for c in range(2):
            part = sums[cy * (2 * k + c) : cy * (2 * k + c + 1)]
            acc[c] = acc[c] + fold8(jnp.take_along_axis(part, index, axis=1, mode="promise_in_bounds"))
    return tuple(acc)


def spread_rhs(g0, g1, cols_ref, pad_ref, out_ref, scalars, grid):
    gx, gy = grid
    n = gx * gy
    lane = lanes((8, 128))
    acc = None
    for c, g in enumerate((g0, g1)):
        total = jnp.broadcast_to(jnp.sum(g, axis=0, keepdims=True), (8, 128))
        for q in range(4):
            source = lane // 32 + 4 * q
            below = jnp.take_along_axis(total, jnp.maximum(source - 1, 0), axis=1, mode="promise_in_bounds")
            weight = jnp.take_along_axis(total, source, axis=1, mode="promise_in_bounds")
            weight = weight - jnp.where(source == 0, 0.0, below)
            term = cols_ref[pl.ds((c * 4 + q) * n, n), :] * weight[0:1]
            acc = term if acc is None else acc + term
    whole = (acc + pltpu.roll(acc, 64, 1)) + (pltpu.roll(acc, 32, 1) + pltpu.roll(acc, 96, 1))
    margin = (pad_ref.shape[0] - n) // 2
    pad_ref[0:margin, :] = jnp.zeros((margin, 128), F32)
    pad_ref[margin + n : 2 * margin + n, :] = jnp.zeros((margin, 128), F32)
    pad_ref[margin : margin + n, :] = whole
    place = lax.broadcasted_iota(jnp.int32, (n, 128), 0) % gy
    group = lanes((n, 128)) // 32
    outs = [jnp.zeros((n, 128), F32) for _ in range(3)]
    for dx in (-1, 0, 1):
        for dy in (-1, 0, 1):
            k = (dx + 1) * 3 + dy + 1
            start = margin + dx * gy + dy
            piece = pad_ref[start : start + n, :]
            ok = (group == k % 4) & (place + dy >= 0) & (place + dy < gy)
            outs[k // 4] = jnp.where(ok, piece, outs[k // 4])
    outs[2] = outs[2] + jnp.broadcast_to(scalars, (n, 128))
    for r in range(4):
        out_ref[pl.ds(r, n, stride=4), :] = outs[r] if r < 3 else jnp.zeros((n, 128), F32)


def scalar_row(items):
    lane = lanes((1, 128))
    row = jnp.zeros((1, 128), F32)
    for where, acc in items:
        s = jnp.sum(jnp.sum(acc, axis=0, keepdims=True), axis=1, keepdims=True)
        row = jnp.where(lane == where, jnp.broadcast_to(s, (1, 128)), row)
    return row


def smooth_plane(f, g, u, k, coefs, y0, y1):
    a0, a1 = operate_plane(f, k, coefs, y0, y1)
    e0, e1 = u[0, k, y0:y1, :] - a0, u[1, k, y0:y1, :] - a1
    refs, i = coefs
    p, q = refs[2][i, y0:y1, :], refs[3][i, y0:y1, :]
    g[0, k, 8 + y0 : 8 + y1, :] = f[0, k, 8 + y0 : 8 + y1, :] + (p * e0 - q * e1)
    g[1, k, 8 + y0 : 8 + y1, :] = f[1, k, 8 + y0 : 8 + y1, :] + (p * e1 + q * e0)


def window(halo, cy):
    if halo > 4:
        return 0, cy + 2 * HALO
    if halo > 0:
        return HALO - 4, HALO + cy + 4
    return HALO, HALO + cy


def pairs(lo, size, fn, low, high):
    for x in range(lo, HALO):
        y = size - 1 - x
        fn(x, low(x), HALO - x)
        fn(y, high(y), HALO - x)


def centre(f, g, u, t, t_rim, places, halo, s, ends, own, rows, t_rows, inner=None):
    mine, low, high = places
    cx, cy = own
    size = cx + 2 * HALO
    y0, y1 = HALO, HALO + cy
    pairs(
        HALO - halo + 1, size,
        lambda k, c, far: smooth_plane(f, g, u, k, c, *window(halo - 1 - far, cy)), low, high,
    )
    for x in range(HALO, HALO + cx) if inner is None else (HALO, HALO + cx - 1):
        smooth_plane(f, g, u, x, mine(x), *rows)
    u_own = lambda i: (u[0, i + HALO, y0:y1, :], u[1, i + HALO, y0:y1, :])

    def outer(k, c, far):
        q0, q1 = window(halo - 2 - far, cy)
        a0, a1 = operate_plane(g, k, c, q0, q1)
        t_rim[0, c[1], q0:q1, :], t_rim[1, c[1], q0:q1, :] = a0, a1

    pairs(HALO - halo + 2, size, outer, low, high)

    ones = below_ones()

    def middle(b, acc):
        where = [b * GROUP + k for k in range(GROUP)]
        return last_planes(g, u_own, t, s, mine, where, ends, own, t_rows, ones, acc)

    zero = jnp.zeros((8, 128), F32)
    if inner is None:
        return planes(0, cx // GROUP, middle, (zero, zero), width=16 // GROUP)
    where = [0, 1, cx - 2, cx - 1]
    return last_planes(g, u_own, t, s, mine, where, ends, own, t_rows, ones, inner)


def last_planes(g, u_own, t, s, mine, where, ends, own, t_rows, ones, acc, shift=HALO):
    cy = own[1]
    y0, y1 = HALO, HALO + cy
    r0, r1 = t_rows
    parts = []
    for i in where:
        k = i + shift
        a0, a1 = operate_plane(g, k, mine(i + HALO), r0, r1)
        t[0, i, r0:r1, :], t[1, i, r0:r1, :] = a0, a1
        lo = y0 - r0
        s[0, i] = g[0, k, 8 + y0 : 8 + y1, :]
        s[1, i] = g[1, k, 8 + y0 : 8 + y1, :]
        v0, v1 = u_own(i)
        parts.append((halves(v0 - a0[lo : lo + cy]), halves(v1 - a1[lo : lo + cy])))
    return restrict(parts, ends, where, ones, acc)


def fill(store, y0, y1, wave, layer, a):
    sq = wave * wave
    ab = sq * (layer * layer * (pml_strength / 9.0))
    d = 6.0 - sq
    w = jnp.where(wave > 0.0, damping * pl.reciprocal(d * d + ab * ab), 0.0)
    refs, i = store
    refs[0][i, y0:y1, :] = d
    refs[1][i, y0:y1, :] = ab
    refs[2][i, y0:y1, :] = d * w
    refs[3][i, y0:y1, :] = ab * w
    refs[4][i, y0:y1, :] = a


def own_kernel(own, rhs, wave, layer, agg, ylo, yhi, diag, absorb, sre, sim, ids, ends, sq_out,
               t, s, share, g_edge, u, f, g):
    cx, cy = own
    ey = cy + 2 * HALO
    home = (diag, absorb, sre, sim, ids)

    def inner(i, acc):
        store = (home, i)
        fill(store, 0, HALO, ylo[2, i], ylo[3, i], ylo[4, i].astype(jnp.int32))
        fill(store, HALO + cy, ey, yhi[2, i], yhi[3, i], yhi[4, i].astype(jnp.int32))
        fill(store, HALO, HALO + cy, wave[i], layer[i].astype(F32), agg[i])
        r0, r1 = rhs[0, i], rhs[1, i]
        return acc + fold8(r0 * r0 + r1 * r1)

    sq = planes(0, cx, inner, jnp.zeros((8, 128), F32), width=8)
    sq_out[...] = scalar_row([(40, sq)])

    def find(i):
        a = agg[i]
        lane = lanes(a.shape)
        low = jnp.zeros(a.shape, jnp.int32)
        step = a.shape[1] // 2
        while step >= 1:
            probe = low + step
            val = jnp.take_along_axis(a, probe - 1, axis=1, mode="promise_in_bounds")
            low = jnp.where(val <= lane, probe, low)
            step //= 2
        val = jnp.take_along_axis(a, low, axis=1, mode="promise_in_bounds")
        low = jnp.where(val <= lane, low + 1, low)
        ends[i] = jnp.maximum(low - 1, 0)

    planes(0, cx, find, width=8)

    def first(i, lo, hi, r0, r1):
        p, q = sre[i, lo:hi, :], sim[i, lo:hi, :]
        u[0, i, lo:hi, :] = r0
        u[1, i, lo:hi, :] = r1
        f[0, i, 8 + lo : 8 + hi, :] = p * r0 - q * r1
        f[1, i, 8 + lo : 8 + hi, :] = p * r1 + q * r0

    for i in range(cx):
        first(i, 0, HALO, ylo[0, i], ylo[1, i])
        first(i, HALO, HALO + cy, rhs[0, i], rhs[1, i])
        first(i, HALO + cy, ey, yhi[0, i], yhi[1, i])
    for i in range(1, cx - 1):
        smooth_plane(f, g, u, i, (home, i), 0, ey)
    for k, i in enumerate((1, 2, cx - 3, cx - 2)):
        for c in range(2):
            g_edge[c, k] = g[c, i]
    zero = jnp.zeros((8, 128), F32)
    acc = zero, zero
    ones = below_ones()
    for b in range(2, cx - 2, GROUP):
        acc = last_planes(
            g, lambda i: (rhs[0, i], rhs[1, i]), t, s, lambda x: (home, x - HALO),
            list(range(b, b + GROUP)), ends, own, (0, ey), ones, acc, shift=0,
        )
    for i in (1, cx - 2):
        for c in range(2):
            s[c, i] = g[c, i, 8 + HALO : 8 + HALO + cy, :]
    share[0:8, :], share[8:16, :] = acc


def start_kernel(grid, own, *refs):
    rhs, ylo, yhi, xlo, xhi, clo, chi, cols, ends, sq, _, _, share, g_edge = refs[:14]
    home, rim = refs[14:19], refs[19:24]
    t, t_rim, s, out_ref, u, f, g, pad = refs[24:]
    cx, cy = own
    ey = cy + 2 * HALO
    y0, y1 = HALO, HALO + cy
    mine = lambda x: (home, x - HALO)
    low = lambda x: (rim, x)
    high = lambda x: (rim, x - cx)

    def first(place, k, lo, hi, r0, r1):
        refs, i = place
        p, q = refs[2][i, lo:hi, :], refs[3][i, lo:hi, :]
        u[0, k, lo:hi, :] = r0
        u[1, k, lo:hi, :] = r1
        f[0, k, 8 + lo : 8 + hi, :] = p * r0 - q * r1
        f[1, k, 8 + lo : 8 + hi, :] = p * r1 + q * r0

    for k in range(HALO):
        for buf, corner, i, x in ((xlo, clo, HALO - 1 - k, HALO - 1 - k), (xhi, chi, k, HALO + cx + k)):
            place = low(x) if x < HALO else high(x)
            below, above = corner_plane(corner, k)
            for src, lo, hi in ((below, 0, y0), (buf[:, i], y0, y1), (above, y1, ey)):
                fill(place, lo, hi, src[2], src[3], src[4].astype(jnp.int32))
                first(place, x, lo, hi, src[0], src[1])

    def inner(x):
        i = x - HALO
        first(mine(x), x, 0, y0, ylo[0, i], ylo[1, i])
        first(mine(x), x, y0, y1, rhs[0, i], rhs[1, i])
        first(mine(x), x, y1, ey, yhi[0, i], yhi[1, i])

    for i in (0, 1, cx - 2, cx - 1):
        inner(HALO + i)
    for k, i in enumerate((1, 2, cx - 3, cx - 2)):
        for c in range(2):
            g[c, HALO + i] = g_edge[c, k]
    g0, g1 = centre(
        f, g, u, t, t_rim, (mine, low, high), HALO, s, ends, own, (0, ey), (0, ey), (share[0:8, :], share[8:16, :])
    )
    spread_rhs(g0, g1, cols, pad, out_ref, sq[...], grid)


def read_scalars(raw, olds, j):
    h = []
    for i in range(j):
        a0, a1 = pick(raw, 32 + 2 * i), pick(raw, 33 + 2 * i)
        for k in range(i):
            b0, b1 = pick(olds[i], 32 + 2 * k), pick(olds[i], 33 + 2 * k)
            a0, a1 = a0 - (b0 * h[k][0] + b1 * h[k][1]), a1 - (b0 * h[k][1] - b1 * h[k][0])
        inv = pick(olds[i], 41)
        h.append((a0 * inv, a1 * inv))
    sq = pick(raw, 40)
    for a0, a1 in h:
        sq = sq - (a0 * a0 + a1 * a1)
    length = jnp.sqrt(jnp.maximum(sq, 0.0) + epsilon)
    return h, length


def write_scalars(out, h, length, inv):
    lane = lanes((1, 128))
    row = jnp.where(lane == 40, length[0:1], inv[0:1])
    for k, pair in enumerate(h):
        for c in range(2):
            row = jnp.where(lane == 32 + 2 * k + c, pair[c][0:1], row)
    out[...] = row


def like(v, rows):
    return jnp.concatenate([v] * (rows // 8), axis=0)


def combine(scalars, new, old):
    h, inv = scalars
    a0, a1 = new
    rows = a0.shape[0]
    for i in range(len(h)):
        b0, b1 = old(i)
        r, q = like(h[i][0], rows), like(h[i][1], rows)
        a0 = a0 - (r * b0 - q * b1)
        a1 = a1 - (r * b1 + q * b0)
    s = like(inv, rows)
    return a0 * s, a1 * s


def splats(row, first):
    return [pick(row, first + k) for k in range(AGG)]


def marks(index):
    return [(index & 1) == 1, (index & 3) >= 2, (index & 7) >= 4, index >= 8]


def choose(values, bits):
    rows = bits[0].shape[0]
    level = [like(v, rows) for v in values]
    for bit in bits:
        level = [jnp.where(bit, level[k + 1], level[k]) for k in range(0, len(level), 2)]
    return level[0]


def prolong_plane(pc, k, ids, i, table, own, dx, values=None, wide_y=True):
    cy = own[1]
    ey = cy + 2 * HALO
    for dy, lo, hi in ((0, 0, HALO), (1, HALO, HALO + cy), (2, HALO + cy, ey)):
        n = dx * 3 + dy
        if dy != 1 and not wide_y:
            continue
        if values is not None and dy == 1:
            bits = marks(ids[i, lo:hi, :])
            for c in range(2):
                pc[c, k, 8 + lo : 8 + hi, :] = choose(values[c], bits)
            continue
        src = table[:, 128 * (n // 4) : 128 * (n // 4) + 128]
        index = ids[i, lo:hi, :] + 32 * (n % 4)
        pc[0, k, 8 + lo : 8 + hi, :] = take(src, index)
        pc[1, k, 8 + lo : 8 + hi, :] = take(src, index + AGG)


def image_plane(pc, k, coefs, t_in, m_old, scalars, lo, hi):
    i = coefs[1]
    a0, a1 = operate_plane(pc, k, coefs, lo, hi)
    m = combine(
        scalars,
        (t_in[0, i, lo:hi, :], t_in[1, i, lo:hi, :]),
        lambda n: (m_old[n][0, i, lo:hi, :], m_old[n][1, i, lo:hi, :]),
    )
    return m, (m[0] + a0, m[1] + a1)


def image_store(pc, u, f, k, coefs, t_in, m_old, scalars, m_out, lo, hi):
    m, (u0, u1) = image_plane(pc, k, coefs, t_in, m_old, scalars, lo, hi)
    refs, i = coefs
    if m_out is not None:
        m_out[0, i, lo:hi, :], m_out[1, i, lo:hi, :] = m
    p, q = refs[2][i, lo:hi, :], refs[3][i, lo:hi, :]
    u[0, k, lo:hi, :], u[1, k, lo:hi, :] = u0, u1
    f[0, k, 8 + lo : 8 + hi, :] = p * u0 - q * u1
    f[1, k, 8 + lo : 8 + hi, :] = p * u1 + q * u0
    return u0, u1


def step_kernel(j, grid, own, *refs):
    refs = list(refs)
    take_refs = lambda k: [refs.pop(0) for _ in range(k)]
    last = j == ITERS - 1
    rcv = refs.pop(0)
    home, rim = take_refs(5), take_refs(5)
    ends, cols, t_own, t_rim = take_refs(4)
    m_own, m_rim = take_refs(j), take_refs(0 if last else j)
    u_in, c_old, h_old = take_refs(j + 1), take_refs(j), take_refs(j)
    c_out, h_out, out_ref = take_refs(3)
    if not last:
        m_out, t, u_out, s_out = take_refs(4)
    mr_out = tr_out = None
    if j < ITERS - 2:
        mr_out, tr_out = take_refs(2)
    pc = refs.pop(0)
    if not last:
        u, f, pad = take_refs(3)
    cx, cy = own
    mine = lambda x: (home, x - HALO)
    low = lambda x: (rim, x)
    high = lambda x: (rim, x - cx)
    y0, y1 = HALO, HALO + cy
    halo = HALO - 2 - 2 * j
    rows = window(halo, cy)
    size = cx + 2 * HALO

    n = rcv.shape[0] // 4
    row = jnp.concatenate(
        [jnp.sum(rcv[pl.ds(r, n, stride=4), :], axis=0, keepdims=True) for r in range(3)], axis=1
    )
    h, length = read_scalars(row[:, 256:384], [r[...] for r in h_old], j)
    inv = 1.0 / length
    write_scalars(h_out, h, length, inv)
    scalars = h, inv
    wide = lambda v: jnp.concatenate([v[0:1]] * 3, axis=1)
    table = row
    for i in range(j):
        old = c_old[i][...]
        table = table - (wide(h[i][0]) * old + wide(h[i][1]) * turn_rows(old))
    table = table * wide(inv)
    c_out[...] = table

    for x in range(HALO - halo - 1, HALO):
        y = 2 * HALO - 1 - x
        wide_y = halo + 1 - (HALO - x) > 0
        prolong_plane(pc, x, rim[4], x, table, own, 0, wide_y=wide_y)
        prolong_plane(pc, y + cx, rim[4], y, table, own, 2, wide_y=wide_y)
    values = [splats(table[:, 128:256], AGG * c) for c in range(2)]
    planes(HALO, HALO + cx, lambda x: prolong_plane(pc, x, home[4], x - HALO, table, own, 1, values))

    def outer(k, c, far):
        image_store(pc, u, f, k, c, t_rim, m_rim, scalars, mr_out, *window(halo - far, cy))

    pairs(HALO - halo, size, outer, low, high)

    def middle(x, acc):
        i = x - HALO
        if last:
            u0, u1 = image_plane(pc, x, mine(x), t_own, m_own, scalars, y0, y1)[1]
        else:
            u0, u1 = image_store(pc, u, f, x, mine(x), t_own, m_own, scalars, m_out, *rows)
            lo = y0 - rows[0]
            u0, u1 = u0[lo : lo + cy], u1[lo : lo + cy]
            u_out[0, i], u_out[1, i] = u0, u1
        new = []
        for k in range(j + 1):
            b0, b1 = u_in[k][0, i], u_in[k][1, i]
            new.append(fold8(b0 * u0 + b1 * u1))
            new.append(fold8(b0 * u1 - b1 * u0))
        new.append(fold8(u0 * u0 + u1 * u1))
        return tuple(a + b for a, b in zip(acc, new))

    zero = jnp.zeros((8, 128), F32)
    acc = planes(HALO, HALO + cx, middle, (zero,) * (2 * j + 3))
    items = [(32 + k, acc[k]) for k in range(2 * j + 2)] + [(40, acc[-1])]
    dots = scalar_row(items)
    if last:
        out_ref[...] = jnp.broadcast_to(dots, out_ref.shape)
        return
    t_rows = rows if j < ITERS - 2 else (y0, y1)
    g0, g1 = centre(f, pc, u, t, tr_out, (mine, low, high), halo, s_out, ends, own, rows, t_rows)
    spread_rhs(g0, g1, cols, pad, out_ref, dots, grid)


def pack_kernel(rhs, wave, layer, agg, ylow, yhigh, xlow, xhigh, yint, xint, sems):
    cx, cy = wave.shape[:2]
    every = slice(None)
    cuts = (
        (ylow, yint, 0, every, pl.ds(0, HALO)),
        (yhigh, yint, 2, every, pl.ds(cy - HALO, HALO)),
        (xlow, xint, 0, pl.ds(0, HALO), every),
        (xhigh, xint, 2, pl.ds(cx - HALO, HALO), every),
    )
    copies = []
    for k, (out, ints, slot, xs, ys) in enumerate(cuts):
        for i, (src, dst) in enumerate((
            (rhs.at[:, xs, ys, :], out.at[0:2]),
            (wave.at[xs, ys, :], out.at[2]),
            (layer.at[xs, ys, :], ints.at[slot]),
            (agg.at[xs, ys, :], ints.at[slot + 1]),
        )):
            copies.append(pltpu.make_async_copy(src, dst, sems.at[4 * k + i]))
    for copy in copies:
        copy.start()
    for copy in copies:
        copy.wait()
    for out, ints, slot, _, _ in cuts:
        out[3] = ints[slot].astype(F32)
        out[4] = ints[slot + 1].astype(F32)


def corner_kernel(ylo, yhi, low, high):
    cx = ylo.shape[1]
    row = lax.broadcasted_iota(jnp.int32, (5, HALO, ylo.shape[3]), 1)
    for out, plane in ((low, lambda k: k), (high, lambda k: cx - 1 - k)):
        for p in range(HALO // 2):
            a, b = plane(p), plane(HALO - 2 - p)
            out[:, p, 0:HALO, :] = jnp.where(row > p, ylo[:, a], pltpu.roll(ylo[:, b], p + 1, 1))
            out[:, p, HALO : 2 * HALO, :] = jnp.where(
                row < HALO - 1 - p, yhi[:, a], pltpu.roll(yhi[:, b], HALO - 1 - p, 1)
            )


def corner_plane(buf, k):
    if k == HALO - 1:
        zero = jnp.zeros((5, HALO, buf.shape[3]), F32)
        return zero, zero
    p = min(k, HALO - 2 - k)
    below, above = buf[:, p, 0:HALO, :], buf[:, p, HALO : 2 * HALO, :]
    if k != p:
        below, above = pltpu.roll(below, HALO - 1 - p, 1), pltpu.roll(above, p + 1, 1)
    return below, above


def columns_kernel(inverse, out, turned):
    turned[:, 0:32] = inverse[...].T
    group = lanes(out.shape) // 32
    total = jnp.zeros(out.shape, F32)
    for r in range(4):
        part = turned[pl.ds(r, out.shape[0], stride=4), :]
        part = jnp.where(group == 0, part, 0.0)
        total = total + (part if r == 0 else pltpu.roll(part, 32 * r, 1))
    out[...] = total


def arrange_kernel(got, out):
    n = got.shape[0] // 4
    for q in range(4):
        rows = got[pl.ds(q, n, stride=4), :]
        out[q * n : (q + 1) * n, :] = rows
        out[(4 + q) * n : (5 + q) * n, :] = turn(rows)


def cmul(a, b):
    return a[0] * b[0] - a[1] * b[1], a[0] * b[1] + a[1] * b[0]


def finish_kernel(own, *refs):
    rcv, ids = refs[0], refs[1]
    z = refs[2 : 2 + ITERS]
    c = refs[2 + ITERS : 2 + 2 * ITERS]
    rows = refs[2 + 2 * ITERS : 2 + 3 * ITERS]
    sol, hess = refs[2 + 3 * ITERS :]
    cx, cy = own
    final = jnp.sum(rcv[pl.ds(2, rcv.shape[0] // 4, stride=4), :], axis=0, keepdims=True)
    scal = [r[...] for r in rows]
    beta = pick(scal[0], 40)
    upper, sub = [], []
    for j in range(1, ITERS):
        upper.append([(pick(scal[j], 32 + 2 * i), pick(scal[j], 33 + 2 * i)) for i in range(j)])
        sub.append(pick(scal[j], 40))
    h, length = read_scalars(final, scal, ITERS)
    upper.append(h)
    sub.append(length)
    r_i = lax.broadcasted_iota(jnp.int32, (8, 128), 0)
    c_i = lanes((8, 128))
    for comp in range(2):
        block = jnp.zeros((8, 128), F32)
        for j in range(ITERS):
            for i in range(j + 1):
                block = jnp.where((r_i == j) & (c_i == i), upper[j][i][comp], block)
            if comp == 0:
                block = jnp.where((r_i == j) & (c_i == j + 1), sub[j], block)
        hess[comp] = block[0:ITERS, 0 : ITERS + 1]
    zero = jnp.zeros((8, 128), F32)
    target = [(beta, zero)]
    rot = []
    tri = []
    for j in range(ITERS):
        col = list(upper[j])
        for i in range(j):
            cr, ci, s = rot[i]
            a, b = col[i], col[i + 1]
            up = cmul((cr, -ci), a)
            dn = cmul((cr, ci), b)
            col[i] = (up[0] + s * b[0], up[1] + s * b[1])
            col[i + 1] = (dn[0] - s * a[0], dn[1] - s * a[1])
        a = col[j]
        big = jnp.sqrt(a[0] * a[0] + a[1] * a[1] + sub[j] * sub[j])
        w = 1.0 / big
        cr, ci, s = a[0] * w, a[1] * w, sub[j] * w
        rot.append((cr, ci, s))
        g = target[j]
        target[j] = cmul((cr, -ci), g)
        target.append((-s * g[0], -s * g[1]))
        col[j] = big
        tri.append(col)
    y = [None] * ITERS
    for j in reversed(range(ITERS)):
        a0, a1 = target[j]
        for k in range(j + 1, ITERS):
            b = cmul(tri[k][j], y[k])
            a0, a1 = a0 - b[0], a1 - b[1]
        w = 1.0 / tri[j][j]
        y[j] = (a0 * w, a1 * w)
    table = jnp.zeros((1, 128), F32)
    for j in range(ITERS):
        old = c[j][:, 128:256]
        table = table + (y[j][0][0:1] * old + y[j][1][0:1] * turn(old))

    gamma = list(y)
    for j in reversed(range(ITERS)):
        w = 1.0 / (sub[j - 1] if j > 0 else beta)
        gamma[j] = (gamma[j][0] * w, gamma[j][1] * w)
        for i in range(j):
            b = cmul(upper[j - 1][i], gamma[j])
            gamma[i] = (gamma[i][0] - b[0], gamma[i][1] - b[1])

    values = splats(table, AGG)

    def go(i):
        index = ids[i, HALO : HALO + cy, :]
        a0, a1 = take(table, index), choose(values, marks(index))
        for j in range(ITERS):
            b = cmul((like(gamma[j][0], cy), like(gamma[j][1], cy)), (z[j][0, i], z[j][1, i]))
            a0, a1 = a0 + b[0], a1 + b[1]
        sol[0, i], sol[1, i] = a0, a1

    planes(0, cx, go)


def shape(*dims, dtype=F32):
    return jax.ShapeDtypeStruct(dims, dtype)


def call(kernel, outs, scratch, args, flops=100_000_000, space=pltpu.VMEM, aliases=None):
    return pl.pallas_call(
        kernel,
        out_shape=outs,
        in_specs=[pl.BlockSpec(memory_space=space)] * len(args),
        out_specs=[pl.BlockSpec(memory_space=pltpu.VMEM)] * len(outs),
        scratch_shapes=scratch,
        input_output_aliases=aliases or {},
        compiler_params=pltpu.CompilerParams(vmem_limit_bytes=VLIMIT),
        cost_estimate=pl.CostEstimate(flops=flops, bytes_accessed=1_000_000, transcendentals=0),
    )(*args)


def exchange(x):
    return lax.all_to_all(x, AXES, 0, 0, tiled=True)


def program(right_side, wavenumber, pml_layer, aggregate, coarse_inverse):
    gx, gy = lax.axis_size("gx"), lax.axis_size("gy")
    n = gx * gy
    cx, cy, cz = wavenumber.shape
    own = (cx, cy)
    ex, ey = cx + 2 * HALO, cy + 2 * HALO
    grid = (gx, gy)
    margin = -(-(gy + 1) // 8) * 8

    def swap(low, high, axis):
        count = lax.axis_size(axis)
        up = [(i, i + 1) for i in range(count - 1)]
        down = [(b, a) for a, b in up]
        low_in = lax.ppermute(high, axis, up)
        high_in = lax.ppermute(low, axis, down)
        return low_in, high_in

    strip, slab = shape(5, cx, HALO, cz), shape(5, HALO, cy, cz)
    ylow, yhigh, xlow, xhigh = call(
        pack_kernel, [strip, strip, slab, slab],
        [pltpu.VMEM((4, cx, HALO, cz), jnp.int32), pltpu.VMEM((4, HALO, cy, cz), jnp.int32), pltpu.SemaphoreType.DMA((16,))],
        [pltpu.with_memory_space_constraint(x, pltpu.HBM) for x in (right_side, wavenumber, pml_layer, aggregate)],
        space=pltpu.HBM,
    )
    ylo, yhi = swap(ylow, yhigh, "gy")
    xlo, xhi = swap(xlow, xhigh, "gx")
    (inverse,) = call(
        columns_kernel, [shape(4 * n, 128)], [pltpu.VMEM((AGG * n, 128), F32)],
        [coarse_inverse.reshape(2 * AGG, AGG * n)],
    )
    cols = exchange(inverse)
    right_side, wavenumber, pml_layer, aggregate, ylo, yhi, cols = lax.optimization_barrier(
        (right_side, wavenumber, pml_layer, aggregate, ylo, yhi, cols)
    )
    corner = shape(5, HALO // 2, 2 * HALO, cz)
    clow, chigh = call(corner_kernel, [corner, corner], [], [ylo, yhi])
    clo, chi = swap(clow, chigh, "gx")
    (cols,) = call(arrange_kernel, [shape(8 * n, 128)], [], [cols])
    I32 = jnp.int32
    home = [shape(cx, ey, cz)] * 4 + [shape(cx, ey, cz, dtype=I32)]
    rim = [shape(2 * HALO, ey, cz)] * 4 + [shape(2 * HALO, ey, cz, dtype=I32)]
    home2, rim2 = shape(2, cx, ey, cz), shape(2, 2 * HALO, ey, cz)
    mine = shape(2, cx, cy, cz)
    chunk = shape(4 * n, 128)
    vmem = lambda *dims, dtype=F32: pltpu.VMEM(dims, dtype)
    tall = vmem(2, ex, ey + 16, cz)
    flat = vmem(2, ex, ey, cz)
    pad = vmem(n + 2 * margin, 128)

    short_tall = vmem(2, cx, ey + 16, cz)
    *own_coefs, ends, sq, t_own, s, share, g_edge = call(
        functools.partial(own_kernel, own),
        home + [shape(cx, cy, cz, dtype=I32), shape(1, 128), home2, mine, shape(16, 128), shape(2, 4, ey + 16, cz)],
        [vmem(2, cx, ey, cz), short_tall, short_tall],
        [right_side, wavenumber, pml_layer, aggregate, ylo, yhi],
    )
    res = call(
        functools.partial(start_kernel, grid, own),
        rim + [home2, rim2, mine, chunk],
        [flat, tall, tall, pad],
        [right_side, ylo, yhi, xlo, xhi, clo, chi, cols, ends, sq, t_own, s, share, g_edge] + own_coefs,
        aliases={10: 5, 11: 7},
    )
    rim_coefs = list(res[:5])
    t_own, t_rim, s, send = res[5:]
    got = exchange(send)
    ms, mrs, us, ss, cs, hs = [], [], [right_side], [s], [], []
    for j in range(ITERS):
        last = j == ITERS - 1
        args = [got] + own_coefs + rim_coefs + [ends, cols, t_own, t_rim] + ms + ([] if last else mrs) + us + cs + hs
        outs = [shape(1, 384), shape(1, 128), chunk]
        scratch = [tall]
        if not last:
            outs += [home2, home2, mine, mine]
            if j < ITERS - 2:
                outs += [rim2, rim2]
            scratch += [flat, tall, pad]
        c, h, send, *rest = call(functools.partial(step_kernel, j, grid, own), outs, scratch, args)
        got = exchange(send)
        if not last:
            m, t_own, u, s = rest[:4]
            us.append(u)
            ms.append(m)
            ss.append(s)
            if j < ITERS - 2:
                mrs.append(rest[4])
                t_rim = rest[5]
        cs.append(c)
        hs.append(h)
    sol, hess = call(
        functools.partial(finish_kernel, own),
        [mine, shape(2, ITERS, ITERS + 1)],
        [],
        [got, own_coefs[4]] + ss + cs + hs,
    )
    return sol, jnp.swapaxes(hess, 1, 2)


def solution(mesh):
    return jax.shard_map(
        program,
        mesh=mesh,
        in_specs=(
            P(None, "gx", "gy", None),
            P("gx", "gy", None),
            P("gx", "gy", None),
            P("gx", "gy", None),
            P(None, ("gx", "gy"), None),
        ),
        out_specs=(P(None, "gx", "gy", None), P()),
        check_vma=False,
    )
```

```python
import functools

import jax
import jax.numpy as jnp
from jax import lax
from jax.experimental import pallas as pl
from jax.experimental.pallas import tpu as pltpu
from jax.sharding import PartitionSpec as P


ITERS = 4
HALO = 2 * ITERS
GROUP = 4
AXES = ("gx", "gy")
AGG = 16
damping = 0.8
pml_strength = 3.0
epsilon = 1e-06
F32 = jnp.float32
VLIMIT = 16 * 1024 * 1024


def lanes(shape):
    return lax.broadcasted_iota(jnp.int32, shape, len(shape) - 1)


def turn(x):
    odd = (lanes(x.shape) // AGG) % 2 == 1
    return jnp.where(odd, pltpu.roll(x, AGG, 1), -pltpu.roll(x, x.shape[1] - AGG, 1))


def turn_rows(x):
    parts = [turn(x[:, i : i + 128]) for i in range(0, x.shape[1], 128)]
    return jnp.concatenate(parts, axis=1)


def pick(row, lane):
    return jnp.broadcast_to(row[:, lane : lane + 1], (8, 128))


def take(table, index):
    rows = index.shape[0]
    src = jnp.broadcast_to(table, (rows, 128))
    return jnp.take_along_axis(src, index, axis=1, mode="promise_in_bounds")


def planes(lo, hi, fn, carry=None, width=16):
    count = hi - lo
    step = max(d for d in range(1, count + 1) if count % d == 0 and d <= width + width // 2)
    if step * 2 < width and count > width:
        step = width
    whole = count // step * step

    def go(i, c):
        for k in range(step):
            x = lo + i * step + k
            if carry is None:
                fn(x)
            else:
                c = fn(x, c)
        return c

    c = 0 if carry is None else carry
    if whole // step == 1:
        c = go(0, c)
    else:
        c = lax.fori_loop(0, whole // step, go, c)
    for x in range(lo + whole, hi):
        if carry is None:
            fn(x)
        else:
            c = fn(x, c)
    return c


def stencil(ref, c, x, y0, y1):
    mid = ref[c, x, 8 + y0 : 8 + y1, :]
    lane = lanes(mid.shape)
    last = mid.shape[-1] - 1
    total = jnp.where(lane == 0, 0.0, pltpu.roll(mid, 1, 1)) + jnp.where(lane == last, 0.0, pltpu.roll(mid, last, 1))
    total = total + (ref[c, x - 1, 8 + y0 : 8 + y1, :] + ref[c, x + 1, 8 + y0 : 8 + y1, :])
    return mid, total + (ref[c, x, 7 + y0 : 7 + y1, :] + ref[c, x, 9 + y0 : 9 + y1, :])


def operate_plane(ref, k, coefs, y0, y1):
    refs, i = coefs
    d = refs[0][i, y0:y1, :]
    a = refs[1][i, y0:y1, :]
    m0, t0 = stencil(ref, 0, k, y0, y1)
    m1, t1 = stencil(ref, 1, k, y0, y1)
    return d * m0 - t0 + a * m1, d * m1 - t1 - a * m0


def fold8(x):
    out = x[0:8]
    for i in range(8, x.shape[0], 8):
        out = out + x[i : i + 8]
    return out


def halves(x):
    top = x.astype(jnp.bfloat16)
    return jnp.concatenate([top, (x - top.astype(F32)).astype(jnp.bfloat16)], axis=1)


def below_ones():
    r = lax.broadcasted_iota(jnp.int32, (256, 128), 0) % 128
    return jnp.where(r <= lanes((256, 128)), 1.0, 0.0).astype(jnp.bfloat16)


def restrict(parts, ends, where, ones, acc):
    cy = parts[0][0].shape[0]
    sums = jnp.dot(
        jnp.concatenate([p for pair in parts for p in pair], axis=0), ones, preferred_element_type=F32
    )
    acc = list(acc)
    for k in range(len(parts)):
        index = ends[where[k]]
        for c in range(2):
            part = sums[cy * (2 * k + c) : cy * (2 * k + c + 1)]
            acc[c] = acc[c] + fold8(jnp.take_along_axis(part, index, axis=1, mode="promise_in_bounds"))
    return tuple(acc)


def spread_rhs(g0, g1, cols_ref, pad_ref, out_ref, scalars, grid):
    gx, gy = grid
    n = gx * gy
    lane = lanes((8, 128))
    acc = None
    for c, g in enumerate((g0, g1)):
        total = jnp.broadcast_to(jnp.sum(g, axis=0, keepdims=True), (8, 128))
        for q in range(4):
            source = lane // 32 + 4 * q
            below = jnp.take_along_axis(total, jnp.maximum(source - 1, 0), axis=1, mode="promise_in_bounds")
            weight = jnp.take_along_axis(total, source, axis=1, mode="promise_in_bounds")
            weight = weight - jnp.where(source == 0, 0.0, below)
            term = cols_ref[pl.ds((c * 4 + q) * n, n), :] * weight[0:1]
            acc = term if acc is None else acc + term
    whole = (acc + pltpu.roll(acc, 64, 1)) + (pltpu.roll(acc, 32, 1) + pltpu.roll(acc, 96, 1))
    margin = (pad_ref.shape[0] - n) // 2
    pad_ref[0:margin, :] = jnp.zeros((margin, 128), F32)
    pad_ref[margin + n : 2 * margin + n, :] = jnp.zeros((margin, 128), F32)
    pad_ref[margin : margin + n, :] = whole
    place = lax.broadcasted_iota(jnp.int32, (n, 128), 0) % gy
    group = lanes((n, 128)) // 32
    outs = [jnp.zeros((n, 128), F32) for _ in range(3)]
    for dx in (-1, 0, 1):
        for dy in (-1, 0, 1):
            k = (dx + 1) * 3 + dy + 1
            start = margin + dx * gy + dy
            piece = pad_ref[start : start + n, :]
            ok = (group == k % 4) & (place + dy >= 0) & (place + dy < gy)
            outs[k // 4] = jnp.where(ok, piece, outs[k // 4])
    outs[2] = outs[2] + jnp.broadcast_to(scalars, (n, 128))
    for r in range(4):
        out_ref[pl.ds(r, n, stride=4), :] = outs[r] if r < 3 else jnp.zeros((n, 128), F32)


def scalar_row(items):
    lane = lanes((1, 128))
    row = jnp.zeros((1, 128), F32)
    for where, acc in items:
        s = jnp.sum(jnp.sum(acc, axis=0, keepdims=True), axis=1, keepdims=True)
        row = jnp.where(lane == where, jnp.broadcast_to(s, (1, 128)), row)
    return row


def smooth_plane(f, g, u, k, coefs, y0, y1):
    a0, a1 = operate_plane(f, k, coefs, y0, y1)
    e0, e1 = u[0, k, y0:y1, :] - a0, u[1, k, y0:y1, :] - a1
    refs, i = coefs
    p, q = refs[2][i, y0:y1, :], refs[3][i, y0:y1, :]
    g[0, k, 8 + y0 : 8 + y1, :] = f[0, k, 8 + y0 : 8 + y1, :] + (p * e0 - q * e1)
    g[1, k, 8 + y0 : 8 + y1, :] = f[1, k, 8 + y0 : 8 + y1, :] + (p * e1 + q * e0)


def window(halo, cy):
    if halo > 4:
        return 0, cy + 2 * HALO
    if halo > 0:
        return HALO - 4, HALO + cy + 4
    return HALO, HALO + cy


def pairs(lo, size, fn, low, high):
    for x in range(lo, HALO):
        y = size - 1 - x
        fn(x, low(x), HALO - x)
        fn(y, high(y), HALO - x)


def centre(f, g, u, t, t_rim, places, halo, s, ends, own, rows, t_rows, inner=None):
    mine, low, high = places
    cx, cy = own
    size = cx + 2 * HALO
    y0, y1 = HALO, HALO + cy
    pairs(
        HALO - halo + 1, size,
        lambda k, c, far: smooth_plane(f, g, u, k, c, *window(halo - 1 - far, cy)), low, high,
    )
    for x in range(HALO, HALO + cx) if inner is None else (HALO, HALO + cx - 1):
        smooth_plane(f, g, u, x, mine(x), *rows)
    u_own = lambda i: (u[0, i + HALO, y0:y1, :], u[1, i + HALO, y0:y1, :])

    def outer(k, c, far):
        q0, q1 = window(halo - 2 - far, cy)
        a0, a1 = operate_plane(g, k, c, q0, q1)
        t_rim[0, c[1], q0:q1, :], t_rim[1, c[1], q0:q1, :] = a0, a1

    pairs(HALO - halo + 2, size, outer, low, high)

    ones = below_ones()
    size_of = 2 * GROUP

    def middle(b, acc):
        where = [b * size_of + k for k in range(size_of)]
        return last_planes(g, u_own, t, s, mine, where, ends, own, t_rows, ones, acc)

    zero = jnp.zeros((8, 128), F32)
    if inner is None:
        return planes(0, cx // size_of, middle, (zero, zero), width=16 // size_of)
    where = [0, 1, cx - 2, cx - 1]
    return last_planes(g, u_own, t, s, mine, where, ends, own, t_rows, ones, inner)


def last_planes(g, u_own, t, s, mine, where, ends, own, t_rows, ones, acc, shift=HALO):
    cy = own[1]
    y0, y1 = HALO, HALO + cy
    r0, r1 = t_rows
    parts = []
    for i in where:
        k = i + shift
        a0, a1 = operate_plane(g, k, mine(i + HALO), r0, r1)
        t[0, i, r0:r1, :], t[1, i, r0:r1, :] = a0, a1
        lo = y0 - r0
        s[0, i] = g[0, k, 8 + y0 : 8 + y1, :]
        s[1, i] = g[1, k, 8 + y0 : 8 + y1, :]
        v0, v1 = u_own(i)
        parts.append((halves(v0 - a0[lo : lo + cy]), halves(v1 - a1[lo : lo + cy])))
    return restrict(parts, ends, where, ones, acc)


def fill(store, y0, y1, wave, layer, a):
    sq = wave * wave
    ab = sq * (layer * layer * (pml_strength / 9.0))
    d = 6.0 - sq
    w = jnp.where(wave > 0.0, damping * pl.reciprocal(d * d + ab * ab), 0.0)
    refs, i = store
    refs[0][i, y0:y1, :] = d
    refs[1][i, y0:y1, :] = ab
    refs[2][i, y0:y1, :] = d * w
    refs[3][i, y0:y1, :] = ab * w
    refs[4][i, y0:y1, :] = a


def own_kernel(own, rhs, wave, layer, agg, ylo, yhi, diag, absorb, sre, sim, ids, ends, sq_out,
               t, s, share, g_edge, u, f, g):
    cx, cy = own
    ey = cy + 2 * HALO
    home = (diag, absorb, sre, sim, ids)

    def inner(i, acc):
        store = (home, i)
        fill(store, 0, HALO, ylo[2, i], ylo[3, i], ylo[4, i].astype(jnp.int32))
        fill(store, HALO + cy, ey, yhi[2, i], yhi[3, i], yhi[4, i].astype(jnp.int32))
        fill(store, HALO, HALO + cy, wave[i], layer[i].astype(F32), agg[i])
        r0, r1 = rhs[0, i], rhs[1, i]
        return acc + fold8(r0 * r0 + r1 * r1)

    sq = planes(0, cx, inner, jnp.zeros((8, 128), F32), width=8)
    sq_out[...] = scalar_row([(40, sq)])

    def find(i):
        a = agg[i]
        lane = lanes(a.shape)
        low = jnp.zeros(a.shape, jnp.int32)
        step = a.shape[1] // 2
        while step >= 1:
            probe = low + step
            val = jnp.take_along_axis(a, probe - 1, axis=1, mode="promise_in_bounds")
            low = jnp.where(val <= lane, probe, low)
            step //= 2
        val = jnp.take_along_axis(a, low, axis=1, mode="promise_in_bounds")
        low = jnp.where(val <= lane, low + 1, low)
        ends[i] = jnp.maximum(low - 1, 0)

    planes(0, cx, find, width=8)

    def first(i, lo, hi, r0, r1):
        p, q = sre[i, lo:hi, :], sim[i, lo:hi, :]
        u[0, i, lo:hi, :] = r0
        u[1, i, lo:hi, :] = r1
        f[0, i, 8 + lo : 8 + hi, :] = p * r0 - q * r1
        f[1, i, 8 + lo : 8 + hi, :] = p * r1 + q * r0

    for i in range(cx):
        first(i, 0, HALO, ylo[0, i], ylo[1, i])
        first(i, HALO, HALO + cy, rhs[0, i], rhs[1, i])
        first(i, HALO + cy, ey, yhi[0, i], yhi[1, i])
    for i in range(1, cx - 1):
        smooth_plane(f, g, u, i, (home, i), 0, ey)
    for k, i in enumerate((1, 2, cx - 3, cx - 2)):
        for c in range(2):
            g_edge[c, k] = g[c, i]
    zero = jnp.zeros((8, 128), F32)
    acc = zero, zero
    ones = below_ones()
    for b in range(2, cx - 2, GROUP):
        acc = last_planes(
            g, lambda i: (rhs[0, i], rhs[1, i]), t, s, lambda x: (home, x - HALO),
            list(range(b, b + GROUP)), ends, own, (0, ey), ones, acc, shift=0,
        )
    for i in (1, cx - 2):
        for c in range(2):
            s[c, i] = g[c, i, 8 + HALO : 8 + HALO + cy, :]
    share[0:8, :], share[8:16, :] = acc


def start_kernel(grid, own, *refs):
    rhs, ylo, yhi, xlo, xhi, clo, chi, cols, ends, sq, _, _, share, g_edge = refs[:14]
    home, rim = refs[14:19], refs[19:24]
    t, t_rim, s, out_ref, u, f, g, pad = refs[24:]
    cx, cy = own
    ey = cy + 2 * HALO
    y0, y1 = HALO, HALO + cy
    mine = lambda x: (home, x - HALO)
    low = lambda x: (rim, x)
    high = lambda x: (rim, x - cx)

    def first(place, k, lo, hi, r0, r1):
        refs, i = place
        p, q = refs[2][i, lo:hi, :], refs[3][i, lo:hi, :]
        u[0, k, lo:hi, :] = r0
        u[1, k, lo:hi, :] = r1
        f[0, k, 8 + lo : 8 + hi, :] = p * r0 - q * r1
        f[1, k, 8 + lo : 8 + hi, :] = p * r1 + q * r0

    for k in range(HALO):
        for buf, corner, i, x in ((xlo, clo, HALO - 1 - k, HALO - 1 - k), (xhi, chi, k, HALO + cx + k)):
            place = low(x) if x < HALO else high(x)
            below, above = corner_plane(corner, k)
            for src, lo, hi in ((below, 0, y0), (buf[:, i], y0, y1), (above, y1, ey)):
                fill(place, lo, hi, src[2], src[3], src[4].astype(jnp.int32))
                first(place, x, lo, hi, src[0], src[1])

    def inner(x):
        i = x - HALO
        first(mine(x), x, 0, y0, ylo[0, i], ylo[1, i])
        first(mine(x), x, y0, y1, rhs[0, i], rhs[1, i])
        first(mine(x), x, y1, ey, yhi[0, i], yhi[1, i])

    for i in (0, 1, cx - 2, cx - 1):
        inner(HALO + i)
    for k, i in enumerate((1, 2, cx - 3, cx - 2)):
        for c in range(2):
            g[c, HALO + i] = g_edge[c, k]
    g0, g1 = centre(
        f, g, u, t, t_rim, (mine, low, high), HALO, s, ends, own, (0, ey), (0, ey), (share[0:8, :], share[8:16, :])
    )
    spread_rhs(g0, g1, cols, pad, out_ref, sq[...], grid)


def read_scalars(raw, olds, j):
    h = []
    for i in range(j):
        a0, a1 = pick(raw, 32 + 2 * i), pick(raw, 33 + 2 * i)
        for k in range(i):
            b0, b1 = pick(olds[i], 32 + 2 * k), pick(olds[i], 33 + 2 * k)
            a0, a1 = a0 - (b0 * h[k][0] + b1 * h[k][1]), a1 - (b0 * h[k][1] - b1 * h[k][0])
        inv = pick(olds[i], 41)
        h.append((a0 * inv, a1 * inv))
    sq = pick(raw, 40)
    for a0, a1 in h:
        sq = sq - (a0 * a0 + a1 * a1)
    length = jnp.sqrt(jnp.maximum(sq, 0.0) + epsilon)
    return h, length


def write_scalars(out, h, length, inv):
    lane = lanes((1, 128))
    row = jnp.where(lane == 40, length[0:1], inv[0:1])
    for k, pair in enumerate(h):
        for c in range(2):
            row = jnp.where(lane == 32 + 2 * k + c, pair[c][0:1], row)
    out[...] = row


def like(v, rows):
    return jnp.concatenate([v] * (rows // 8), axis=0)


def combine(scalars, new, old):
    h, inv = scalars
    a0, a1 = new
    rows = a0.shape[0]
    for i in range(len(h)):
        b0, b1 = old(i)
        r, q = like(h[i][0], rows), like(h[i][1], rows)
        a0 = a0 - (r * b0 - q * b1)
        a1 = a1 - (r * b1 + q * b0)
    s = like(inv, rows)
    return a0 * s, a1 * s


def splats(row, first):
    return [pick(row, first + k) for k in range(AGG)]


def marks(index):
    return [(index & 1) == 1, (index & 3) >= 2, (index & 7) >= 4, index >= 8]


def choose(values, bits):
    rows = bits[0].shape[0]
    level = [like(v, rows) for v in values]
    for bit in bits:
        level = [jnp.where(bit, level[k + 1], level[k]) for k in range(0, len(level), 2)]
    return level[0]


def prolong_plane(pc, k, ids, i, table, own, dx, values=None, wide_y=True):
    cy = own[1]
    ey = cy + 2 * HALO
    for dy, lo, hi in ((0, 0, HALO), (1, HALO, HALO + cy), (2, HALO + cy, ey)):
        n = dx * 3 + dy
        if dy != 1 and not wide_y:
            continue
        if values is not None and dy == 1:
            bits = marks(ids[i, lo:hi, :])
            for c in range(2):
                pc[c, k, 8 + lo : 8 + hi, :] = choose(values[c], bits)
            continue
        src = table[:, 128 * (n // 4) : 128 * (n // 4) + 128]
        index = ids[i, lo:hi, :] + 32 * (n % 4)
        pc[0, k, 8 + lo : 8 + hi, :] = take(src, index)
        pc[1, k, 8 + lo : 8 + hi, :] = take(src, index + AGG)


def image_plane(pc, k, coefs, t_in, m_old, scalars, lo, hi):
    i = coefs[1]
    a0, a1 = operate_plane(pc, k, coefs, lo, hi)
    m = combine(
        scalars,
        (t_in[0, i, lo:hi, :], t_in[1, i, lo:hi, :]),
        lambda n: (m_old[n][0, i, lo:hi, :], m_old[n][1, i, lo:hi, :]),
    )
    return m, (m[0] + a0, m[1] + a1)


def image_store(pc, u, f, k, coefs, t_in, m_old, scalars, m_out, lo, hi):
    m, (u0, u1) = image_plane(pc, k, coefs, t_in, m_old, scalars, lo, hi)
    refs, i = coefs
    if m_out is not None:
        m_out[0, i, lo:hi, :], m_out[1, i, lo:hi, :] = m
    p, q = refs[2][i, lo:hi, :], refs[3][i, lo:hi, :]
    u[0, k, lo:hi, :], u[1, k, lo:hi, :] = u0, u1
    f[0, k, 8 + lo : 8 + hi, :] = p * u0 - q * u1
    f[1, k, 8 + lo : 8 + hi, :] = p * u1 + q * u0
    return u0, u1


def step_kernel(j, grid, own, *refs):
    refs = list(refs)
    take_refs = lambda k: [refs.pop(0) for _ in range(k)]
    last = j == ITERS - 1
    rcv = refs.pop(0)
    home, rim = take_refs(5), take_refs(5)
    ends, cols, t_own, t_rim = take_refs(4)
    m_own, m_rim = take_refs(j), take_refs(0 if last else j)
    u_in, c_old, h_old = take_refs(j + 1), take_refs(j), take_refs(j)
    c_out, h_out, out_ref = take_refs(3)
    if not last:
        m_out, t, u_out, s_out = take_refs(4)
    mr_out = tr_out = None
    if j < ITERS - 2:
        mr_out, tr_out = take_refs(2)
    pc = refs.pop(0)
    if not last:
        u, f, pad = take_refs(3)
    cx, cy = own
    mine = lambda x: (home, x - HALO)
    low = lambda x: (rim, x)
    high = lambda x: (rim, x - cx)
    y0, y1 = HALO, HALO + cy
    halo = HALO - 2 - 2 * j
    rows = window(halo, cy)
    size = cx + 2 * HALO

    n = rcv.shape[0] // 4
    row = jnp.concatenate(
        [jnp.sum(rcv[pl.ds(r, n, stride=4), :], axis=0, keepdims=True) for r in range(3)], axis=1
    )
    h, length = read_scalars(row[:, 256:384], [r[...] for r in h_old], j)
    inv = 1.0 / length
    write_scalars(h_out, h, length, inv)
    scalars = h, inv
    wide = lambda v: jnp.concatenate([v[0:1]] * 3, axis=1)
    table = row
    for i in range(j):
        old = c_old[i][...]
        table = table - (wide(h[i][0]) * old + wide(h[i][1]) * turn_rows(old))
    table = table * wide(inv)
    c_out[...] = table

    for x in range(HALO - halo - 1, HALO):
        y = 2 * HALO - 1 - x
        wide_y = halo + 1 - (HALO - x) > 0
        prolong_plane(pc, x, rim[4], x, table, own, 0, wide_y=wide_y)
        prolong_plane(pc, y + cx, rim[4], y, table, own, 2, wide_y=wide_y)
    values = [splats(table[:, 128:256], AGG * c) for c in range(2)]
    planes(HALO, HALO + cx, lambda x: prolong_plane(pc, x, home[4], x - HALO, table, own, 1, values))

    def outer(k, c, far):
        image_store(pc, u, f, k, c, t_rim, m_rim, scalars, mr_out, *window(halo - far, cy))

    pairs(HALO - halo, size, outer, low, high)

    def middle(x, acc):
        i = x - HALO
        if last:
            u0, u1 = image_plane(pc, x, mine(x), t_own, m_own, scalars, y0, y1)[1]
        else:
            u0, u1 = image_store(pc, u, f, x, mine(x), t_own, m_own, scalars, m_out, *rows)
            lo = y0 - rows[0]
            u0, u1 = u0[lo : lo + cy], u1[lo : lo + cy]
            u_out[0, i], u_out[1, i] = u0, u1
        new = []
        for k in range(j + 1):
            b0, b1 = u_in[k][0, i], u_in[k][1, i]
            new.append(fold8(b0 * u0 + b1 * u1))
            new.append(fold8(b0 * u1 - b1 * u0))
        new.append(fold8(u0 * u0 + u1 * u1))
        return tuple(a + b for a, b in zip(acc, new))

    zero = jnp.zeros((8, 128), F32)
    acc = planes(HALO, HALO + cx, middle, (zero,) * (2 * j + 3))
    items = [(32 + k, acc[k]) for k in range(2 * j + 2)] + [(40, acc[-1])]
    dots = scalar_row(items)
    if last:
        out_ref[...] = jnp.broadcast_to(dots, out_ref.shape)
        return
    t_rows = rows if j < ITERS - 2 else (y0, y1)
    g0, g1 = centre(f, pc, u, t, tr_out, (mine, low, high), halo, s_out, ends, own, rows, t_rows)
    spread_rhs(g0, g1, cols, pad, out_ref, dots, grid)


def pack_kernel(rhs, wave, layer, agg, ylow, yhigh, xlow, xhigh, yint, xint, sems):
    cx, cy = wave.shape[:2]
    every = slice(None)
    cuts = (
        (ylow, yint, 0, every, pl.ds(0, HALO)),
        (yhigh, yint, 2, every, pl.ds(cy - HALO, HALO)),
        (xlow, xint, 0, pl.ds(0, HALO), every),
        (xhigh, xint, 2, pl.ds(cx - HALO, HALO), every),
    )
    copies = []
    for k, (out, ints, slot, xs, ys) in enumerate(cuts):
        for i, (src, dst) in enumerate((
            (rhs.at[:, xs, ys, :], out.at[0:2]),
            (wave.at[xs, ys, :], out.at[2]),
            (layer.at[xs, ys, :], ints.at[slot]),
            (agg.at[xs, ys, :], ints.at[slot + 1]),
        )):
            copies.append(pltpu.make_async_copy(src, dst, sems.at[4 * k + i]))
    for copy in copies:
        copy.start()
    for copy in copies:
        copy.wait()
    for out, ints, slot, _, _ in cuts:
        out[3] = ints[slot].astype(F32)
        out[4] = ints[slot + 1].astype(F32)


def corner_kernel(ylo, yhi, low, high):
    cx = ylo.shape[1]
    row = lax.broadcasted_iota(jnp.int32, (5, HALO, ylo.shape[3]), 1)
    for out, plane in ((low, lambda k: k), (high, lambda k: cx - 1 - k)):
        for p in range(HALO // 2):
            a, b = plane(p), plane(HALO - 2 - p)
            out[:, p, 0:HALO, :] = jnp.where(row > p, ylo[:, a], pltpu.roll(ylo[:, b], p + 1, 1))
            out[:, p, HALO : 2 * HALO, :] = jnp.where(
                row < HALO - 1 - p, yhi[:, a], pltpu.roll(yhi[:, b], HALO - 1 - p, 1)
            )


def corner_plane(buf, k):
    if k == HALO - 1:
        zero = jnp.zeros((5, HALO, buf.shape[3]), F32)
        return zero, zero
    p = min(k, HALO - 2 - k)
    below, above = buf[:, p, 0:HALO, :], buf[:, p, HALO : 2 * HALO, :]
    if k != p:
        below, above = pltpu.roll(below, HALO - 1 - p, 1), pltpu.roll(above, p + 1, 1)
    return below, above


def columns_kernel(inverse, out, turned):
    turned[:, 0:32] = inverse[...].T
    group = lanes(out.shape) // 32
    total = jnp.zeros(out.shape, F32)
    for r in range(4):
        part = turned[pl.ds(r, out.shape[0], stride=4), :]
        part = jnp.where(group == 0, part, 0.0)
        total = total + (part if r == 0 else pltpu.roll(part, 32 * r, 1))
    out[...] = total


def arrange_kernel(got, out):
    n = got.shape[0] // 4
    for q in range(4):
        rows = got[pl.ds(q, n, stride=4), :]
        out[q * n : (q + 1) * n, :] = rows
        out[(4 + q) * n : (5 + q) * n, :] = turn(rows)


def cmul(a, b):
    return a[0] * b[0] - a[1] * b[1], a[0] * b[1] + a[1] * b[0]


def finish_kernel(own, *refs):
    rcv, ids = refs[0], refs[1]
    z = refs[2 : 2 + ITERS]
    c = refs[2 + ITERS : 2 + 2 * ITERS]
    rows = refs[2 + 2 * ITERS : 2 + 3 * ITERS]
    sol, hess = refs[2 + 3 * ITERS :]
    cx, cy = own
    final = jnp.sum(rcv[pl.ds(2, rcv.shape[0] // 4, stride=4), :], axis=0, keepdims=True)
    scal = [r[...] for r in rows]
    beta = pick(scal[0], 40)
    upper, sub = [], []
    for j in range(1, ITERS):
        upper.append([(pick(scal[j], 32 + 2 * i), pick(scal[j], 33 + 2 * i)) for i in range(j)])
        sub.append(pick(scal[j], 40))
    h, length = read_scalars(final, scal, ITERS)
    upper.append(h)
    sub.append(length)
    r_i = lax.broadcasted_iota(jnp.int32, (8, 128), 0)
    c_i = lanes((8, 128))
    for comp in range(2):
        block = jnp.zeros((8, 128), F32)
        for j in range(ITERS):
            for i in range(j + 1):
                block = jnp.where((r_i == j) & (c_i == i), upper[j][i][comp], block)
            if comp == 0:
                block = jnp.where((r_i == j) & (c_i == j + 1), sub[j], block)
        hess[comp] = block[0:ITERS, 0 : ITERS + 1]
    zero = jnp.zeros((8, 128), F32)
    target = [(beta, zero)]
    rot = []
    tri = []
    for j in range(ITERS):
        col = list(upper[j])
        for i in range(j):
            cr, ci, s = rot[i]
            a, b = col[i], col[i + 1]
            up = cmul((cr, -ci), a)
            dn = cmul((cr, ci), b)
            col[i] = (up[0] + s * b[0], up[1] + s * b[1])
            col[i + 1] = (dn[0] - s * a[0], dn[1] - s * a[1])
        a = col[j]
        big = jnp.sqrt(a[0] * a[0] + a[1] * a[1] + sub[j] * sub[j])
        w = 1.0 / big
        cr, ci, s = a[0] * w, a[1] * w, sub[j] * w
        rot.append((cr, ci, s))
        g = target[j]
        target[j] = cmul((cr, -ci), g)
        target.append((-s * g[0], -s * g[1]))
        col[j] = big
        tri.append(col)
    y = [None] * ITERS
    for j in reversed(range(ITERS)):
        a0, a1 = target[j]
        for k in range(j + 1, ITERS):
            b = cmul(tri[k][j], y[k])
            a0, a1 = a0 - b[0], a1 - b[1]
        w = 1.0 / tri[j][j]
        y[j] = (a0 * w, a1 * w)
    table = jnp.zeros((1, 128), F32)
    for j in range(ITERS):
        old = c[j][:, 128:256]
        table = table + (y[j][0][0:1] * old + y[j][1][0:1] * turn(old))

    gamma = list(y)
    for j in reversed(range(ITERS)):
        w = 1.0 / (sub[j - 1] if j > 0 else beta)
        gamma[j] = (gamma[j][0] * w, gamma[j][1] * w)
        for i in range(j):
            b = cmul(upper[j - 1][i], gamma[j])
            gamma[i] = (gamma[i][0] - b[0], gamma[i][1] - b[1])

    values = splats(table, AGG)

    def go(i):
        index = ids[i, HALO : HALO + cy, :]
        a0, a1 = take(table, index), choose(values, marks(index))
        for j in range(ITERS):
            b = cmul((like(gamma[j][0], cy), like(gamma[j][1], cy)), (z[j][0, i], z[j][1, i]))
            a0, a1 = a0 + b[0], a1 + b[1]
        sol[0, i], sol[1, i] = a0, a1

    planes(0, cx, go)


def shape(*dims, dtype=F32):
    return jax.ShapeDtypeStruct(dims, dtype)


def call(kernel, outs, scratch, args, flops=100_000_000, space=pltpu.VMEM, aliases=None):
    return pl.pallas_call(
        kernel,
        out_shape=outs,
        in_specs=[pl.BlockSpec(memory_space=space)] * len(args),
        out_specs=[pl.BlockSpec(memory_space=pltpu.VMEM)] * len(outs),
        scratch_shapes=scratch,
        input_output_aliases=aliases or {},
        compiler_params=pltpu.CompilerParams(vmem_limit_bytes=VLIMIT),
        cost_estimate=pl.CostEstimate(flops=flops, bytes_accessed=1_000_000, transcendentals=0),
    )(*args)


def exchange(x):
    return lax.all_to_all(x, AXES, 0, 0, tiled=True)


def program(right_side, wavenumber, pml_layer, aggregate, coarse_inverse):
    gx, gy = lax.axis_size("gx"), lax.axis_size("gy")
    n = gx * gy
    cx, cy, cz = wavenumber.shape
    own = (cx, cy)
    ex, ey = cx + 2 * HALO, cy + 2 * HALO
    grid = (gx, gy)
    margin = -(-(gy + 1) // 8) * 8

    def swap(low, high, axis):
        count = lax.axis_size(axis)
        up = [(i, i + 1) for i in range(count - 1)]
        down = [(b, a) for a, b in up]
        low_in = lax.ppermute(high, axis, up)
        high_in = lax.ppermute(low, axis, down)
        return low_in, high_in

    strip, slab = shape(5, cx, HALO, cz), shape(5, HALO, cy, cz)
    ylow, yhigh, xlow, xhigh = call(
        pack_kernel, [strip, strip, slab, slab],
        [pltpu.VMEM((4, cx, HALO, cz), jnp.int32), pltpu.VMEM((4, HALO, cy, cz), jnp.int32), pltpu.SemaphoreType.DMA((16,))],
        [pltpu.with_memory_space_constraint(x, pltpu.HBM) for x in (right_side, wavenumber, pml_layer, aggregate)],
        space=pltpu.HBM,
    )
    ylo, yhi = swap(ylow, yhigh, "gy")
    xlo, xhi = swap(xlow, xhigh, "gx")
    (inverse,) = call(
        columns_kernel, [shape(4 * n, 128)], [pltpu.VMEM((AGG * n, 128), F32)],
        [coarse_inverse.reshape(2 * AGG, AGG * n)],
    )
    cols = exchange(inverse)
    right_side, wavenumber, pml_layer, aggregate, ylo, yhi, cols = lax.optimization_barrier(
        (right_side, wavenumber, pml_layer, aggregate, ylo, yhi, cols)
    )
    corner = shape(5, HALO // 2, 2 * HALO, cz)
    clow, chigh = call(corner_kernel, [corner, corner], [], [ylo, yhi])
    clo, chi = swap(clow, chigh, "gx")
    (cols,) = call(arrange_kernel, [shape(8 * n, 128)], [], [cols])
    I32 = jnp.int32
    home = [shape(cx, ey, cz)] * 4 + [shape(cx, ey, cz, dtype=I32)]
    rim = [shape(2 * HALO, ey, cz)] * 4 + [shape(2 * HALO, ey, cz, dtype=I32)]
    home2, rim2 = shape(2, cx, ey, cz), shape(2, 2 * HALO, ey, cz)
    mine = shape(2, cx, cy, cz)
    chunk = shape(4 * n, 128)
    vmem = lambda *dims, dtype=F32: pltpu.VMEM(dims, dtype)
    tall = vmem(2, ex, ey + 16, cz)
    flat = vmem(2, ex, ey, cz)
    pad = vmem(n + 2 * margin, 128)

    short_tall = vmem(2, cx, ey + 16, cz)
    *own_coefs, ends, sq, t_own, s, share, g_edge = call(
        functools.partial(own_kernel, own),
        home + [shape(cx, cy, cz, dtype=I32), shape(1, 128), home2, mine, shape(16, 128), shape(2, 4, ey + 16, cz)],
        [vmem(2, cx, ey, cz), short_tall, short_tall],
        [right_side, wavenumber, pml_layer, aggregate, ylo, yhi],
    )
    res = call(
        functools.partial(start_kernel, grid, own),
        rim + [home2, rim2, mine, chunk],
        [flat, tall, tall, pad],
        [right_side, ylo, yhi, xlo, xhi, clo, chi, cols, ends, sq, t_own, s, share, g_edge] + own_coefs,
        aliases={10: 5, 11: 7},
    )
    rim_coefs = list(res[:5])
    t_own, t_rim, s, send = res[5:]
    got = exchange(send)
    ms, mrs, us, ss, cs, hs = [], [], [right_side], [s], [], []
    for j in range(ITERS):
        last = j == ITERS - 1
        args = [got] + own_coefs + rim_coefs + [ends, cols, t_own, t_rim] + ms + ([] if last else mrs) + us + cs + hs
        outs = [shape(1, 384), shape(1, 128), chunk]
        scratch = [tall]
        if not last:
            outs += [home2, home2, mine, mine]
            if j < ITERS - 2:
                outs += [rim2, rim2]
            scratch += [flat, tall, pad]
        c, h, send, *rest = call(functools.partial(step_kernel, j, grid, own), outs, scratch, args)
        got = exchange(send)
        if not last:
            m, t_own, u, s = rest[:4]
            us.append(u)
            ms.append(m)
            ss.append(s)
            if j < ITERS - 2:
                mrs.append(rest[4])
                t_rim = rest[5]
        cs.append(c)
        hs.append(h)
    sol, hess = call(
        functools.partial(finish_kernel, own),
        [mine, shape(2, ITERS, ITERS + 1)],
        [],
        [got, own_coefs[4]] + ss + cs + hs,
    )
    return sol, jnp.swapaxes(hess, 1, 2)


def solution(mesh):
    return jax.shard_map(
        program,
        mesh=mesh,
        in_specs=(
            P(None, "gx", "gy", None),
            P("gx", "gy", None),
            P("gx", "gy", None),
            P("gx", "gy", None),
            P(None, ("gx", "gy"), None),
        ),
        out_specs=(P(None, "gx", "gy", None), P()),
        check_vma=False,
    )
```
